32 devices in a mesh: blk: 16 (over z, y, core), rel: 2 (over x).
Axes of the slice: x: 2, y: 2, z: 4, core: 2. Of those that a mesh axis runs over, the one named last changes fastest.
Arguments:
- source_table: float32 [400, 24576], P(None, ('blk', 'rel')), may hold values from -1.2 to 1.2
- source_state: float32 [24576], P(('blk', 'rel')), may hold values from 0.001 to 0.1
- target_table: float32 [400, 24576], P(None, ('blk', 'rel')), may hold values from -1.2 to 1.2
- target_state: float32 [24576], P(('blk', 'rel')), may hold values from 0.001 to 0.1
- relation_ops: float32 [400, 2048], P(None, 'blk'), may hold values from 0.5 to 1.5
- relation_state: float32 [400, 2048], P(None, 'blk'), may hold values from 0.01 to 1
- source_ids: int32 [2, 16384], P(None, ('blk', 'rel')), may hold values from 0 to 767
- target_ids: int32 [2, 16384], P(None, ('blk', 'rel')), may hold values from 0 to 767
- relation_ids: int32 [2, 16384], P(None, ('blk', 'rel')), may hold values from 0 to 127
- negative_ids: int32 [2, 16384], P(None, ('blk', 'rel')), may hold values from 0 to 767
Outputs:
- new_source: float32 [400, 24576], P(None, ('blk', 'rel'))
- new_source_state: float32 [24576], P(('blk', 'rel'))
- held_target: float32 [400, 24576], P(None, ('blk', 'rel'))
- held_target_state: float32 [24576], P(('blk', 'rel'))
- new_relations: float32 [400, 2048], P(None, 'blk')
- new_relation_state: float32 [400, 2048], P(None, 'blk')
The draws below stay inside these ranges and needn't reach their ends.
All inputs are finite; a program needn't handle non-finite values.
Results may differ from the reference program's by a relative error of at most 0.0001.
Values sent between devices are 32-bit elements; how exact they have to be, the bound alone decides.
A program may use at most 64 MiB of HBM per device.

```python
import math
import jax
import jax.numpy as jnp
from jax import lax

D = 400
ROWS = 768
EDGE_DEV = 512
NEG_DEV = 512
REL_DEV = 128
BUCKETS = 2
ENTITIES = 24576
EDGES = 16384
NEGS = 16384
RELS = 2048
N_BLK = 16
N_REL = 2


def touch_ends(entries, own_key, low, top_value):
    spot = [jax.random.randint(jax.random.fold_in(own_key, axis), (), 0, length) for axis, length in enumerate(entries.shape)]
    main_axis = entries.shape.index(max(entries.shape))
    beside = spot[:main_axis] + [(spot[main_axis] + 1) % entries.shape[main_axis]] + spot[main_axis + 1:]
    return entries.at[tuple(spot)].set(low).at[tuple(beside)].set(top_value)


def shard_levels(rng, shape, split, smallest, high):
    def one(dim, blocks):
        heights = jax.random.uniform(jax.random.fold_in(jax.random.fold_in(rng, 6), dim), (blocks,), jnp.float32, smallest / len(split), high / len(split))
        return jnp.repeat(jnp.exp(heights), shape[dim] // blocks).reshape((-1,) + (1,) * (len(shape) - dim - 1))

    gain = one(*split[0])
    for cut in split[1:]:
        gain = gain * one(*cut)
    return gain


def bell_draw(rng, shape, deviation, limit, shards=(), dtype=jnp.bfloat16):
    gain = shard_levels(rng, shape, shards, -0.22, 0.18) if shards else 1.0
    drawn = jax.random.normal(rng, shape, jnp.float32) * deviation * gain
    return jnp.minimum(jnp.maximum(drawn, -limit), limit).astype(dtype)


def setup_inputs(seed: int = 0) -> dict:
    streams_of = jax.random.split(jax.random.key(seed), 11)
    source_table = bell_draw(streams_of[0], (D, ENTITIES), 0.2, 1.2, ((1, 32),), jnp.float32)
    source_state = jnp.clip(jnp.exp(math.log(0.1) - 4.6051702 * jax.random.uniform(streams_of[1], (ENTITIES,), jnp.float32) ** shard_levels(streams_of[1], (ENTITIES,), ((0, 32),), -0.2, 0.2)), 0.001, 0.1)
    target_table = bell_draw(streams_of[2], (D, ENTITIES), 0.2, 1.2, ((1, 32),), jnp.float32)
    target_state = jnp.clip(jnp.exp(math.log(0.1) - 4.6051702 * jax.random.uniform(streams_of[3], (ENTITIES,), jnp.float32) ** shard_levels(streams_of[3], (ENTITIES,), ((0, 32),), -0.2, 0.2)), 0.001, 0.1)
    relation_ops = jnp.clip(0.5 + 1.0 * jax.random.uniform(streams_of[4], (D, RELS), jnp.float32) ** shard_levels(streams_of[4], (D, RELS), ((1, 16),), -0.2, 0.2), 0.5, 1.5)
    relation_state = jnp.clip(jnp.exp(math.log(1.0) - 4.6051702 * jax.random.uniform(streams_of[5], (D, RELS), jnp.float32) ** shard_levels(streams_of[5], (D, RELS), ((1, 16),), -0.2, 0.2)), 0.01, 1.0)
    source_ids = touch_ends(jax.random.randint(streams_of[6], (BUCKETS, EDGES), 0, ROWS), jax.random.fold_in(streams_of[6], 1), 0, ROWS - 1).astype(jnp.int32)
    target_ids = touch_ends(jax.random.randint(streams_of[7], (BUCKETS, EDGES), 0, ROWS), jax.random.fold_in(streams_of[7], 1), 0, ROWS - 1).astype(jnp.int32)
    relation_ids = touch_ends(jax.random.randint(streams_of[8], (BUCKETS, EDGES), 0, REL_DEV), jax.random.fold_in(streams_of[8], 1), 0, REL_DEV - 1).astype(jnp.int32)
    negative_ids = touch_ends(jax.random.randint(streams_of[9], (BUCKETS, NEGS), 0, ROWS), jax.random.fold_in(streams_of[9], 1), 0, ROWS - 1).astype(jnp.int32)
    return {"source_table": source_table, "source_state": source_state, "target_table": target_table, "target_state": target_state, "relation_ops": relation_ops, "relation_state": relation_state, "source_ids": source_ids, "target_ids": target_ids, "relation_ids": relation_ids, "negative_ids": negative_ids}


learn_rate = 0.1
epsilon = 1e-06
HIGHEST = lax.Precision.HIGHEST

def row_adagrad(matrix, row_state, gradient):
    fresh = row_state + lax.optimization_barrier(jnp.mean(gradient * gradient, axis=0))
    return (matrix - learn_rate * gradient / (jnp.sqrt(fresh) + epsilon)[None, :], fresh)

def slice_step(source_side, source_rows, target_side, target_rows, relations, source_idx, target_idx, relation_idx, negative_idx):
    source = jnp.take(source_side, source_idx, axis=1)
    target = jnp.take(target_side, target_idx, axis=1)
    negative = jnp.take(target_side, negative_idx, axis=1)
    relation = jnp.take(relations, relation_idx, axis=1)
    queries = source * relation
    positive = lax.optimization_barrier(jnp.sum(queries * target, axis=0))
    neg_score = lax.dot_general(queries, negative, (((0,), (0,)), ((), ())), precision=HIGHEST)
    pos_coef = -jax.nn.sigmoid(-positive)
    neg_coef = jax.nn.sigmoid(neg_score) / negative_idx.shape[0]
    grad_query = target * pos_coef[None, :] + lax.dot_general(negative, neg_coef, (((1,), (1,)), ((), ())), precision=HIGHEST)
    grad_target = queries * pos_coef[None, :]
    grad_negative = jnp.dot(queries, neg_coef, precision=HIGHEST)
    target_grad = jnp.zeros_like(target_side).at[:, target_idx].add(grad_target).at[:, negative_idx].add(grad_negative)
    source_grad = jnp.zeros_like(source_side).at[:, source_idx].add(grad_query * relation)
    relation_grad = jnp.zeros_like(relations).at[:, relation_idx].add(grad_query * source)
    new_target, new_target_rows = row_adagrad(target_side, target_rows, target_grad)
    new_source, new_source_rows = row_adagrad(source_side, source_rows, source_grad)
    return (new_source, new_source_rows, new_target, new_target_rows, relation_grad)

def reference(source_table, source_state, target_table, target_state, relation_ops, relation_state, source_ids, target_ids, relation_ids, negative_ids):
    slice_count = N_BLK * N_REL

    def split_table(matrix):
        return matrix.reshape(D, slice_count, ROWS).transpose(1, 0, 2)

    def join_table(blocks):
        return blocks.transpose(1, 0, 2).reshape(D, slice_count * ROWS)
    source_blocks = split_table(source_table)
    source_rows = source_state.reshape(slice_count, ROWS)
    target_blocks = split_table(target_table)
    target_rows = target_state.reshape(slice_count, ROWS)
    relation_blocks = relation_ops.reshape(D, N_BLK, REL_DEV).transpose(1, 0, 2)
    source_split = source_ids.reshape(BUCKETS, slice_count, EDGE_DEV)
    target_split = target_ids.reshape(BUCKETS, slice_count, EDGE_DEV)
    relation_split = relation_ids.reshape(BUCKETS, slice_count, EDGE_DEV)
    negative_split = negative_ids.reshape(BUCKETS, slice_count, NEG_DEV)
    owners = (jnp.arange(slice_count) // N_REL).astype(jnp.int32)
    summed = jnp.zeros((N_BLK, D, REL_DEV), jnp.float32)

    def per_slice(items):
        src_side, src_rows, tgt_side, tgt_rows, owner, src_idx, tgt_idx, rel_idx, neg_idx = items
        return slice_step(src_side, src_rows, tgt_side, tgt_rows, relation_blocks[owner], src_idx, tgt_idx, rel_idx, neg_idx)
    for bucket in range(BUCKETS):
        if bucket > 0:
            target_blocks = jnp.roll(target_blocks, N_REL, axis=0)
            target_rows = jnp.roll(target_rows, N_REL, axis=0)
        source_blocks, source_rows, target_blocks, target_rows, relation_grads = lax.map(per_slice, (source_blocks, source_rows, target_blocks, target_rows, owners, source_split[bucket], target_split[bucket], relation_split[bucket], negative_split[bucket]))
        summed = summed + relation_grads.reshape(N_BLK, N_REL, D, REL_DEV).sum(axis=1)
    summed_flat = summed.transpose(1, 0, 2).reshape(D, N_BLK * REL_DEV)
    new_relation_state = relation_state + summed_flat * summed_flat
    new_relations = relation_ops - learn_rate * summed_flat / (jnp.sqrt(new_relation_state) + epsilon)
    return (join_table(source_blocks), source_rows.reshape(slice_count * ROWS), join_table(target_blocks), target_rows.reshape(slice_count * ROWS), new_relations, new_relation_state)
```

```python
import functools

import jax
import jax.numpy as jnp
from jax import lax
from jax.experimental import pallas as pl
from jax.experimental.pallas import tpu as pltpu
from jax.sharding import PartitionSpec as P

learn_rate = 0.1
epsilon = 1e-06
LANES = 128
MESH = pl.DeviceIdType.MESH
F32 = jnp.float32
BF16 = jnp.bfloat16


def split(x):
    high = x.astype(BF16)
    return high, (x - high.astype(F32)).astype(BF16)


def nn(a, b):
    return lax.dot_general(a, b, (((1,), (0,)), ((), ())), preferred_element_type=F32)


def nt(a, b):
    return lax.dot_general(a, b, (((1,), (1,)), ((), ())), preferred_element_type=F32)


def column(row):
    wide = jnp.broadcast_to(row.astype(F32), (8, row.shape[1]))
    return jnp.transpose(wide)[:, :1].astype(jnp.int32)


def chunk_plan(rows):
    if rows % 256 == 0 and rows >= 512:
        widths = [LANES] + [256] * (rows // 256 - 1) + [LANES]
    else:
        widths = [LANES] * (rows // LANES)
    return [(sum(widths[:i]), w) for i, w in enumerate(widths)]


def row_blocks(dims):
    half = (dims // 2 + 15) // 16 * 16
    return [(0, half), (half, dims - half)]


def emit(*refs):
    inputs, outputs, (first, second, sem) = refs[:6], refs[6:12], refs[12:]
    copies = []
    for i in (0, 2, 4, 5):
        copies.append(pltpu.make_async_copy(inputs[i], outputs[i], sem.at[i]))
        copies[-1].start()
    for i, line in ((1, first), (3, second)):
        line[...] = inputs[i][0, :]
        copies.append(pltpu.make_async_copy(line, outputs[i], sem.at[i]))
        copies[-1].start()
    for copy in copies:
        copy.wait()


def kernel(n_blk, n_rel, plan, blocks, *refs):
    refs = list(refs)

    def take(n):
        out = refs[:n]
        del refs[:n]
        return out

    src_in, srow_in, tgt_in, trow_in, rel_in, rstate_in, sid_in, rid_in, tid_in, nid_in = take(10)
    out_src, out_srow, out_tgt, out_trow, out_rel, out_rstate = take(6)
    src_ref, srow_ref, tgt_ref, trow_ref, rel_ref, rstate_ref, sid_ref, rid_ref, tid_ref, nid_ref = take(10)
    load_sem, hot, rhot, qt_ref, q_ref, picked, relation, gq_ref, rel_all = take(9)
    rsend_sem, rrecv_sem, send_sem, recv_sem, row_send, row_recv = take(6)
    tables, weights = take(len(plan)), take(len(plan))
    send, recv = take(len(plan)), take(len(plan))
    dims, rows = src_ref.shape
    buckets, edges = sid_ref.shape
    negs = nid_ref.shape[1]
    rels = rel_ref.shape[1]
    final = len(plan) - 1
    my_blk = lax.axis_index("blk")
    my_rel = lax.axis_index("rel")
    nxt = lax.rem(my_blk + 1, n_blk)
    prv = lax.rem(my_blk + n_blk - 1, n_blk)

    loads = []

    def load(there, here):
        loads.append(pltpu.make_async_copy(there, here, load_sem.at[len(loads)]))
        loads[-1].start()
        return loads[-1]

    load_ids = [load(sid_in, sid_ref), load(rid_in, rid_ref)]
    load_rel = load(rel_in, rel_ref)
    load_src = [load(src_in.at[pl.ds(r, n)], src_ref.at[pl.ds(r, n)]) for r, n in blocks]
    load_other = [load(tid_in, tid_ref), load(nid_in, nid_ref), load(trow_in, trow_ref)]
    load_tgt = load(tgt_in, tgt_ref)
    load_late = [load(srow_in, srow_ref), load(rstate_in, rstate_ref)]

    barrier = pltpu.get_barrier_semaphore()
    pl.semaphore_signal(barrier, inc=1, device_id={"blk": prv}, device_id_type=MESH)
    for step in range(1, n_rel):
        pl.semaphore_signal(
            barrier, inc=1, device_id={"rel": lax.rem(my_rel + step, n_rel)}, device_id_type=MESH
        )

    def hop(bucket, c):
        return pltpu.make_async_remote_copy(
            src_ref=send[c].at[bucket],
            dst_ref=recv[c].at[bucket],
            send_sem=send_sem.at[0, bucket, c],
            recv_sem=recv_sem.at[0, bucket, c],
            device_id={"blk": nxt},
            device_id_type=MESH,
        )

    def row_hop(bucket, c):
        return pltpu.make_async_remote_copy(
            src_ref=row_send.at[bucket, c, :, pl.ds(0, plan[c][1])],
            dst_ref=row_recv.at[bucket, c, :, pl.ds(0, plan[c][1])],
            send_sem=send_sem.at[1, bucket, c],
            recv_sem=recv_sem.at[1, bucket, c],
            device_id={"blk": nxt},
            device_id_type=MESH,
        )

    def rel_hop(to, slot, step, b):
        r, n = blocks[b]
        return pltpu.make_async_remote_copy(
            src_ref=rel_all.at[slot, pl.ds(r, n)],
            dst_ref=rel_all.at[slot, pl.ds(r, n)],
            send_sem=rsend_sem.at[step - 1, b],
            recv_sem=rrecv_sem.at[slot, b],
            device_id={"rel": to},
            device_id_type=MESH,
        )

    def put_pair(ref, hi, lo, twice):
        width = hi.shape[1]
        if width == LANES:
            ref[0, :, :LANES] = hi
            ref[0, :, LANES:] = lo
            if twice:
                ref[1, :, :LANES] = hi
                ref[1, :, LANES:] = hi
        else:
            ref[0] = hi
            ref[1] = lo

    def fold(wide):
        return wide[:, :LANES] + wide[:, LANES:]

    for copy in load_ids:
        copy.wait()

    for bucket in range(buckets):
        last = bucket + 1 == buckets
        now_src = src_ref if bucket == 0 else out_src
        sid = sid_ref[pl.ds(bucket, 1), :]
        rid = rid_ref[pl.ds(bucket, 1), :]
        rhot[...] = (lax.broadcasted_iota(jnp.int32, (rels, edges), 0) == rid).astype(F32).astype(BF16)
        hot[...] = (lax.broadcasted_iota(jnp.int32, (rows, edges), 0) == sid).astype(F32).astype(BF16)
        if bucket == 0:
            load_rel.wait()
        r_hi, r_lo = split(rel_ref[...])
        relation[...] = nn(r_hi, rhot[...]) + nn(r_lo, rhot[...])
        asked = []
        for b, (r, n) in enumerate(blocks):
            part = pl.ds(r, n)
            if bucket == 0:
                load_src[b].wait()
            s_hi, s_lo = split(now_src[part, :])
            got = nn(s_hi, hot[...]) + nn(s_lo, hot[...])
            picked[part, :] = got
            queries = got * relation[part, :]
            hi, lo = split(queries)
            q_ref[0, part, :] = hi
            q_ref[1, part, :] = lo
            asked.append(queries)
        hi, lo = split(jnp.transpose(jnp.concatenate(asked, axis=0)))
        qt_ref[0] = hi
        qt_ref[1] = lo

        if bucket == 0:
            for copy in load_other:
                copy.wait()
        tid = column(tid_ref[pl.ds(bucket, 1), :])
        nid = column(nid_ref[pl.ds(bucket, 1), :])

        def weigh(c):
            start, width = plan[c]
            cols = pl.ds(start, width)
            lane = lax.broadcasted_iota(jnp.int32, (negs, width), 1) + start
            count = jnp.sum((lane == nid).astype(F32), axis=0, keepdims=True) * (1.0 / negs)
            if bucket == 0:
                table = tgt_ref[:, cols]
            else:
                hop(bucket - 1, c).wait_recv()
                table = recv[c][bucket - 1]
            t_hi, t_lo = split(table)
            put_pair(tables[c], t_hi, t_lo, True)
            if width == LANES:
                score = fold(nn(qt_ref[0], tables[c][0])) + nn(qt_ref[1], t_hi)
            else:
                score = nn(qt_ref[0], t_hi) + nn(qt_ref[0], t_lo) + nn(qt_ref[1], t_hi)
            small = jnp.exp(-jnp.abs(score))
            large = 1.0 / (1.0 + small)
            small = small * large
            up = score >= 0
            sig = jnp.where(up, large, small)
            co = jnp.where(up, small, large)
            lane = lax.broadcasted_iota(jnp.int32, (edges, width), 1) + start
            weight = count * sig - jnp.where(lane == tid, co, 0.0)
            w_hi, w_lo = split(weight)
            put_pair(weights[c], w_hi, w_lo, False)

        def query_part(c, part):
            if plan[c][1] == LANES:
                return (
                    nt(tables[c][1, part, :], weights[c][0])
                    + nt(tables[c][0, part, LANES:], weights[c][0, :, :LANES])
                )
            return (
                nt(tables[c][0, part, :], weights[c][0])
                + nt(tables[c][0, part, :], weights[c][1])
                + nt(tables[c][1, part, :], weights[c][0])
            )

        def finish(c):
            start, width = plan[c]
            cols = pl.ds(start, width)
            if bucket == 0:
                table = tgt_ref[:, cols]
                state = trow_ref[cols].reshape(1, width)
            else:
                row_hop(bucket - 1, c).wait_recv()
                table = recv[c][bucket - 1]
                state = row_recv[bucket - 1, c, :, :width]
            if width == LANES:
                grad = fold(nn(q_ref[0], weights[c][0])) + nn(q_ref[1], weights[c][0, :, :LANES])
            else:
                grad = nn(q_ref[0], weights[c][0]) + nn(q_ref[0], weights[c][1]) + nn(q_ref[1], weights[c][0])
            fresh = state + jnp.sum(grad * grad, axis=0, keepdims=True) * (1.0 / dims)
            new = table - grad * (learn_rate / (jnp.sqrt(fresh) + epsilon))
            if last:
                out_tgt[:, cols] = new
                out_trow[:, cols] = fresh
            else:
                send[c][bucket] = new
                row_send[bucket, c, :, :width] = fresh
                hop(bucket, c).start()
                row_hop(bucket, c).start()

        def relate(part, whole):
            g_hi, g_lo = split(whole * picked[part, :])
            rel_grad = nt(g_hi, rhot[...]) + nt(g_lo, rhot[...])
            if bucket == 0:
                rel_all[my_rel, part, :] = rel_grad
            else:
                rel_all[my_rel, part, :] = rel_all[my_rel, part, :] + rel_grad

        if bucket == 0:
            load_tgt.wait()
            for copy in load_late:
                copy.wait()
            pl.semaphore_wait(barrier, n_rel)
        everything = pl.ds(0, dims)
        if not last:
            for c in range(len(plan)):
                weigh(c)
                finish(c)
            total = query_part(0, everything)
            for c in range(1, len(plan)):
                total += query_part(c, everything)
            gq_ref[...] = total
            relate(everything, total)
        else:
            for c in range(final):
                weigh(c)
                part = query_part(c, everything)
                gq_ref[...] = part if c == 0 else gq_ref[...] + part
                finish(c)
            weigh(final)
            for b, (r, n) in enumerate(blocks):
                part = pl.ds(r, n)
                whole = query_part(final, part)
                if final > 0:
                    whole = gq_ref[part, :] + whole
                gq_ref[part, :] = whole
                relate(part, whole)
                for step in range(1, n_rel):
                    rel_hop(lax.rem(my_rel + step, n_rel), my_rel, step, b).start()
            finish(final)
        g_hi, g_lo = split(gq_ref[...] * relation[...])
        src_grad = nt(g_hi, hot[...]) + nt(g_lo, hot[...])
        now_srow = srow_ref[...].reshape(1, rows) if bucket == 0 else out_srow[...]
        fresh = now_srow + jnp.sum(src_grad * src_grad, axis=0, keepdims=True) * (1.0 / dims)
        out_src[...] = now_src[...] - src_grad * (learn_rate / (jnp.sqrt(fresh) + epsilon))
        out_srow[...] = fresh

    for bucket in range(buckets - 1):
        for c in range(len(plan)):
            hop(bucket, c).wait_send()
            row_hop(bucket, c).wait_send()
    for b, (r, n) in enumerate(blocks):
        part = pl.ds(r, n)
        for step in range(1, n_rel):
            peer = lax.rem(my_rel + n_rel - step, n_rel)
            arrived = rel_hop(peer, peer, step, b)
            arrived.wait_send()
            arrived.wait_recv()
        total = rel_all[0, part, :]
        for step in range(1, n_rel):
            total = total + rel_all[step, part, :]
        new_state = rstate_ref[part, :] + total * total
        out_rstate[part, :] = new_state
        out_rel[part, :] = rel_ref[part, :] - learn_rate * total / (jnp.sqrt(new_state) + epsilon)


def solution(mesh):
    n_blk, n_rel = mesh.shape["blk"], mesh.shape["rel"]

    def per_device(
        source_table, source_state, target_table, target_state, relation_ops, relation_state,
        source_ids, target_ids, relation_ids, negative_ids,
    ):
        dims, rows = source_table.shape
        rels = relation_ops.shape[1]
        buckets, edges = source_ids.shape
        plan = chunk_plan(rows)
        blocks = row_blocks(dims)
        chunks = len(plan)
        vmem = pl.BlockSpec(memory_space=pltpu.VMEM)
        shape = jax.ShapeDtypeStruct
        moves = [pltpu.VMEM((buckets - 1, dims, width), F32) for _, width in plan]
        out = pl.pallas_call(
            functools.partial(kernel, n_blk, n_rel, plan, blocks),
            out_shape=(
                pltpu.VMEM((dims, rows), F32), pltpu.VMEM((1, rows), F32),
                pltpu.VMEM((dims, rows), F32), pltpu.VMEM((1, rows), F32),
                pltpu.VMEM((dims, rels), F32), pltpu.VMEM((dims, rels), F32),
            ),
            in_specs=[pl.BlockSpec(memory_space=pltpu.HBM)] * 10,
            out_specs=(vmem,) * 6,
            scratch_shapes=[
                pltpu.VMEM((dims, rows), F32), pltpu.VMEM((rows,), F32),
                pltpu.VMEM((dims, rows), F32), pltpu.VMEM((rows,), F32),
                pltpu.VMEM((dims, rels), F32), pltpu.VMEM((dims, rels), F32),
                *[pltpu.VMEM(ids.shape, jnp.int32) for ids in (source_ids, relation_ids, target_ids, negative_ids)],
                pltpu.SemaphoreType.DMA((9 + len(blocks),)),
                pltpu.VMEM((rows, edges), BF16),
                pltpu.VMEM((rels, edges), BF16),
                pltpu.VMEM((2, edges, dims), BF16),
                pltpu.VMEM((2, dims, edges), BF16),
                pltpu.VMEM((dims, edges), F32),
                pltpu.VMEM((dims, edges), F32),
                pltpu.VMEM((dims, edges), F32),
                pltpu.VMEM((n_rel, dims, rels), F32),
                pltpu.SemaphoreType.DMA((n_rel, len(blocks))),
                pltpu.SemaphoreType.DMA((n_rel, len(blocks))),
                pltpu.SemaphoreType.DMA((2, buckets - 1, chunks)),
                pltpu.SemaphoreType.DMA((2, buckets - 1, chunks)),
                pltpu.VMEM((buckets - 1, chunks, 1, 256), F32),
                pltpu.VMEM((buckets - 1, chunks, 1, 256), F32),
                *[pltpu.VMEM((2, dims, 256), BF16) for _ in plan],
                *[pltpu.VMEM((2, edges, 256), BF16) for _ in plan],
                *moves,
                *moves,
            ],
            compiler_params=pltpu.CompilerParams(
                collective_id=0, has_side_effects=True, vmem_limit_bytes=40 * 1024 * 1024
            ),
        )(*(
            pltpu.with_memory_space_constraint(x, pltpu.HBM) for x in (
                source_table, source_state, target_table, target_state,
                relation_ops, relation_state, source_ids, relation_ids,
                target_ids, negative_ids,
            )
        ))
        hbm = pl.BlockSpec(memory_space=pl.ANY)
        return pl.pallas_call(
            emit,
            out_shape=(
                shape((dims, rows), F32), shape((rows,), F32),
                shape((dims, rows), F32), shape((rows,), F32),
                shape((dims, rels), F32), shape((dims, rels), F32),
            ),
            in_specs=[vmem] * 6,
            out_specs=(hbm,) * 6,
            scratch_shapes=[pltpu.VMEM((rows,), F32), pltpu.VMEM((rows,), F32), pltpu.SemaphoreType.DMA((6,))],
            compiler_params=pltpu.CompilerParams(vmem_limit_bytes=16 * 1024 * 1024),
        )(*out)

    split_both = ("blk", "rel")
    return jax.shard_map(
        per_device,
        mesh=mesh,
        in_specs=(
            P(None, split_both), P(split_both), P(None, split_both), P(split_both),
            P(None, "blk"), P(None, "blk"),
            P(None, split_both), P(None, split_both), P(None, split_both), P(None, split_both),
        ),
        out_specs=(
            P(None, split_both), P(split_both), P(None, split_both), P(split_both),
            P(None, "blk"), P(None, "blk"),
        ),
        check_vma=False,
    )
```

```python
import functools

import jax
import jax.numpy as jnp
from jax import lax
from jax.experimental import pallas as pl
from jax.experimental.pallas import tpu as pltpu
from jax.sharding import PartitionSpec as P

learn_rate = 0.1
epsilon = 1e-06
LANES = 128
MESH = pl.DeviceIdType.MESH
F32 = jnp.float32
BF16 = jnp.bfloat16


def split(x):
    high = x.astype(BF16)
    return high, (x - high.astype(F32)).astype(BF16)


def nn(a, b):
    return lax.dot_general(a, b, (((1,), (0,)), ((), ())), preferred_element_type=F32)


def nt(a, b):
    return lax.dot_general(a, b, (((1,), (1,)), ((), ())), preferred_element_type=F32)


def column(row):
    wide = jnp.broadcast_to(row.astype(F32), (8, row.shape[1]))
    return jnp.transpose(wide)[:, :1].astype(jnp.int32)


def one_hot(row, height):
    low = lax.rem(row, LANES)
    inner = (lax.broadcasted_iota(jnp.int32, (LANES, row.shape[1]), 0) == low).astype(F32).astype(BF16)
    if height == LANES:
        return inner
    out = []
    for start in range(0, height, LANES):
        here = (row - low == start).astype(F32).astype(BF16)
        out.append(inner * jnp.broadcast_to(here, inner.shape))
    return jnp.concatenate(out, axis=0)


def chunk_plan(rows):
    if rows % 256 == 0 and rows >= 512:
        widths = [LANES] + [256] * (rows // 256 - 1) + [LANES]
    else:
        widths = [LANES] * (rows // LANES)
    return [(sum(widths[:i]), w) for i, w in enumerate(widths)]


def row_blocks(dims):
    first = min(256, dims // 16 * 16)
    half = (dims // 2 + 15) // 16 * 16
    return [(0, first), (first, dims - first)], [(0, half), (half, dims - half)]


def lane_gather(table, index):
    tall = table.shape[0]
    groups = table.shape[1] // LANES
    out = []
    for start in range(0, index.shape[1], LANES):
        one = jnp.broadcast_to(index[:, start:start + LANES], (tall, LANES))
        low = lax.rem(one, LANES)
        got = jnp.take_along_axis(table[:, :LANES], low, axis=1)
        for g in range(1, groups):
            other = jnp.take_along_axis(table[:, g * LANES:(g + 1) * LANES], low, axis=1)
            got = jnp.where(one >= g * LANES, other, got)
        out.append(got)
    return jnp.concatenate(out, axis=1)


def emit(*refs):
    inputs, outputs, (first, second, sem) = refs[:6], refs[6:12], refs[12:]
    copies = []
    for i in (0, 2, 4, 5):
        copies.append(pltpu.make_async_copy(inputs[i], outputs[i], sem.at[i]))
        copies[-1].start()
    for i, line in ((1, first), (3, second)):
        line[...] = inputs[i][0, :]
        copies.append(pltpu.make_async_copy(line, outputs[i], sem.at[i]))
        copies[-1].start()
    for copy in copies:
        copy.wait()


def kernel(n_blk, n_rel, plan, arrivals, blocks, *refs):
    refs = list(refs)

    def take(n):
        out = refs[:n]
        del refs[:n]
        return out

    src_in, srow_in, tgt_in, trow_in, rel_in, rstate_in, sid_in, rid_in, tid_in, nid_in = take(10)
    out_src, out_srow, out_tgt, out_trow, out_rel, out_rstate = take(6)
    src_ref, srow_ref, tgt_ref, trow_ref, rel_ref, rstate_ref, sid_ref, rid_ref, tid_ref, nid_ref = take(10)
    load_sem, hot, rhot, qt_ref, q_ref, picked, relation, gq_ref, counts, rel_all = take(10)
    rsend_sem, rrecv_sem, send_sem, recv_sem, row_send, row_recv = take(6)
    tables, weights = take(len(plan)), take(len(plan))
    send, recv = take(len(plan)), take(len(plan))
    dims, rows = src_ref.shape
    buckets, edges = sid_ref.shape
    negs = nid_ref.shape[1]
    rels = rel_ref.shape[1]
    final = len(plan) - 1
    groups = [(e, min(256, edges - e)) for e in range(0, edges, 256)]
    my_blk = lax.axis_index("blk")
    my_rel = lax.axis_index("rel")
    nxt = lax.rem(my_blk + 1, n_blk)
    prv = lax.rem(my_blk + n_blk - 1, n_blk)

    loads = []

    def load(there, here):
        loads.append(pltpu.make_async_copy(there, here, load_sem.at[len(loads)]))
        loads[-1].start()
        return loads[-1]

    load_ids = [
        load(sid_in, sid_ref), load(rid_in, rid_ref), load(nid_in, nid_ref), load(tid_in, tid_ref)
    ]
    load_rel = load(rel_in, rel_ref)
    load_src = [load(src_in.at[pl.ds(r, n)], src_ref.at[pl.ds(r, n)]) for r, n in arrivals]
    load_tgt = [
        load(tgt_in.at[:, pl.ds(start, width)], tgt_ref.at[:, pl.ds(start, width)])
        for start, width in ((0, plan[0][1]), (plan[0][1], rows - plan[0][1])) if width
    ]
    load_late = [load(trow_in, trow_ref), load(srow_in, srow_ref), load(rstate_in, rstate_ref)]

    barrier = pltpu.get_barrier_semaphore()
    pl.semaphore_signal(barrier, inc=1, device_id={"blk": prv}, device_id_type=MESH)
    for step in range(1, n_rel):
        pl.semaphore_signal(
            barrier, inc=1, device_id={"rel": lax.rem(my_rel + step, n_rel)}, device_id_type=MESH
        )

    def hop(bucket, c):
        return pltpu.make_async_remote_copy(
            src_ref=send[c].at[bucket],
            dst_ref=recv[c].at[bucket],
            send_sem=send_sem.at[0, bucket, c],
            recv_sem=recv_sem.at[0, bucket, c],
            device_id={"blk": nxt},
            device_id_type=MESH,
        )

    def row_hop(bucket, c):
        return pltpu.make_async_remote_copy(
            src_ref=row_send.at[bucket, c, :, pl.ds(0, plan[c][1])],
            dst_ref=row_recv.at[bucket, c, :, pl.ds(0, plan[c][1])],
            send_sem=send_sem.at[1, bucket, c],
            recv_sem=recv_sem.at[1, bucket, c],
            device_id={"blk": nxt},
            device_id_type=MESH,
        )

    def rel_hop(to, slot, step, b):
        r, n = blocks[b]
        return pltpu.make_async_remote_copy(
            src_ref=rel_all.at[slot, pl.ds(r, n)],
            dst_ref=rel_all.at[slot, pl.ds(r, n)],
            send_sem=rsend_sem.at[step - 1, b],
            recv_sem=rrecv_sem.at[slot, b],
            device_id={"rel": to},
            device_id_type=MESH,
        )

    def put_pair(ref, hi, lo, twice, part=slice(None)):
        width = hi.shape[1]
        if width == LANES:
            ref[0, part, :LANES] = hi
            ref[0, part, LANES:] = lo
            if twice:
                ref[1, :, :LANES] = hi
                ref[1, :, LANES:] = hi
        else:
            ref[0, part, :] = hi
            ref[1, part, :] = lo

    def fold(wide):
        return wide[:, :LANES] + wide[:, LANES:]

    for copy in load_ids:
        copy.wait()

    for bucket in range(buckets):
        last = bucket + 1 == buckets
        now_src = src_ref if bucket == 0 else out_src
        sid = sid_ref[pl.ds(bucket, 1), :]
        rid = rid_ref[pl.ds(bucket, 1), :]
        if bucket == 0:
            load_rel.wait()
        hot[...] = one_hot(sid, rows)
        nid = column(nid_ref[pl.ds(bucket, 1), :])
        tid = column(tid_ref[pl.ds(bucket, 1), :])
        for start in range(0, rows, LANES):
            lane = lax.broadcasted_iota(jnp.int32, (negs, LANES), 1) + start
            counts[:, pl.ds(start, LANES)] = jnp.sum(
                (lane == nid).astype(F32), axis=0, keepdims=True
            ) * (0.5 / negs)
        relation[...] = lane_gather(rel_ref[...], rid)
        if bucket == 0:
            for copy in load_src + load_tgt[:1]:
                copy.wait()
        s_hi, s_lo = split(now_src[...])
        for e, m in groups:
            some = pl.ds(e, m)
            picked[:, some] = nn(s_hi, hot[:, some]) + nn(s_lo, hot[:, some])
        for e, m in groups:
            some = pl.ds(e, m)
            queries = picked[:, some] * relation[:, some]
            hi, lo = split(jnp.transpose(queries * 0.5))
            qt_ref[0, some, :] = hi
            qt_ref[1, some, :] = lo
            hi, lo = split(queries)
            q_ref[0, :, some] = hi
            q_ref[1, :, some] = lo
        rhot[...] = one_hot(rid, rels)

        def weigh(c):
            start, width = plan[c]
            cols = pl.ds(start, width)
            table = tgt_ref[:, cols] if bucket == 0 else recv[c][bucket - 1]
            t_hi, t_lo = split(table)
            put_pair(tables[c], t_hi, t_lo, True)
            count = counts[:, cols]
            lane = lax.broadcasted_iota(jnp.int32, (edges // len(groups), width), 1) + start
            for e, m in groups:
                some = pl.ds(e, m)
                if width == LANES:
                    score = fold(nn(qt_ref[0, some, :], tables[c][0])) + nn(qt_ref[1, some, :], t_hi)
                else:
                    score = (
                        nn(qt_ref[0, some, :], t_hi) + nn(qt_ref[0, some, :], t_lo) + nn(qt_ref[1, some, :], t_hi)
                    )
                half = jnp.tanh(score)
                weight = count * half + count - jnp.where(lane == tid[e:e + m], 0.5 - 0.5 * half, 0.0)
                w_hi, w_lo = split(weight)
                put_pair(weights[c], w_hi, w_lo, False, some)

        def query_part(c, part):
            if plan[c][1] == LANES:
                return (
                    nt(tables[c][1, part, :], weights[c][0])
                    + nt(tables[c][0, part, LANES:], weights[c][0, :, :LANES])
                )
            return (
                nt(tables[c][0, part, :], weights[c][0])
                + nt(tables[c][0, part, :], weights[c][1])
                + nt(tables[c][1, part, :], weights[c][0])
            )

        def finish(c):
            start, width = plan[c]
            cols = pl.ds(start, width)
            if bucket == 0:
                table = tgt_ref[:, cols]
                state = trow_ref[cols].reshape(1, width)
            else:
                table = recv[c][bucket - 1]
                state = row_recv[bucket - 1, c, :, :width]
            if width == LANES:
                grad = fold(nn(q_ref[0], weights[c][0])) + nn(q_ref[1], weights[c][0, :, :LANES])
            else:
                grad = nn(q_ref[0], weights[c][0]) + nn(q_ref[0], weights[c][1]) + nn(q_ref[1], weights[c][0])
            fresh = state + jnp.sum(grad * grad, axis=0, keepdims=True) * (1.0 / dims)
            new = table - grad * (learn_rate / (jnp.sqrt(fresh) + epsilon))
            if last:
                out_tgt[:, cols] = new
                out_trow[:, cols] = fresh
            else:
                send[c][bucket] = new
                row_send[bucket, c, :, :width] = fresh

        def relate(part, whole):
            g_hi, g_lo = split(whole * picked[part, :])
            rel_grad = nt(g_hi, rhot[...]) + nt(g_lo, rhot[...])
            if bucket == 0:
                rel_all[my_rel, part, :] = rel_grad
            else:
                rel_all[my_rel, part, :] = rel_all[my_rel, part, :] + rel_grad

        everything = pl.ds(0, dims)

        def arrive(c):
            if bucket > 0:
                hop(bucket - 1, c).wait_recv()
                row_hop(bucket - 1, c).wait_recv()

        def depart(c):
            hop(bucket, c).start()
            row_hop(bucket, c).start()

        if not last:
            arrive(0)
            weigh(0)
            if bucket == 0:
                load_late[0].wait()
            finish(0)
            if bucket == 0:
                pl.semaphore_wait(barrier, n_rel)
            depart(0)
            if bucket == 0:
                for copy in load_tgt[1:] + load_late[1:]:
                    copy.wait()
            if final > 0:
                arrive(1)
                weigh(1)
            for c in range(1, final + 1):
                if c < final:
                    arrive(c + 1)
                finish(c)
                if c < final:
                    weigh(c + 1)
                depart(c)
            total = query_part(0, everything)
            for c in range(1, len(plan)):
                total += query_part(c, everything)
            gq_ref[...] = total
            relate(everything, total)
        else:
            def gather_query(c):
                part = query_part(c, everything)
                gq_ref[...] = part if c == 0 else gq_ref[...] + part

            for c in range(final):
                arrive(c)
                weigh(c)
                if c > 0:
                    gather_query(c - 1)
                    finish(c - 1)
            if final > 0:
                gather_query(final - 1)
                finish(final - 1)
            arrive(final)
            weigh(final)
            for b, (r, n) in enumerate(blocks):
                part = pl.ds(r, n)
                whole = query_part(final, part)
                if final > 0:
                    whole = gq_ref[part, :] + whole
                gq_ref[part, :] = whole
                relate(part, whole)
                for step in range(1, n_rel):
                    rel_hop(lax.rem(my_rel + step, n_rel), my_rel, step, b).start()
            finish(final)
        g_hi, g_lo = split(gq_ref[...] * relation[...])
        src_grad = nt(g_hi, hot[...]) + nt(g_lo, hot[...])
        now_srow = srow_ref[...].reshape(1, rows) if bucket == 0 else out_srow[...]
        fresh = now_srow + jnp.sum(src_grad * src_grad, axis=0, keepdims=True) * (1.0 / dims)
        out_src[...] = now_src[...] - src_grad * (learn_rate / (jnp.sqrt(fresh) + epsilon))
        out_srow[...] = fresh

    for bucket in range(buckets - 1):
        for c in range(len(plan)):
            hop(bucket, c).wait_send()
            row_hop(bucket, c).wait_send()
    for b, (r, n) in enumerate(blocks):
        part = pl.ds(r, n)
        for step in range(1, n_rel):
            peer = lax.rem(my_rel + n_rel - step, n_rel)
            arrived = rel_hop(peer, peer, step, b)
            arrived.wait_send()
            arrived.wait_recv()
        total = rel_all[0, part, :]
        for step in range(1, n_rel):
            total = total + rel_all[step, part, :]
        new_state = rstate_ref[part, :] + total * total
        out_rstate[part, :] = new_state
        out_rel[part, :] = rel_ref[part, :] - learn_rate * total / (jnp.sqrt(new_state) + epsilon)


def solution(mesh):
    n_blk, n_rel = mesh.shape["blk"], mesh.shape["rel"]

    def per_device(
        source_table, source_state, target_table, target_state, relation_ops, relation_state,
        source_ids, target_ids, relation_ids, negative_ids,
    ):
        dims, rows = source_table.shape
        rels = relation_ops.shape[1]
        buckets, edges = source_ids.shape
        plan = chunk_plan(rows)
        arrivals, blocks = row_blocks(dims)
        chunks = len(plan)
        vmem = pl.BlockSpec(memory_space=pltpu.VMEM)
        shape = jax.ShapeDtypeStruct
        moves = [pltpu.VMEM((buckets - 1, dims, width), F32) for _, width in plan]
        out = pl.pallas_call(
            functools.partial(kernel, n_blk, n_rel, plan, arrivals, blocks),
            out_shape=(
                pltpu.VMEM((dims, rows), F32), pltpu.VMEM((1, rows), F32),
                pltpu.VMEM((dims, rows), F32), pltpu.VMEM((1, rows), F32),
                pltpu.VMEM((dims, rels), F32), pltpu.VMEM((dims, rels), F32),
            ),
            in_specs=[pl.BlockSpec(memory_space=pltpu.HBM)] * 10,
            out_specs=(vmem,) * 6,
            scratch_shapes=[
                pltpu.VMEM((dims, rows), F32), pltpu.VMEM((rows,), F32),
                pltpu.VMEM((dims, rows), F32), pltpu.VMEM((rows,), F32),
                pltpu.VMEM((dims, rels), F32), pltpu.VMEM((dims, rels), F32),
                *[pltpu.VMEM(ids.shape, jnp.int32) for ids in (source_ids, relation_ids, target_ids, negative_ids)],
                pltpu.SemaphoreType.DMA((10 + len(arrivals),)),
                pltpu.VMEM((rows, edges), BF16),
                pltpu.VMEM((rels, edges), BF16),
                pltpu.VMEM((2, edges, dims), BF16),
                pltpu.VMEM((2, dims, edges), BF16),
                pltpu.VMEM((dims, edges), F32),
                pltpu.VMEM((dims, edges), F32),
                pltpu.VMEM((dims, edges), F32),
                pltpu.VMEM((1, rows), F32),
                pltpu.VMEM((n_rel, dims, rels), F32),
                pltpu.SemaphoreType.DMA((n_rel, len(blocks))),
                pltpu.SemaphoreType.DMA((n_rel, len(blocks))),
                pltpu.SemaphoreType.DMA((2, buckets - 1, chunks)),
                pltpu.SemaphoreType.DMA((2, buckets - 1, chunks)),
                pltpu.VMEM((buckets - 1, chunks, 1, 256), F32),
                pltpu.VMEM((buckets - 1, chunks, 1, 256), F32),
                *[pltpu.VMEM((2, dims, 256), BF16) for _ in plan],
                *[pltpu.VMEM((2, edges, 256), BF16) for _ in plan],
                *moves,
                *moves,
            ],
            compiler_params=pltpu.CompilerParams(
                collective_id=0, has_side_effects=True, vmem_limit_bytes=40 * 1024 * 1024
            ),
        )(*(
            pltpu.with_memory_space_constraint(x, pltpu.HBM) for x in (
                source_table, source_state, target_table, target_state,
                relation_ops, relation_state, source_ids, relation_ids,
                target_ids, negative_ids,
            )
        ))
        hbm = pl.BlockSpec(memory_space=pl.ANY)
        return pl.pallas_call(
            emit,
            out_shape=(
                shape((dims, rows), F32), shape((rows,), F32),
                shape((dims, rows), F32), shape((rows,), F32),
                shape((dims, rels), F32), shape((dims, rels), F32),
            ),
            in_specs=[vmem] * 6,
            out_specs=(hbm,) * 6,
            scratch_shapes=[pltpu.VMEM((rows,), F32), pltpu.VMEM((rows,), F32), pltpu.SemaphoreType.DMA((6,))],
            compiler_params=pltpu.CompilerParams(vmem_limit_bytes=16 * 1024 * 1024),
        )(*out)

    split_both = ("blk", "rel")
    return jax.shard_map(
        per_device,
        mesh=mesh,
        in_specs=(
            P(None, split_both), P(split_both), P(None, split_both), P(split_both),
            P(None, "blk"), P(None, "blk"),
            P(None, split_both), P(None, split_both), P(None, split_both), P(None, split_both),
        ),
        out_specs=(
            P(None, split_both), P(split_both), P(None, split_both), P(split_both),
            P(None, "blk"), P(None, "blk"),
        ),
        check_vma=False,
    )
```

```python
import functools

import jax
import jax.numpy as jnp
from jax import lax
from jax.experimental import pallas as pl
from jax.experimental.pallas import tpu as pltpu
from jax.sharding import PartitionSpec as P

learn_rate = 0.1
epsilon = 1e-06
LANES = 128
MESH = pl.DeviceIdType.MESH
F32 = jnp.float32
BF16 = jnp.bfloat16


def split(x):
    high = x.astype(BF16)
    return high, (x - high.astype(F32)).astype(BF16)


def nn(a, b):
    return lax.dot_general(a, b, (((1,), (0,)), ((), ())), preferred_element_type=F32)


def nt(a, b):
    return lax.dot_general(a, b, (((1,), (1,)), ((), ())), preferred_element_type=F32)


def column(row):
    wide = jnp.broadcast_to(row.astype(F32), (8, row.shape[1]))
    return jnp.transpose(wide)[:, :1].astype(jnp.int32)


def one_hot(row, height):
    low = lax.rem(row, LANES)
    inner = (lax.broadcasted_iota(jnp.int32, (LANES, row.shape[1]), 0) == low).astype(F32).astype(BF16)
    if height == LANES:
        return inner
    out = []
    for start in range(0, height, LANES):
        here = (row - low == start).astype(F32).astype(BF16)
        out.append(inner * jnp.broadcast_to(here, inner.shape))
    return jnp.concatenate(out, axis=0)


def chunk_plan(rows):
    if rows % 256 == 0 and rows >= 512:
        widths = [LANES] + [256] * (rows // 256 - 1) + [LANES]
    else:
        widths = [LANES] * (rows // LANES)
    return [(sum(widths[:i]), w) for i, w in enumerate(widths)]


def piece_plan(plan, dims, n_blk):
    half, quarter = (dims // 2 + 15) // 16 * 16, (dims // 4 + 15) // 16 * 16
    relays = n_blk >= 16 and len(plan) > 2
    pieces = []
    for c in range(len(plan)):
        if relays and c == 0:
            pieces += [(c, 0, half, n_blk - 4), (c, half, dims - half, n_blk - 8)]
        elif relays and c == 1:
            pieces += [(c, 0, quarter, n_blk - 12), (c, quarter, dims - quarter, None)]
        else:
            pieces += [(c, 0, dims, None)]
    return pieces


def row_blocks(dims):
    first = min(256, dims // 16 * 16)
    half = (dims // 2 + 15) // 16 * 16
    return [(0, first), (first, dims - first)], [(0, half), (half, dims - half)]


def lane_gather(table, index):
    tall = table.shape[0]
    groups = table.shape[1] // LANES
    out = []
    for start in range(0, index.shape[1], LANES):
        one = jnp.broadcast_to(index[:, start:start + LANES], (tall, LANES))
        low = lax.rem(one, LANES)
        got = jnp.take_along_axis(table[:, :LANES], low, axis=1)
        for g in range(1, groups):
            other = jnp.take_along_axis(table[:, g * LANES:(g + 1) * LANES], low, axis=1)
            got = jnp.where(one >= g * LANES, other, got)
        out.append(got)
    return jnp.concatenate(out, axis=1)


def emit(*refs):
    inputs, outputs, (first, second, sem) = refs[:6], refs[6:12], refs[12:]
    copies = []
    for i in (0, 2, 4, 5):
        copies.append(pltpu.make_async_copy(inputs[i], outputs[i], sem.at[i]))
        copies[-1].start()
    for i, line in ((1, first), (3, second)):
        line[...] = inputs[i][0, :]
        copies.append(pltpu.make_async_copy(line, outputs[i], sem.at[i]))
        copies[-1].start()
    for copy in copies:
        copy.wait()


def kernel(n_blk, n_rel, plan, pieces, arrivals, blocks, *refs):
    refs = list(refs)

    def take(n):
        out = refs[:n]
        del refs[:n]
        return out

    src_in, srow_in, tgt_in, trow_in, rel_in, rstate_in, sid_in, rid_in, tid_in, nid_in = take(10)
    out_src, out_srow, out_tgt, out_trow, out_rel, out_rstate = take(6)
    src_ref, srow_ref, tgt_ref, trow_ref, rel_ref, rstate_ref, sid_ref, rid_ref, tid_ref, nid_ref = take(10)
    load_sem, hot, rhot, qt_ref, q_ref, picked, relation, gq_ref, counts, rel_all = take(10)
    rsend_sem, rrecv_sem, send_sem, recv_sem, row_send, row_recv = take(6)
    tables, weights = take(len(plan)), take(len(plan))
    send, recv = take(len(plan)), take(len(plan))
    relayed = [p for p, piece in enumerate(pieces) if piece[3] is not None]
    relay_refs = dict(zip(relayed, take(len(relayed))))
    relay_recv, relay_send, row_send_sem, row_recv_sem = take(4)
    dims, rows = src_ref.shape
    buckets, edges = sid_ref.shape
    negs = nid_ref.shape[1]
    rels = rel_ref.shape[1]
    final = len(plan) - 1
    groups = [(e, min(256, edges - e)) for e in range(0, edges, 256)]
    my_blk = lax.axis_index("blk")
    my_rel = lax.axis_index("rel")
    nxt = lax.rem(my_blk + 1, n_blk)
    prv = lax.rem(my_blk + n_blk - 1, n_blk)

    loads = []

    def load(there, here):
        loads.append(pltpu.make_async_copy(there, here, load_sem.at[len(loads)]))
        loads[-1].start()
        return loads[-1]

    load_ids = [
        load(sid_in, sid_ref), load(rid_in, rid_ref), load(nid_in, nid_ref), load(tid_in, tid_ref)
    ]
    load_rel = load(rel_in, rel_ref)
    load_src = [load(src_in.at[pl.ds(r, n)], src_ref.at[pl.ds(r, n)]) for r, n in arrivals]
    load_tgt = [
        load(tgt_in.at[:, pl.ds(start, width)], tgt_ref.at[:, pl.ds(start, width)])
        for start, width in ((0, plan[0][1]), (plan[0][1], rows - plan[0][1])) if width
    ]
    load_late = [load(trow_in, trow_ref), load(srow_in, srow_ref), load(rstate_in, rstate_ref)]

    barrier = pltpu.get_barrier_semaphore()
    pl.semaphore_signal(barrier, inc=1, device_id={"blk": prv}, device_id_type=MESH)
    for step in range(1, n_rel):
        pl.semaphore_signal(
            barrier, inc=1, device_id={"rel": lax.rem(my_rel + step, n_rel)}, device_id_type=MESH
        )

    for p in relayed:
        at = pieces[p][3]

        @pl.when(my_blk == 0)
        def _():
            pl.semaphore_signal(barrier, inc=1, device_id={"blk": jnp.int32(at)}, device_id_type=MESH)

        @pl.when(my_blk == at)
        def _():
            pl.semaphore_signal(barrier, inc=1, device_id={"blk": n_blk - 1}, device_id_type=MESH)

    def enter():
        expected = jnp.int32(n_rel)
        for p in relayed:
            expected += (my_blk == n_blk - 1).astype(jnp.int32) + (my_blk == pieces[p][3]).astype(jnp.int32)
        pl.semaphore_wait(barrier, expected)

    def hop(bucket, p):
        c, r, n, _ = pieces[p]
        return pltpu.make_async_remote_copy(
            src_ref=send[c].at[bucket, pl.ds(r, n)],
            dst_ref=recv[c].at[bucket, pl.ds(r, n)],
            send_sem=send_sem.at[bucket, p],
            recv_sem=recv_sem.at[bucket, p],
            device_id={"blk": nxt},
            device_id_type=MESH,
        )

    def to_relay(bucket, p):
        c, r, n, at = pieces[p]
        return pltpu.make_async_remote_copy(
            src_ref=send[c].at[bucket, pl.ds(r, n)],
            dst_ref=relay_refs[p].at[bucket],
            send_sem=send_sem.at[bucket, p],
            recv_sem=relay_recv.at[bucket, p],
            device_id={"blk": jnp.int32(at)},
            device_id_type=MESH,
        )

    def from_relay(bucket, p):
        c, r, n, _ = pieces[p]
        return pltpu.make_async_remote_copy(
            src_ref=relay_refs[p].at[bucket],
            dst_ref=recv[c].at[bucket, pl.ds(r, n)],
            send_sem=relay_send.at[bucket, p],
            recv_sem=recv_sem.at[bucket, p],
            device_id={"blk": jnp.int32(0)},
            device_id_type=MESH,
        )

    def relay(bucket, p):
        @pl.when(my_blk == pieces[p][3])
        def _():
            to_relay(bucket, p).wait_recv()
            from_relay(bucket, p).start()

    def row_hop(bucket, c):
        return pltpu.make_async_remote_copy(
            src_ref=row_send.at[bucket, c, :, pl.ds(0, plan[c][1])],
            dst_ref=row_recv.at[bucket, c, :, pl.ds(0, plan[c][1])],
            send_sem=row_send_sem.at[bucket, c],
            recv_sem=row_recv_sem.at[bucket, c],
            device_id={"blk": nxt},
            device_id_type=MESH,
        )

    def rel_hop(to, slot, step, b):
        r, n = blocks[b]
        return pltpu.make_async_remote_copy(
            src_ref=rel_all.at[slot, pl.ds(r, n)],
            dst_ref=rel_all.at[slot, pl.ds(r, n)],
            send_sem=rsend_sem.at[step - 1, b],
            recv_sem=rrecv_sem.at[slot, b],
            device_id={"rel": to},
            device_id_type=MESH,
        )

    def put_pair(ref, hi, lo, twice, part=slice(None)):
        width = hi.shape[1]
        if width == LANES:
            ref[0, part, :LANES] = hi
            ref[0, part, LANES:] = lo
            if twice:
                ref[1, :, :LANES] = hi
                ref[1, :, LANES:] = hi
        else:
            ref[0, part, :] = hi
            ref[1, part, :] = lo

    def fold(wide):
        return wide[:, :LANES] + wide[:, LANES:]

    for copy in load_ids:
        copy.wait()

    for bucket in range(buckets):
        last = bucket + 1 == buckets
        now_src = src_ref if bucket == 0 else out_src
        sid = sid_ref[pl.ds(bucket, 1), :]
        rid = rid_ref[pl.ds(bucket, 1), :]
        if bucket == 0:
            load_rel.wait()
        hot[...] = one_hot(sid, rows)
        nid = column(nid_ref[pl.ds(bucket, 1), :])
        tid = column(tid_ref[pl.ds(bucket, 1), :])
        for start in range(0, rows, LANES):
            lane = lax.broadcasted_iota(jnp.int32, (negs, LANES), 1) + start
            counts[:, pl.ds(start, LANES)] = jnp.sum(
                (lane == nid).astype(F32), axis=0, keepdims=True
            ) * (0.5 / negs)
        relation[...] = lane_gather(rel_ref[...], rid)
        if bucket == 0:
            for copy in load_src + load_tgt[:1]:
                copy.wait()
        s_hi, s_lo = split(now_src[...])
        for e, m in groups:
            some = pl.ds(e, m)
            picked[:, some] = nn(s_hi, hot[:, some]) + nn(s_lo, hot[:, some])
        for e, m in groups:
            some = pl.ds(e, m)
            queries = picked[:, some] * relation[:, some]
            hi, lo = split(jnp.transpose(queries * 0.5))
            qt_ref[0, some, :] = hi
            qt_ref[1, some, :] = lo
            hi, lo = split(queries)
            q_ref[0, :, some] = hi
            q_ref[1, :, some] = lo
        rhot[...] = one_hot(rid, rels)

        def weigh(c):
            start, width = plan[c]
            cols = pl.ds(start, width)
            table = tgt_ref[:, cols] if bucket == 0 else recv[c][bucket - 1]
            t_hi, t_lo = split(table)
            put_pair(tables[c], t_hi, t_lo, True)
            count = counts[:, cols]
            lane = lax.broadcasted_iota(jnp.int32, (edges // len(groups), width), 1) + start
            for e, m in groups:
                some = pl.ds(e, m)
                if width == LANES:
                    score = fold(nn(qt_ref[0, some, :], tables[c][0])) + nn(qt_ref[1, some, :], t_hi)
                else:
                    score = (
                        nn(qt_ref[0, some, :], t_hi) + nn(qt_ref[0, some, :], t_lo) + nn(qt_ref[1, some, :], t_hi)
                    )
                half = jnp.tanh(score)
                weight = count * half + count - jnp.where(lane == tid[e:e + m], 0.5 - 0.5 * half, 0.0)
                w_hi, w_lo = split(weight)
                put_pair(weights[c], w_hi, w_lo, False, some)

        def query_part(c, part):
            if plan[c][1] == LANES:
                return (
                    nt(tables[c][1, part, :], weights[c][0])
                    + nt(tables[c][0, part, LANES:], weights[c][0, :, :LANES])
                )
            return (
                nt(tables[c][0, part, :], weights[c][0])
                + nt(tables[c][0, part, :], weights[c][1])
                + nt(tables[c][1, part, :], weights[c][0])
            )

        def finish(c):
            start, width = plan[c]
            cols = pl.ds(start, width)
            if bucket == 0:
                table = tgt_ref[:, cols]
                state = trow_ref[cols].reshape(1, width)
            else:
                table = recv[c][bucket - 1]
                state = row_recv[bucket - 1, c, :, :width]
            if width == LANES:
                grad = fold(nn(q_ref[0], weights[c][0])) + nn(q_ref[1], weights[c][0, :, :LANES])
            else:
                grad = nn(q_ref[0], weights[c][0]) + nn(q_ref[0], weights[c][1]) + nn(q_ref[1], weights[c][0])
            fresh = state + jnp.sum(grad * grad, axis=0, keepdims=True) * (1.0 / dims)
            new = table - grad * (learn_rate / (jnp.sqrt(fresh) + epsilon))
            if last:
                out_tgt[:, cols] = new
                out_trow[:, cols] = fresh
            else:
                send[c][bucket] = new
                row_send[bucket, c, :, :width] = fresh

        def relate(part, whole):
            g_hi, g_lo = split(whole * picked[part, :])
            rel_grad = nt(g_hi, rhot[...]) + nt(g_lo, rhot[...])
            if bucket == 0:
                rel_all[my_rel, part, :] = rel_grad
            else:
                rel_all[my_rel, part, :] = rel_all[my_rel, part, :] + rel_grad

        everything = pl.ds(0, dims)

        def arrive(c):
            if bucket > 0:
                for p, piece in enumerate(pieces):
                    if piece[0] == c:
                        hop(bucket - 1, p).wait_recv()
                row_hop(bucket - 1, c).wait_recv()

        def depart(c):
            for p, piece in enumerate(pieces):
                if piece[0] != c:
                    continue
                if p in relayed:
                    @pl.when(my_blk == n_blk - 1)
                    def _():
                        to_relay(bucket, p).start()

                    @pl.when(my_blk != n_blk - 1)
                    def _():
                        hop(bucket, p).start()
                else:
                    hop(bucket, p).start()
            row_hop(bucket, c).start()

        if not last:
            arrive(0)
            weigh(0)
            if bucket == 0:
                load_late[0].wait()
            finish(0)
            if bucket == 0:
                enter()
            depart(0)
            if bucket == 0:
                for copy in load_tgt[1:] + load_late[1:]:
                    copy.wait()
            if final > 0:
                arrive(1)
                weigh(1)
            for c in range(1, final + 1):
                if c < final:
                    arrive(c + 1)
                finish(c)
                if c < final:
                    weigh(c + 1)
                depart(c)
            for p in relayed:
                if pieces[p][0] == 0:
                    relay(bucket, p)
            total = query_part(0, everything)
            for c in range(1, len(plan)):
                total += query_part(c, everything)
            gq_ref[...] = total
            relate(everything, total)
        else:
            def gather_query(c):
                part = query_part(c, everything)
                gq_ref[...] = part if c == 0 else gq_ref[...] + part

            for c in range(final):
                arrive(c)
                weigh(c)
                if c > 0:
                    gather_query(c - 1)
                    finish(c - 1)
            if final > 0:
                gather_query(final - 1)
                finish(final - 1)
            arrive(final)
            weigh(final)
            for b, (r, n) in enumerate(blocks):
                part = pl.ds(r, n)
                whole = query_part(final, part)
                if final > 0:
                    whole = gq_ref[part, :] + whole
                gq_ref[part, :] = whole
                relate(part, whole)
                for step in range(1, n_rel):
                    rel_hop(lax.rem(my_rel + step, n_rel), my_rel, step, b).start()
            finish(final)
        g_hi, g_lo = split(gq_ref[...] * relation[...])
        src_grad = nt(g_hi, hot[...]) + nt(g_lo, hot[...])
        now_srow = srow_ref[...].reshape(1, rows) if bucket == 0 else out_srow[...]
        fresh = now_srow + jnp.sum(src_grad * src_grad, axis=0, keepdims=True) * (1.0 / dims)
        out_src[...] = now_src[...] - src_grad * (learn_rate / (jnp.sqrt(fresh) + epsilon))
        out_srow[...] = fresh
        if not last:
            for p in relayed:
                if pieces[p][0] > 0:
                    relay(bucket, p)

    for bucket in range(buckets - 1):
        for p in range(len(pieces)):
            hop(bucket, p).wait_send()
        for p in relayed:
            @pl.when(my_blk == pieces[p][3])
            def _():
                from_relay(bucket, p).wait_send()
        for c in range(len(plan)):
            row_hop(bucket, c).wait_send()
    for b, (r, n) in enumerate(blocks):
        part = pl.ds(r, n)
        for step in range(1, n_rel):
            peer = lax.rem(my_rel + n_rel - step, n_rel)
            arrived = rel_hop(peer, peer, step, b)
            arrived.wait_send()
            arrived.wait_recv()
        total = rel_all[0, part, :]
        for step in range(1, n_rel):
            total = total + rel_all[step, part, :]
        new_state = rstate_ref[part, :] + total * total
        out_rstate[part, :] = new_state
        out_rel[part, :] = rel_ref[part, :] - learn_rate * total / (jnp.sqrt(new_state) + epsilon)


def solution(mesh):
    n_blk, n_rel = mesh.shape["blk"], mesh.shape["rel"]

    def per_device(
        source_table, source_state, target_table, target_state, relation_ops, relation_state,
        source_ids, target_ids, relation_ids, negative_ids,
    ):
        dims, rows = source_table.shape
        rels = relation_ops.shape[1]
        buckets, edges = source_ids.shape
        plan = chunk_plan(rows)
        arrivals, blocks = row_blocks(dims)
        pieces = piece_plan(plan, dims, n_blk)
        chunks = len(plan)
        vmem = pl.BlockSpec(memory_space=pltpu.VMEM)
        shape = jax.ShapeDtypeStruct
        moves = [pltpu.VMEM((buckets - 1, dims, width), F32) for _, width in plan]
        out = pl.pallas_call(
            functools.partial(kernel, n_blk, n_rel, plan, pieces, arrivals, blocks),
            out_shape=(
                pltpu.VMEM((dims, rows), F32), pltpu.VMEM((1, rows), F32),
                pltpu.VMEM((dims, rows), F32), pltpu.VMEM((1, rows), F32),
                pltpu.VMEM((dims, rels), F32), pltpu.VMEM((dims, rels), F32),
            ),
            in_specs=[pl.BlockSpec(memory_space=pltpu.HBM)] * 10,
            out_specs=(vmem,) * 6,
            scratch_shapes=[
                pltpu.VMEM((dims, rows), F32), pltpu.VMEM((rows,), F32),
                pltpu.VMEM((dims, rows), F32), pltpu.VMEM((rows,), F32),
                pltpu.VMEM((dims, rels), F32), pltpu.VMEM((dims, rels), F32),
                *[pltpu.VMEM(ids.shape, jnp.int32) for ids in (source_ids, relation_ids, target_ids, negative_ids)],
                pltpu.SemaphoreType.DMA((10 + len(arrivals),)),
                pltpu.VMEM((rows, edges), BF16),
                pltpu.VMEM((rels, edges), BF16),
                pltpu.VMEM((2, edges, dims), BF16),
                pltpu.VMEM((2, dims, edges), BF16),
                pltpu.VMEM((dims, edges), F32),
                pltpu.VMEM((dims, edges), F32),
                pltpu.VMEM((dims, edges), F32),
                pltpu.VMEM((1, rows), F32),
                pltpu.VMEM((n_rel, dims, rels), F32),
                pltpu.SemaphoreType.DMA((n_rel, len(blocks))),
                pltpu.SemaphoreType.DMA((n_rel, len(blocks))),
                pltpu.SemaphoreType.DMA((buckets - 1, len(pieces))),
                pltpu.SemaphoreType.DMA((buckets - 1, len(pieces))),
                pltpu.VMEM((buckets - 1, chunks, 1, 256), F32),
                pltpu.VMEM((buckets - 1, chunks, 1, 256), F32),
                *[pltpu.VMEM((2, dims, 256), BF16) for _ in plan],
                *[pltpu.VMEM((2, edges, 256), BF16) for _ in plan],
                *moves,
                *moves,
                *[
                    pltpu.VMEM((buckets - 1, n, plan[c][1]), F32)
                    for c, _, n, at in pieces if at is not None
                ],
                pltpu.SemaphoreType.DMA((buckets - 1, len(pieces))),
                pltpu.SemaphoreType.DMA((buckets - 1, len(pieces))),
                pltpu.SemaphoreType.DMA((buckets - 1, chunks)),
                pltpu.SemaphoreType.DMA((buckets - 1, chunks)),
            ],
            compiler_params=pltpu.CompilerParams(
                collective_id=0, has_side_effects=True, vmem_limit_bytes=40 * 1024 * 1024
            ),
        )(*(
            pltpu.with_memory_space_constraint(x, pltpu.HBM) for x in (
                source_table, source_state, target_table, target_state,
                relation_ops, relation_state, source_ids, relation_ids,
                target_ids, negative_ids,
            )
        ))
        hbm = pl.BlockSpec(memory_space=pl.ANY)
        return pl.pallas_call(
            emit,
            out_shape=(
                shape((dims, rows), F32), shape((rows,), F32),
                shape((dims, rows), F32), shape((rows,), F32),
                shape((dims, rels), F32), shape((dims, rels), F32),
            ),
            in_specs=[vmem] * 6,
            out_specs=(hbm,) * 6,
            scratch_shapes=[pltpu.VMEM((rows,), F32), pltpu.VMEM((rows,), F32), pltpu.SemaphoreType.DMA((6,))],
            compiler_params=pltpu.CompilerParams(vmem_limit_bytes=16 * 1024 * 1024),
        )(*out)

    split_both = ("blk", "rel")
    return jax.shard_map(
        per_device,
        mesh=mesh,
        in_specs=(
            P(None, split_both), P(split_both), P(None, split_both), P(split_both),
            P(None, "blk"), P(None, "blk"),
            P(None, split_both), P(None, split_both), P(None, split_both), P(None, split_both),
        ),
        out_specs=(
            P(None, split_both), P(split_both), P(None, split_both), P(split_both),
            P(None, "blk"), P(None, "blk"),
        ),
        check_vma=False,
    )
```

```python
import functools

import jax
import jax.numpy as jnp
from jax import lax
from jax.experimental import pallas as pl
from jax.experimental.pallas import tpu as pltpu
from jax.sharding import PartitionSpec as P

learn_rate = 0.1
epsilon = 1e-06
LANES = 128
MESH = pl.DeviceIdType.MESH
F32 = jnp.float32
BF16 = jnp.bfloat16


def split(x):
    high = x.astype(BF16)
    return high, (x - high.astype(F32)).astype(BF16)


def nn(a, b):
    return lax.dot_general(a, b, (((1,), (0,)), ((), ())), preferred_element_type=F32)


def nt(a, b):
    return lax.dot_general(a, b, (((1,), (1,)), ((), ())), preferred_element_type=F32)


def column(row):
    wide = jnp.broadcast_to(row.astype(F32), (8, row.shape[1]))
    return jnp.transpose(wide)[:, :1].astype(jnp.int32)


def one_hot(row, height):
    low = lax.rem(row, LANES)
    inner = (lax.broadcasted_iota(jnp.int32, (LANES, row.shape[1]), 0) == low).astype(F32).astype(BF16)
    if height == LANES:
        return inner
    out = []
    for start in range(0, height, LANES):
        here = (row - low == start).astype(F32).astype(BF16)
        out.append(inner * jnp.broadcast_to(here, inner.shape))
    return jnp.concatenate(out, axis=0)


def chunk_plan(rows):
    if rows % 256 == 0 and rows >= 512:
        widths = [LANES] + [256] * (rows // 256 - 1) + [LANES]
    else:
        widths = [LANES] * (rows // LANES)
    return [(sum(widths[:i]), w) for i, w in enumerate(widths)]


def piece_plan(plan, dims, n_blk):
    half, eighth = (dims // 2 + 15) // 16 * 16, dims // 128 * 16
    relays = n_blk >= 16 and len(plan) > 2
    pieces = []
    for c in range(len(plan)):
        if relays and c == 0:
            pieces += [(c, 0, half, n_blk - 8), (c, half, dims - half, n_blk - 12)]
        elif relays and c == 1:
            pieces += [
                (c, 0, eighth, n_blk - 8), (c, eighth, eighth, n_blk - 12), (c, 2 * eighth, dims - 2 * eighth, None)
            ]
        else:
            pieces += [(c, 0, dims, None)]
    return pieces


def row_blocks(dims):
    first = min(256, dims // 16 * 16)
    half = (dims // 2 + 15) // 16 * 16
    return [(0, first), (first, dims - first)], [(0, half), (half, dims - half)]


def lane_gather(table, index):
    tall = table.shape[0]
    groups = table.shape[1] // LANES
    out = []
    for start in range(0, index.shape[1], LANES):
        one = jnp.broadcast_to(index[:, start:start + LANES], (tall, LANES))
        low = lax.rem(one, LANES)
        got = jnp.take_along_axis(table[:, :LANES], low, axis=1)
        for g in range(1, groups):
            other = jnp.take_along_axis(table[:, g * LANES:(g + 1) * LANES], low, axis=1)
            got = jnp.where(one >= g * LANES, other, got)
        out.append(got)
    return jnp.concatenate(out, axis=1)


def emit(*refs):
    inputs, outputs, (first, second, sem) = refs[:6], refs[6:12], refs[12:]
    copies = []
    for i in (0, 2, 4, 5):
        copies.append(pltpu.make_async_copy(inputs[i], outputs[i], sem.at[i]))
        copies[-1].start()
    for i, line in ((1, first), (3, second)):
        line[...] = inputs[i][0, :]
        copies.append(pltpu.make_async_copy(line, outputs[i], sem.at[i]))
        copies[-1].start()
    for copy in copies:
        copy.wait()


def kernel(n_blk, n_rel, plan, pieces, arrivals, blocks, *refs):
    refs = list(refs)

    def take(n):
        out = refs[:n]
        del refs[:n]
        return out

    src_in, srow_in, tgt_in, trow_in, rel_in, rstate_in, sid_in, rid_in, tid_in, nid_in = take(10)
    out_src, out_srow, out_tgt, out_trow, out_rel, out_rstate = take(6)
    src_ref, srow_ref, tgt_ref, trow_ref, rel_ref, rstate_ref, sid_ref, rid_ref, tid_ref, nid_ref = take(10)
    load_sem, hot, rhot, qt_ref, q_ref, picked, relation, gq_ref, counts, rel_all = take(10)
    rsend_sem, rrecv_sem, send_sem, recv_sem, row_send, row_recv = take(6)
    tables, weights = take(len(plan)), take(len(plan))
    send, recv = take(len(plan)), take(len(plan))
    relayed = [p for p, piece in enumerate(pieces) if piece[3] is not None]
    helpers = sorted({pieces[p][3] for p in relayed})
    relay_refs = dict(zip(relayed, take(len(relayed))))
    relay_recv, relay_send, row_send_sem, row_recv_sem = take(4)
    dims, rows = src_ref.shape
    buckets, edges = sid_ref.shape
    negs = nid_ref.shape[1]
    rels = rel_ref.shape[1]
    final = len(plan) - 1
    groups = [(e, min(256, edges - e)) for e in range(0, edges, 256)]
    my_blk = lax.axis_index("blk")
    my_rel = lax.axis_index("rel")
    nxt = lax.rem(my_blk + 1, n_blk)
    prv = lax.rem(my_blk + n_blk - 1, n_blk)

    loads = []

    def load(there, here):
        loads.append(pltpu.make_async_copy(there, here, load_sem.at[len(loads)]))
        loads[-1].start()
        return loads[-1]

    load_ids = [
        load(sid_in, sid_ref), load(rid_in, rid_ref), load(nid_in, nid_ref), load(tid_in, tid_ref)
    ]
    load_rel = load(rel_in, rel_ref)
    load_src = [load(src_in.at[pl.ds(r, n)], src_ref.at[pl.ds(r, n)]) for r, n in arrivals]
    load_tgt = [
        load(tgt_in.at[:, pl.ds(start, width)], tgt_ref.at[:, pl.ds(start, width)])
        for start, width in ((0, plan[0][1]), (plan[0][1], rows - plan[0][1])) if width
    ]
    load_late = [load(trow_in, trow_ref), load(srow_in, srow_ref), load(rstate_in, rstate_ref)]

    barrier = pltpu.get_barrier_semaphore()
    pl.semaphore_signal(barrier, inc=1, device_id={"blk": prv}, device_id_type=MESH)
    for step in range(1, n_rel):
        pl.semaphore_signal(
            barrier, inc=1, device_id={"rel": lax.rem(my_rel + step, n_rel)}, device_id_type=MESH
        )

    for at in helpers:
        @pl.when(my_blk == 0)
        def _():
            pl.semaphore_signal(barrier, inc=1, device_id={"blk": jnp.int32(at)}, device_id_type=MESH)

        @pl.when(my_blk == at)
        def _():
            pl.semaphore_signal(barrier, inc=1, device_id={"blk": n_blk - 1}, device_id_type=MESH)

    def enter():
        expected = jnp.int32(n_rel)
        for at in helpers:
            expected += (my_blk == n_blk - 1).astype(jnp.int32) + (my_blk == at).astype(jnp.int32)
        pl.semaphore_wait(barrier, expected)

    def hop(bucket, p):
        c, r, n, _ = pieces[p]
        return pltpu.make_async_remote_copy(
            src_ref=send[c].at[bucket, pl.ds(r, n)],
            dst_ref=recv[c].at[bucket, pl.ds(r, n)],
            send_sem=send_sem.at[bucket, p],
            recv_sem=recv_sem.at[bucket, p],
            device_id={"blk": nxt},
            device_id_type=MESH,
        )

    def to_relay(bucket, p):
        c, r, n, at = pieces[p]
        return pltpu.make_async_remote_copy(
            src_ref=send[c].at[bucket, pl.ds(r, n)],
            dst_ref=relay_refs[p].at[bucket],
            send_sem=send_sem.at[bucket, p],
            recv_sem=relay_recv.at[bucket, p],
            device_id={"blk": jnp.int32(at)},
            device_id_type=MESH,
        )

    def from_relay(bucket, p):
        c, r, n, _ = pieces[p]
        return pltpu.make_async_remote_copy(
            src_ref=relay_refs[p].at[bucket],
            dst_ref=recv[c].at[bucket, pl.ds(r, n)],
            send_sem=relay_send.at[bucket, p],
            recv_sem=recv_sem.at[bucket, p],
            device_id={"blk": jnp.int32(0)},
            device_id_type=MESH,
        )

    def relay(bucket, p):
        @pl.when(my_blk == pieces[p][3])
        def _():
            to_relay(bucket, p).wait_recv()
            from_relay(bucket, p).start()

    def row_hop(bucket, c):
        return pltpu.make_async_remote_copy(
            src_ref=row_send.at[bucket, c, :, pl.ds(0, plan[c][1])],
            dst_ref=row_recv.at[bucket, c, :, pl.ds(0, plan[c][1])],
            send_sem=row_send_sem.at[bucket, c],
            recv_sem=row_recv_sem.at[bucket, c],
            device_id={"blk": nxt},
            device_id_type=MESH,
        )

    def rel_hop(to, slot, step, b):
        r, n = blocks[b]
        return pltpu.make_async_remote_copy(
            src_ref=rel_all.at[slot, pl.ds(r, n)],
            dst_ref=rel_all.at[slot, pl.ds(r, n)],
            send_sem=rsend_sem.at[step - 1, b],
            recv_sem=rrecv_sem.at[slot, b],
            device_id={"rel": to},
            device_id_type=MESH,
        )

    def put_pair(ref, hi, lo, twice, part=slice(None)):
        width = hi.shape[1]
        if width == LANES:
            ref[0, part, :LANES] = hi
            ref[0, part, LANES:] = lo
            if twice:
                ref[1, :, :LANES] = hi
                ref[1, :, LANES:] = hi
        else:
            ref[0, part, :] = hi
            ref[1, part, :] = lo

    def fold(wide):
        return wide[:, :LANES] + wide[:, LANES:]

    for copy in load_ids:
        copy.wait()

    for bucket in range(buckets):
        last = bucket + 1 == buckets
        now_src = src_ref if bucket == 0 else out_src
        sid = sid_ref[pl.ds(bucket, 1), :]
        rid = rid_ref[pl.ds(bucket, 1), :]
        if bucket == 0:
            load_rel.wait()
        hot[...] = one_hot(sid, rows)
        nid = column(nid_ref[pl.ds(bucket, 1), :])
        tid = column(tid_ref[pl.ds(bucket, 1), :])
        for start in range(0, rows, LANES):
            lane = lax.broadcasted_iota(jnp.int32, (negs, LANES), 1) + start
            counts[:, pl.ds(start, LANES)] = jnp.sum(
                (lane == nid).astype(F32), axis=0, keepdims=True
            ) * (0.5 / negs)
        relation[...] = lane_gather(rel_ref[...], rid)
        if bucket == 0:
            for copy in load_src + load_tgt[:1]:
                copy.wait()
        s_hi, s_lo = split(now_src[...])
        for e, m in groups:
            some = pl.ds(e, m)
            picked[:, some] = nn(s_hi, hot[:, some]) + nn(s_lo, hot[:, some])
        for e, m in groups:
            some = pl.ds(e, m)
            queries = picked[:, some] * relation[:, some]
            hi, lo = split(jnp.transpose(queries * 0.5))
            qt_ref[0, some, :] = hi
            qt_ref[1, some, :] = lo
            hi, lo = split(queries)
            q_ref[0, :, some] = hi
            q_ref[1, :, some] = lo
        rhot[...] = one_hot(rid, rels)

        def weigh(c):
            start, width = plan[c]
            cols = pl.ds(start, width)
            table = tgt_ref[:, cols] if bucket == 0 else recv[c][bucket - 1]
            t_hi, t_lo = split(table)
            put_pair(tables[c], t_hi, t_lo, True)
            count = counts[:, cols]
            lane = lax.broadcasted_iota(jnp.int32, (edges // len(groups), width), 1) + start
            for e, m in groups:
                some = pl.ds(e, m)
                if width == LANES:
                    score = fold(nn(qt_ref[0, some, :], tables[c][0])) + nn(qt_ref[1, some, :], t_hi)
                else:
                    score = (
                        nn(qt_ref[0, some, :], t_hi) + nn(qt_ref[0, some, :], t_lo) + nn(qt_ref[1, some, :], t_hi)
                    )
                half = jnp.tanh(score)
                weight = count * half + count - jnp.where(lane == tid[e:e + m], 0.5 - 0.5 * half, 0.0)
                w_hi, w_lo = split(weight)
                put_pair(weights[c], w_hi, w_lo, False, some)

        def query_part(c, part):
            if plan[c][1] == LANES:
                return (
                    nt(tables[c][1, part, :], weights[c][0])
                    + nt(tables[c][0, part, LANES:], weights[c][0, :, :LANES])
                )
            return (
                nt(tables[c][0, part, :], weights[c][0])
                + nt(tables[c][0, part, :], weights[c][1])
                + nt(tables[c][1, part, :], weights[c][0])
            )

        def finish(c):
            start, width = plan[c]
            cols = pl.ds(start, width)
            if bucket == 0:
                table = tgt_ref[:, cols]
                state = trow_ref[cols].reshape(1, width)
            else:
                table = recv[c][bucket - 1]
                state = row_recv[bucket - 1, c, :, :width]
            if width == LANES:
                grad = fold(nn(q_ref[0], weights[c][0])) + nn(q_ref[1], weights[c][0, :, :LANES])
            else:
                grad = nn(q_ref[0], weights[c][0]) + nn(q_ref[0], weights[c][1]) + nn(q_ref[1], weights[c][0])
            fresh = state + jnp.sum(grad * grad, axis=0, keepdims=True) * (1.0 / dims)
            new = table - grad * (learn_rate / (jnp.sqrt(fresh) + epsilon))
            if last:
                out_tgt[:, cols] = new
                out_trow[:, cols] = fresh
            else:
                send[c][bucket] = new
                row_send[bucket, c, :, :width] = fresh

        def relate(part, whole):
            g_hi, g_lo = split(whole * picked[part, :])
            rel_grad = nt(g_hi, rhot[...]) + nt(g_lo, rhot[...])
            if bucket == 0:
                rel_all[my_rel, part, :] = rel_grad
            else:
                rel_all[my_rel, part, :] = rel_all[my_rel, part, :] + rel_grad

        everything = pl.ds(0, dims)

        def arrive(c):
            if bucket > 0:
                for p, piece in enumerate(pieces):
                    if piece[0] == c:
                        hop(bucket - 1, p).wait_recv()
                row_hop(bucket - 1, c).wait_recv()

        def depart(c):
            for p, piece in enumerate(pieces):
                if piece[0] != c:
                    continue
                if p in relayed:
                    @pl.when(my_blk == n_blk - 1)
                    def _():
                        to_relay(bucket, p).start()

                    @pl.when(my_blk != n_blk - 1)
                    def _():
                        hop(bucket, p).start()
                else:
                    hop(bucket, p).start()
            row_hop(bucket, c).start()

        if not last:
            arrive(0)
            weigh(0)
            if bucket == 0:
                load_late[0].wait()
            finish(0)
            if bucket == 0:
                enter()
            depart(0)
            if bucket == 0:
                for copy in load_tgt[1:] + load_late[1:]:
                    copy.wait()
            if final > 0:
                arrive(1)
                weigh(1)
            for c in range(1, final + 1):
                if c < final:
                    arrive(c + 1)
                finish(c)
                if c < final:
                    weigh(c + 1)
                depart(c)
            for p in relayed:
                if pieces[p][0] == 0:
                    relay(bucket, p)
            total = query_part(0, everything)
            for c in range(1, len(plan)):
                total += query_part(c, everything)
            gq_ref[...] = total
            relate(everything, total)
        else:
            def gather_query(c):
                part = query_part(c, everything)
                gq_ref[...] = part if c == 0 else gq_ref[...] + part

            for c in range(final):
                arrive(c)
                weigh(c)
                if c > 0:
                    gather_query(c - 1)
                    finish(c - 1)
            if final > 0:
                gather_query(final - 1)
                finish(final - 1)
            arrive(final)
            weigh(final)
            for b, (r, n) in enumerate(blocks):
                part = pl.ds(r, n)
                whole = query_part(final, part)
                if final > 0:
                    whole = gq_ref[part, :] + whole
                gq_ref[part, :] = whole
                relate(part, whole)
                for step in range(1, n_rel):
                    rel_hop(lax.rem(my_rel + step, n_rel), my_rel, step, b).start()
            finish(final)
        g_hi, g_lo = split(gq_ref[...] * relation[...])
        src_grad = nt(g_hi, hot[...]) + nt(g_lo, hot[...])
        now_srow = srow_ref[...].reshape(1, rows) if bucket == 0 else out_srow[...]
        fresh = now_srow + jnp.sum(src_grad * src_grad, axis=0, keepdims=True) * (1.0 / dims)
        out_src[...] = now_src[...] - src_grad * (learn_rate / (jnp.sqrt(fresh) + epsilon))
        out_srow[...] = fresh
        if not last:
            for p in relayed:
                if pieces[p][0] > 0:
                    relay(bucket, p)

    for bucket in range(buckets - 1):
        for p in range(len(pieces)):
            hop(bucket, p).wait_send()
        for p in relayed:
            @pl.when(my_blk == pieces[p][3])
            def _():
                from_relay(bucket, p).wait_send()
        for c in range(len(plan)):
            row_hop(bucket, c).wait_send()
    for b, (r, n) in enumerate(blocks):
        part = pl.ds(r, n)
        for step in range(1, n_rel):
            peer = lax.rem(my_rel + n_rel - step, n_rel)
            arrived = rel_hop(peer, peer, step, b)
            arrived.wait_send()
            arrived.wait_recv()
        total = rel_all[0, part, :]
        for step in range(1, n_rel):
            total = total + rel_all[step, part, :]
        new_state = rstate_ref[part, :] + total * total
        out_rstate[part, :] = new_state
        out_rel[part, :] = rel_ref[part, :] - learn_rate * total / (jnp.sqrt(new_state) + epsilon)


def solution(mesh):
    n_blk, n_rel = mesh.shape["blk"], mesh.shape["rel"]

    def per_device(
        source_table, source_state, target_table, target_state, relation_ops, relation_state,
        source_ids, target_ids, relation_ids, negative_ids,
    ):
        dims, rows = source_table.shape
        rels = relation_ops.shape[1]
        buckets, edges = source_ids.shape
        plan = chunk_plan(rows)
        arrivals, blocks = row_blocks(dims)
        pieces = piece_plan(plan, dims, n_blk)
        chunks = len(plan)
        vmem = pl.BlockSpec(memory_space=pltpu.VMEM)
        shape = jax.ShapeDtypeStruct
        moves = [pltpu.VMEM((buckets - 1, dims, width), F32) for _, width in plan]
        out = pl.pallas_call(
            functools.partial(kernel, n_blk, n_rel, plan, pieces, arrivals, blocks),
            out_shape=(
                pltpu.VMEM((dims, rows), F32), pltpu.VMEM((1, rows), F32),
                pltpu.VMEM((dims, rows), F32), pltpu.VMEM((1, rows), F32),
                pltpu.VMEM((dims, rels), F32), pltpu.VMEM((dims, rels), F32),
            ),
            in_specs=[pl.BlockSpec(memory_space=pltpu.HBM)] * 10,
            out_specs=(vmem,) * 6,
            scratch_shapes=[
                pltpu.VMEM((dims, rows), F32), pltpu.VMEM((rows,), F32),
                pltpu.VMEM((dims, rows), F32), pltpu.VMEM((rows,), F32),
                pltpu.VMEM((dims, rels), F32), pltpu.VMEM((dims, rels), F32),
                *[pltpu.VMEM(ids.shape, jnp.int32) for ids in (source_ids, relation_ids, target_ids, negative_ids)],
                pltpu.SemaphoreType.DMA((10 + len(arrivals),)),
                pltpu.VMEM((rows, edges), BF16),
                pltpu.VMEM((rels, edges), BF16),
                pltpu.VMEM((2, edges, dims), BF16),
                pltpu.VMEM((2, dims, edges), BF16),
                pltpu.VMEM((dims, edges), F32),
                pltpu.VMEM((dims, edges), F32),
                pltpu.VMEM((dims, edges), F32),
                pltpu.VMEM((1, rows), F32),
                pltpu.VMEM((n_rel, dims, rels), F32),
                pltpu.SemaphoreType.DMA((n_rel, len(blocks))),
                pltpu.SemaphoreType.DMA((n_rel, len(blocks))),
                pltpu.SemaphoreType.DMA((buckets - 1, len(pieces))),
                pltpu.SemaphoreType.DMA((buckets - 1, len(pieces))),
                pltpu.VMEM((buckets - 1, chunks, 1, 256), F32),
                pltpu.VMEM((buckets - 1, chunks, 1, 256), F32),
                *[pltpu.VMEM((2, dims, 256), BF16) for _ in plan],
                *[pltpu.VMEM((2, edges, 256), BF16) for _ in plan],
                *moves,
                *moves,
                *[
                    pltpu.VMEM((buckets - 1, n, plan[c][1]), F32)
                    for c, _, n, at in pieces if at is not None
                ],
                pltpu.SemaphoreType.DMA((buckets - 1, len(pieces))),
                pltpu.SemaphoreType.DMA((buckets - 1, len(pieces))),
                pltpu.SemaphoreType.DMA((buckets - 1, chunks)),
                pltpu.SemaphoreType.DMA((buckets - 1, chunks)),
            ],
            compiler_params=pltpu.CompilerParams(
                collective_id=0, has_side_effects=True, vmem_limit_bytes=40 * 1024 * 1024
            ),
        )(*(
            pltpu.with_memory_space_constraint(x, pltpu.HBM) for x in (
                source_table, source_state, target_table, target_state,
                relation_ops, relation_state, source_ids, relation_ids,
                target_ids, negative_ids,
            )
        ))
        hbm = pl.BlockSpec(memory_space=pl.ANY)
        return pl.pallas_call(
            emit,
            out_shape=(
                shape((dims, rows), F32), shape((rows,), F32),
                shape((dims, rows), F32), shape((rows,), F32),
                shape((dims, rels), F32), shape((dims, rels), F32),
            ),
            in_specs=[vmem] * 6,
            out_specs=(hbm,) * 6,
            scratch_shapes=[pltpu.VMEM((rows,), F32), pltpu.VMEM((rows,), F32), pltpu.SemaphoreType.DMA((6,))],
            compiler_params=pltpu.CompilerParams(vmem_limit_bytes=16 * 1024 * 1024),
        )(*out)

    split_both = ("blk", "rel")
    return jax.shard_map(
        per_device,
        mesh=mesh,
        in_specs=(
            P(None, split_both), P(split_both), P(None, split_both), P(split_both),
            P(None, "blk"), P(None, "blk"),
            P(None, split_both), P(None, split_both), P(None, split_both), P(None, split_both),
        ),
        out_specs=(
            P(None, split_both), P(split_both), P(None, split_both), P(split_both),
            P(None, "blk"), P(None, "blk"),
        ),
        check_vma=False,
    )
```

```python
import functools

import jax
import jax.numpy as jnp
from jax import lax
from jax.experimental import pallas as pl
from jax.experimental.pallas import tpu as pltpu
from jax.sharding import PartitionSpec as P

learn_rate = 0.1
epsilon = 1e-06
LANES = 128
MESH = pl.DeviceIdType.MESH
F32 = jnp.float32
BF16 = jnp.bfloat16


def split(x):
    high = x.astype(BF16)
    return high, (x - high.astype(F32)).astype(BF16)


def nn(a, b):
    return lax.dot_general(a, b, (((1,), (0,)), ((), ())), preferred_element_type=F32)


def nt(a, b):
    return lax.dot_general(a, b, (((1,), (1,)), ((), ())), preferred_element_type=F32)


def column(row):
    wide = jnp.broadcast_to(row.astype(F32), (8, row.shape[1]))
    return jnp.transpose(wide)[:, :1].astype(jnp.int32)


def one_hot(row, height):
    low = lax.rem(row, LANES)
    inner = (lax.broadcasted_iota(jnp.int32, (LANES, row.shape[1]), 0) == low).astype(F32).astype(BF16)
    if height == LANES:
        return inner
    out = []
    for start in range(0, height, LANES):
        here = (row - low == start).astype(F32).astype(BF16)
        out.append(inner * jnp.broadcast_to(here, inner.shape))
    return jnp.concatenate(out, axis=0)


def chunk_plan(rows):
    if rows % 256 == 0 and rows >= 512:
        widths = [LANES] + [256] * (rows // 256 - 1) + [LANES]
    else:
        widths = [LANES] * (rows // LANES)
    return [(sum(widths[:i]), w) for i, w in enumerate(widths)]


def row_blocks(dims):
    first = dims // 64 * 16
    second = first + (dims - first + 31) // 32 * 16
    return [(0, first), (first, second - first), (second, dims - second)]


def lane_gather(table, index):
    tall = table.shape[0]
    groups = table.shape[1] // LANES
    out = []
    for start in range(0, index.shape[1], LANES):
        one = jnp.broadcast_to(index[:, start:start + LANES], (tall, LANES))
        low = lax.rem(one, LANES)
        got = jnp.take_along_axis(table[:, :LANES], low, axis=1)
        for g in range(1, groups):
            other = jnp.take_along_axis(table[:, g * LANES:(g + 1) * LANES], low, axis=1)
            got = jnp.where(one >= g * LANES, other, got)
        out.append(got)
    return jnp.concatenate(out, axis=1)


def emit(*refs):
    inputs, outputs, (first, second, sem) = refs[:6], refs[6:12], refs[12:]
    copies = []
    for i in (0, 2, 4, 5):
        copies.append(pltpu.make_async_copy(inputs[i], outputs[i], sem.at[i]))
        copies[-1].start()
    for i, line in ((1, first), (3, second)):
        line[...] = inputs[i][0, :]
        copies.append(pltpu.make_async_copy(line, outputs[i], sem.at[i]))
        copies[-1].start()
    for copy in copies:
        copy.wait()


def kernel(n_blk, n_rel, plan, blocks, *refs):
    refs = list(refs)

    def take(n):
        out = refs[:n]
        del refs[:n]
        return out

    src_in, srow_in, tgt_in, trow_in, rel_in, rstate_in, sid_in, rid_in, tid_in, nid_in = take(10)
    out_src, out_srow, out_tgt, out_trow, out_rel, out_rstate = take(6)
    src_ref, srow_ref, tgt_ref, trow_ref, rel_ref, rstate_ref, sid_ref, rid_ref, tid_ref, nid_ref = take(10)
    load_sem, hot, rhot, qt_ref, q_ref, picked, relation, gq_ref, counts, rel_all = take(10)
    rsend_sem, rrecv_sem, send_sem, recv_sem, row_send, row_recv = take(6)
    (turned,) = take(1)
    tables, weights = take(len(plan)), take(len(plan))
    send, recv = take(len(plan)), take(len(plan))
    dims, rows = src_ref.shape
    buckets, edges = sid_ref.shape
    negs = nid_ref.shape[1]
    rels = rel_ref.shape[1]
    final = len(plan) - 1
    groups = [(e, min(256, edges - e)) for e in range(0, edges, 256)]
    my_blk = lax.axis_index("blk")
    my_rel = lax.axis_index("rel")
    nxt = lax.rem(my_blk + 1, n_blk)
    prv = lax.rem(my_blk + n_blk - 1, n_blk)

    loads = []

    def load(there, here):
        loads.append(pltpu.make_async_copy(there, here, load_sem.at[len(loads)]))
        loads[-1].start()
        return loads[-1]

    load_ids = [
        load(sid_in, sid_ref), load(rid_in, rid_ref), load(nid_in, nid_ref), load(tid_in, tid_ref)
    ]
    load_rel = load(rel_in, rel_ref)
    load_src = load(src_in, src_ref)
    load_tgt = [
        load(tgt_in.at[:, pl.ds(start, width)], tgt_ref.at[:, pl.ds(start, width)])
        for start, width in ((0, plan[0][1]), (plan[0][1], rows - plan[0][1])) if width
    ]
    load_late = [load(trow_in, trow_ref), load(srow_in, srow_ref), load(rstate_in, rstate_ref)]

    barrier = pltpu.get_barrier_semaphore()
    pl.semaphore_signal(barrier, inc=1, device_id={"blk": prv}, device_id_type=MESH)
    for step in range(1, n_rel):
        pl.semaphore_signal(
            barrier, inc=1, device_id={"rel": lax.rem(my_rel + step, n_rel)}, device_id_type=MESH
        )

    def hop(bucket, c):
        return pltpu.make_async_remote_copy(
            src_ref=send[c].at[bucket],
            dst_ref=recv[c].at[bucket],
            send_sem=send_sem.at[0, bucket, c],
            recv_sem=recv_sem.at[0, bucket, c],
            device_id={"blk": nxt},
            device_id_type=MESH,
        )

    def row_hop(bucket, c):
        return pltpu.make_async_remote_copy(
            src_ref=row_send.at[bucket, c, :, pl.ds(0, plan[c][1])],
            dst_ref=row_recv.at[bucket, c, :, pl.ds(0, plan[c][1])],
            send_sem=send_sem.at[1, bucket, c],
            recv_sem=recv_sem.at[1, bucket, c],
            device_id={"blk": nxt},
            device_id_type=MESH,
        )

    def rel_hop(to, slot, step, b):
        r, n = blocks[b]
        return pltpu.make_async_remote_copy(
            src_ref=rel_all.at[slot, pl.ds(r, n)],
            dst_ref=rel_all.at[slot, pl.ds(r, n)],
            send_sem=rsend_sem.at[step - 1, b],
            recv_sem=rrecv_sem.at[slot, b],
            device_id={"rel": to},
            device_id_type=MESH,
        )

    def put_pair(ref, hi, lo, twice, part=slice(None)):
        width = hi.shape[1]
        if width == LANES:
            ref[0, part, :LANES] = hi
            ref[0, part, LANES:] = lo
            if twice:
                ref[1, :, :LANES] = hi
                ref[1, :, LANES:] = hi
        else:
            ref[0, part, :] = hi
            ref[1, part, :] = lo

    def fold(wide):
        return wide[:, :LANES] + wide[:, LANES:]

    for copy in load_ids:
        copy.wait()

    for bucket in range(buckets):
        last = bucket + 1 == buckets
        now_src = src_ref if bucket == 0 else out_src
        sid = sid_ref[pl.ds(bucket, 1), :]
        rid = rid_ref[pl.ds(bucket, 1), :]
        hot[...] = one_hot(sid, rows)
        if bucket == 0:
            load_rel.wait()
            for copy in (load_src, load_tgt[0], load_late[0]):
                copy.wait()
        s_hi, s_lo = split(now_src[...])
        for e, m in groups:
            some = pl.ds(e, m)
            picked[:, some] = nn(s_hi, hot[:, some]) + nn(s_lo, hot[:, some])
        relation[...] = lane_gather(rel_ref[...], rid)
        for e, m in groups:
            some = pl.ds(e, m)
            hi, lo = split(picked[:, some] * relation[:, some])
            q_ref[0, :, some] = hi
            q_ref[1, :, some] = lo

        def turn():
            for e, m in groups:
                some = pl.ds(e, m)
                hi, lo = split(jnp.transpose(picked[:, some] * relation[:, some] * 0.5))
                qt_ref[0, some, :] = hi
                qt_ref[1, some, :] = lo
            nid = column(nid_ref[pl.ds(bucket, 1), :])
            for start in range(0, rows, LANES):
                lane = lax.broadcasted_iota(jnp.int32, (negs, LANES), 1) + start
                counts[:, pl.ds(start, LANES)] = jnp.sum(
                    (lane == nid).astype(F32), axis=0, keepdims=True
                ) * (0.5 / negs)
            rhot[...] = one_hot(rid, rels)
            return column(tid_ref[pl.ds(bucket, 1), :])

        def weigh_turned():
            table = tgt_ref[:, :LANES]
            hi, lo = split(table)
            put_pair(tables[0], hi, lo, True)
            hi, lo = split(jnp.transpose(table) * 0.5)
            wide = nn(jnp.concatenate([hi, lo], axis=0), q_ref[0])
            score = wide[:LANES] + wide[LANES:] + nn(hi, q_ref[1])
            half = jnp.tanh(score)
            here = lax.broadcasted_iota(jnp.int32, (LANES, negs), 0) == nid_ref[pl.ds(bucket, 1), :]
            count = jnp.sum(here.astype(F32), axis=1, keepdims=True) * (0.5 / negs)
            here = lax.broadcasted_iota(jnp.int32, (LANES, edges), 0) == tid_ref[pl.ds(bucket, 1), :]
            weight = count * half + count - jnp.where(here, 0.5 - 0.5 * half, 0.0)
            hi, lo = split(weight)
            turned[:LANES, :] = hi
            turned[LANES:, :] = lo

        def weigh(c):
            start, width = plan[c]
            cols = pl.ds(start, width)
            table = tgt_ref[:, cols] if bucket == 0 else recv[c][bucket - 1]
            t_hi, t_lo = split(table)
            put_pair(tables[c], t_hi, t_lo, True)
            count = counts[:, cols]
            lane = lax.broadcasted_iota(jnp.int32, (edges // len(groups), width), 1) + start
            for e, m in groups:
                some = pl.ds(e, m)
                if width == LANES:
                    score = fold(nn(qt_ref[0, some, :], tables[c][0])) + nn(qt_ref[1, some, :], t_hi)
                else:
                    score = (
                        nn(qt_ref[0, some, :], t_hi) + nn(qt_ref[0, some, :], t_lo) + nn(qt_ref[1, some, :], t_hi)
                    )
                half = jnp.tanh(score)
                weight = count * half + count - jnp.where(lane == tid[e:e + m], 0.5 - 0.5 * half, 0.0)
                w_hi, w_lo = split(weight)
                put_pair(weights[c], w_hi, w_lo, False, some)

        def query_part(c, part):
            if bucket == 0 and c == 0:
                return nn(tables[c][1, part, :], turned[...]) + nn(tables[c][0, part, LANES:], turned[:LANES, :])
            if plan[c][1] == LANES:
                return (
                    nt(tables[c][1, part, :], weights[c][0])
                    + nt(tables[c][0, part, LANES:], weights[c][0, :, :LANES])
                )
            return (
                nt(tables[c][0, part, :], weights[c][0])
                + nt(tables[c][0, part, :], weights[c][1])
                + nt(tables[c][1, part, :], weights[c][0])
            )

        def finish(c):
            start, width = plan[c]
            cols = pl.ds(start, width)
            if bucket == 0:
                table = tgt_ref[:, cols]
                state = trow_ref[cols].reshape(1, width)
            else:
                table = recv[c][bucket - 1]
                state = row_recv[bucket - 1, c, :, :width]
            if bucket == 0 and c == 0:
                grad = fold(nt(q_ref[0], turned[...])) + nt(q_ref[1], turned[:LANES, :])
            elif width == LANES:
                grad = fold(nn(q_ref[0], weights[c][0])) + nn(q_ref[1], weights[c][0, :, :LANES])
            else:
                grad = nn(q_ref[0], weights[c][0]) + nn(q_ref[0], weights[c][1]) + nn(q_ref[1], weights[c][0])
            fresh = state + jnp.sum(grad * grad, axis=0, keepdims=True) * (1.0 / dims)
            new = table - grad * (learn_rate / (jnp.sqrt(fresh) + epsilon))
            if last:
                out_tgt[:, cols] = new
                out_trow[:, cols] = fresh
            else:
                send[c][bucket] = new
                row_send[bucket, c, :, :width] = fresh

        def relate(part, whole):
            g_hi, g_lo = split(whole * picked[part, :])
            rel_grad = nt(g_hi, rhot[...]) + nt(g_lo, rhot[...])
            if bucket == 0:
                rel_all[my_rel, part, :] = rel_grad
            else:
                rel_all[my_rel, part, :] = rel_all[my_rel, part, :] + rel_grad

        everything = pl.ds(0, dims)

        def arrive(c):
            if bucket > 0:
                hop(bucket - 1, c).wait_recv()
                row_hop(bucket - 1, c).wait_recv()

        def depart(c):
            hop(bucket, c).start()
            row_hop(bucket, c).start()

        if not last:
            if bucket == 0:
                weigh_turned()
                finish(0)
                pl.semaphore_wait(barrier, n_rel)
                depart(0)
                for copy in load_tgt[1:] + load_late[1:]:
                    copy.wait()
                tid = turn()
            else:
                tid = turn()
                arrive(0)
                weigh(0)
                finish(0)
                depart(0)
            if final > 0:
                arrive(1)
                weigh(1)
            for c in range(1, final + 1):
                if c < final:
                    arrive(c + 1)
                finish(c)
                if c == 1:
                    depart(c)
                if c < final:
                    weigh(c + 1)
                if c > 1:
                    depart(c)
            total = query_part(0, everything)
            for c in range(1, len(plan)):
                total += query_part(c, everything)
            gq_ref[...] = total
            relate(everything, total)
        else:
            def gather_query(c):
                part = query_part(c, everything)
                gq_ref[...] = part if c == 0 else gq_ref[...] + part

            tid = turn()
            if bucket == 0:
                pl.semaphore_wait(barrier, n_rel)
                for copy in load_tgt[1:] + load_late[1:]:
                    copy.wait()
            for c in range(final):
                arrive(c)
                weigh_turned() if bucket == 0 and c == 0 else weigh(c)
                if c > 0:
                    gather_query(c - 1)
                    finish(c - 1)
            if final > 0:
                gather_query(final - 1)
                finish(final - 1)
            arrive(final)
            weigh(final)
            for b, (r, n) in enumerate(blocks):
                part = pl.ds(r, n)
                whole = query_part(final, part)
                if final > 0:
                    whole = gq_ref[part, :] + whole
                gq_ref[part, :] = whole
                relate(part, whole)
                for step in range(1, n_rel):
                    rel_hop(lax.rem(my_rel + step, n_rel), my_rel, step, b).start()
            finish(final)
        g_hi, g_lo = split(gq_ref[...] * relation[...])
        src_grad = nt(g_hi, hot[...]) + nt(g_lo, hot[...])
        now_srow = srow_ref[...].reshape(1, rows) if bucket == 0 else out_srow[...]
        fresh = now_srow + jnp.sum(src_grad * src_grad, axis=0, keepdims=True) * (1.0 / dims)
        out_src[...] = now_src[...] - src_grad * (learn_rate / (jnp.sqrt(fresh) + epsilon))
        out_srow[...] = fresh

    for bucket in range(buckets - 1):
        for c in range(len(plan)):
            hop(bucket, c).wait_send()
            row_hop(bucket, c).wait_send()
    for b, (r, n) in enumerate(blocks):
        part = pl.ds(r, n)
        for step in range(1, n_rel):
            peer = lax.rem(my_rel + n_rel - step, n_rel)
            arrived = rel_hop(peer, peer, step, b)
            arrived.wait_send()
            arrived.wait_recv()
        total = rel_all[0, part, :]
        for step in range(1, n_rel):
            total = total + rel_all[step, part, :]
        new_state = rstate_ref[part, :] + total * total
        out_rstate[part, :] = new_state
        out_rel[part, :] = rel_ref[part, :] - learn_rate * total / (jnp.sqrt(new_state) + epsilon)


def solution(mesh):
    n_blk, n_rel = mesh.shape["blk"], mesh.shape["rel"]

    def per_device(
        source_table, source_state, target_table, target_state, relation_ops, relation_state,
        source_ids, target_ids, relation_ids, negative_ids,
    ):
        dims, rows = source_table.shape
        rels = relation_ops.shape[1]
        buckets, edges = source_ids.shape
        plan = chunk_plan(rows)
        blocks = row_blocks(dims)
        chunks = len(plan)
        vmem = pl.BlockSpec(memory_space=pltpu.VMEM)
        shape = jax.ShapeDtypeStruct
        moves = [pltpu.VMEM((buckets - 1, dims, width), F32) for _, width in plan]
        out = pl.pallas_call(
            functools.partial(kernel, n_blk, n_rel, plan, blocks),
            out_shape=(
                pltpu.VMEM((dims, rows), F32), pltpu.VMEM((1, rows), F32),
                pltpu.VMEM((dims, rows), F32), pltpu.VMEM((1, rows), F32),
                pltpu.VMEM((dims, rels), F32), pltpu.VMEM((dims, rels), F32),
            ),
            in_specs=[pl.BlockSpec(memory_space=pltpu.HBM)] * 10,
            out_specs=(vmem,) * 6,
            scratch_shapes=[
                pltpu.VMEM((dims, rows), F32), pltpu.VMEM((rows,), F32),
                pltpu.VMEM((dims, rows), F32), pltpu.VMEM((rows,), F32),
                pltpu.VMEM((dims, rels), F32), pltpu.VMEM((dims, rels), F32),
                *[pltpu.VMEM(ids.shape, jnp.int32) for ids in (source_ids, relation_ids, target_ids, negative_ids)],
                pltpu.SemaphoreType.DMA((11,)),
                pltpu.VMEM((rows, edges), BF16),
                pltpu.VMEM((rels, edges), BF16),
                pltpu.VMEM((2, edges, dims), BF16),
                pltpu.VMEM((2, dims, edges), BF16),
                pltpu.VMEM((dims, edges), F32),
                pltpu.VMEM((dims, edges), F32),
                pltpu.VMEM((dims, edges), F32),
                pltpu.VMEM((1, rows), F32),
                pltpu.VMEM((n_rel, dims, rels), F32),
                pltpu.SemaphoreType.DMA((n_rel, len(blocks))),
                pltpu.SemaphoreType.DMA((n_rel, len(blocks))),
                pltpu.SemaphoreType.DMA((2, buckets - 1, chunks)),
                pltpu.SemaphoreType.DMA((2, buckets - 1, chunks)),
                pltpu.VMEM((buckets - 1, chunks, 1, 256), F32),
                pltpu.VMEM((buckets - 1, chunks, 1, 256), F32),
                pltpu.VMEM((2 * LANES, edges), BF16),
                *[pltpu.VMEM((2, dims, 256), BF16) for _ in plan],
                *[pltpu.VMEM((2, edges, 256), BF16) for _ in plan],
                *moves,
                *moves,
            ],
            compiler_params=pltpu.CompilerParams(
                collective_id=0, has_side_effects=True, vmem_limit_bytes=40 * 1024 * 1024
            ),
        )(*(
            pltpu.with_memory_space_constraint(x, pltpu.HBM) for x in (
                source_table, source_state, target_table, target_state,
                relation_ops, relation_state, source_ids, relation_ids,
                target_ids, negative_ids,
            )
        ))
        hbm = pl.BlockSpec(memory_space=pl.ANY)
        return pl.pallas_call(
            emit,
            out_shape=(
                shape((dims, rows), F32), shape((rows,), F32),
                shape((dims, rows), F32), shape((rows,), F32),
                shape((dims, rels), F32), shape((dims, rels), F32),
            ),
            in_specs=[vmem] * 6,
            out_specs=(hbm,) * 6,
            scratch_shapes=[pltpu.VMEM((rows,), F32), pltpu.VMEM((rows,), F32), pltpu.SemaphoreType.DMA((6,))],
            compiler_params=pltpu.CompilerParams(vmem_limit_bytes=16 * 1024 * 1024),
        )(*out)

    split_both = ("blk", "rel")
    return jax.shard_map(
        per_device,
        mesh=mesh,
        in_specs=(
            P(None, split_both), P(split_both), P(None, split_both), P(split_both),
            P(None, "blk"), P(None, "blk"),
            P(None, split_both), P(None, split_both), P(None, split_both), P(None, split_both),
        ),
        out_specs=(
            P(None, split_both), P(split_both), P(None, split_both), P(split_both),
            P(None, "blk"), P(None, "blk"),
        ),
        check_vma=False,
    )
```

```python
import functools

import jax
import jax.numpy as jnp
from jax import lax
from jax.experimental import pallas as pl
from jax.experimental.pallas import tpu as pltpu
from jax.sharding import PartitionSpec as P

learn_rate = 0.1
epsilon = 1e-06
LANES = 128
MESH = pl.DeviceIdType.MESH
F32 = jnp.float32
BF16 = jnp.bfloat16


def split(x):
    high = x.astype(BF16)
    return high, (x - high.astype(F32)).astype(BF16)


def nn(a, b):
    return lax.dot_general(a, b, (((1,), (0,)), ((), ())), preferred_element_type=F32)


def nt(a, b):
    return lax.dot_general(a, b, (((1,), (1,)), ((), ())), preferred_element_type=F32)


def column(row):
    wide = jnp.broadcast_to(row.astype(F32), (8, row.shape[1]))
    return jnp.transpose(wide)[:, :1].astype(jnp.int32)


def one_hot(row, height):
    low = lax.rem(row, LANES)
    inner = (lax.broadcasted_iota(jnp.int32, (LANES, row.shape[1]), 0) == low).astype(F32).astype(BF16)
    if height == LANES:
        return inner
    out = []
    for start in range(0, height, LANES):
        here = (row - low == start).astype(F32).astype(BF16)
        out.append(inner * jnp.broadcast_to(here, inner.shape))
    return jnp.concatenate(out, axis=0)


def chunk_plan(rows):
    if rows % 256 == 0 and rows >= 512:
        widths = [LANES] + [256] * (rows // 256 - 1) + [LANES]
    else:
        widths = [LANES] * (rows // LANES)
    return [(sum(widths[:i]), w) for i, w in enumerate(widths)]


def row_blocks(dims):
    first = dims // 64 * 16
    second = first + (dims - first + 31) // 32 * 16
    return [(0, first), (first, second - first), (second, dims - second)]


def lane_gather(table, index):
    tall = table.shape[0]
    groups = table.shape[1] // LANES
    out = []
    for start in range(0, index.shape[1], LANES):
        one = jnp.broadcast_to(index[:, start:start + LANES], (tall, LANES))
        low = lax.rem(one, LANES)
        got = jnp.take_along_axis(table[:, :LANES], low, axis=1)
        for g in range(1, groups):
            other = jnp.take_along_axis(table[:, g * LANES:(g + 1) * LANES], low, axis=1)
            got = jnp.where(one >= g * LANES, other, got)
        out.append(got)
    return jnp.concatenate(out, axis=1)


def emit(*refs):
    inputs, outputs, (first, second, sem) = refs[:6], refs[6:12], refs[12:]
    copies = []
    for i in (0, 2, 4, 5):
        copies.append(pltpu.make_async_copy(inputs[i], outputs[i], sem.at[i]))
        copies[-1].start()
    for i, line in ((1, first), (3, second)):
        line[...] = inputs[i][0, :]
        copies.append(pltpu.make_async_copy(line, outputs[i], sem.at[i]))
        copies[-1].start()
    for copy in copies:
        copy.wait()


def kernel(n_blk, n_rel, plan, blocks, *refs):
    refs = list(refs)

    def take(n):
        out = refs[:n]
        del refs[:n]
        return out

    src_in, srow_in, tgt_in, trow_in, rel_in, rstate_in, sid_in, rid_in, tid_in, nid_in = take(10)
    out_src, out_srow, out_tgt, out_trow, out_rel, out_rstate = take(6)
    src_ref, srow_ref, tgt_ref, trow_ref, rel_ref, rstate_ref, sid_ref, rid_ref, tid_ref, nid_ref = take(10)
    load_sem, hot, rhot, qt_ref, q_ref, picked, relation, gq_ref, counts, rel_all = take(10)
    rsend_sem, rrecv_sem, send_sem, recv_sem, row_send, row_recv = take(6)
    (turned,) = take(1)
    tables, weights = take(len(plan)), take(len(plan))
    send, recv = take(len(plan)), take(len(plan))
    dims, rows = src_ref.shape
    buckets, edges = sid_ref.shape
    negs = nid_ref.shape[1]
    rels = rel_ref.shape[1]
    final = len(plan) - 1
    groups = [(e, min(256, edges - e)) for e in range(0, edges, 256)]
    my_blk = lax.axis_index("blk")
    my_rel = lax.axis_index("rel")
    nxt = lax.rem(my_blk + 1, n_blk)
    prv = lax.rem(my_blk + n_blk - 1, n_blk)

    loads = []

    def load(there, here):
        loads.append(pltpu.make_async_copy(there, here, load_sem.at[len(loads)]))
        loads[-1].start()
        return loads[-1]

    load_ids = [
        load(sid_in, sid_ref), load(rid_in, rid_ref), load(nid_in, nid_ref), load(tid_in, tid_ref)
    ]
    quarter = dims // 64 * 16
    ends = [0, quarter, 2 * quarter, 3 * quarter, dims]
    load_src = [
        load(src_in.at[pl.ds(r, n - r)], src_ref.at[pl.ds(r, n - r)]) for r, n in zip(ends[:2], ends[1:3])
    ]
    load_rel = load(rel_in, rel_ref)
    load_src += [
        load(src_in.at[pl.ds(r, n - r)], src_ref.at[pl.ds(r, n - r)]) for r, n in zip(ends[2:4], ends[3:])
    ]
    load_tgt = [
        load(tgt_in.at[:, pl.ds(start, width)], tgt_ref.at[:, pl.ds(start, width)])
        for start, width in ((0, plan[0][1]), (plan[0][1], rows - plan[0][1])) if width
    ]
    load_late = [load(trow_in, trow_ref), load(srow_in, srow_ref), load(rstate_in, rstate_ref)]

    barrier = pltpu.get_barrier_semaphore()
    pl.semaphore_signal(barrier, inc=1, device_id={"blk": prv}, device_id_type=MESH)
    for step in range(1, n_rel):
        pl.semaphore_signal(
            barrier, inc=1, device_id={"rel": lax.rem(my_rel + step, n_rel)}, device_id_type=MESH
        )

    def hop(bucket, c):
        return pltpu.make_async_remote_copy(
            src_ref=send[c].at[bucket],
            dst_ref=recv[c].at[bucket],
            send_sem=send_sem.at[0, bucket, c],
            recv_sem=recv_sem.at[0, bucket, c],
            device_id={"blk": nxt},
            device_id_type=MESH,
        )

    def row_hop(bucket, c):
        return pltpu.make_async_remote_copy(
            src_ref=row_send.at[bucket, c, :, pl.ds(0, plan[c][1])],
            dst_ref=row_recv.at[bucket, c, :, pl.ds(0, plan[c][1])],
            send_sem=send_sem.at[1, bucket, c],
            recv_sem=recv_sem.at[1, bucket, c],
            device_id={"blk": nxt},
            device_id_type=MESH,
        )

    def rel_hop(to, slot, step, b):
        r, n = blocks[b]
        return pltpu.make_async_remote_copy(
            src_ref=rel_all.at[slot, pl.ds(r, n)],
            dst_ref=rel_all.at[slot, pl.ds(r, n)],
            send_sem=rsend_sem.at[step - 1, b],
            recv_sem=rrecv_sem.at[slot, b],
            device_id={"rel": to},
            device_id_type=MESH,
        )

    def put_pair(ref, hi, lo, twice, part=slice(None)):
        width = hi.shape[1]
        if width == LANES:
            ref[0, part, :LANES] = hi
            ref[0, part, LANES:] = lo
            if twice:
                ref[1, :, :LANES] = hi
                ref[1, :, LANES:] = hi
        else:
            ref[0, part, :] = hi
            ref[1, part, :] = lo

    def fold(wide):
        return wide[:, :LANES] + wide[:, LANES:]

    for copy in load_ids:
        copy.wait()

    for bucket in range(buckets):
        last = bucket + 1 == buckets
        now_src = src_ref if bucket == 0 else out_src
        sid = sid_ref[pl.ds(bucket, 1), :]
        rid = rid_ref[pl.ds(bucket, 1), :]
        hot[...] = one_hot(sid, rows)
        for first in (0, 2):
            part = pl.ds(ends[first], ends[first + 2] - ends[first])
            if bucket == 0:
                for copy in load_src[first:first + 2]:
                    copy.wait()
                if first:
                    for copy in (load_rel, load_tgt[0], load_late[0]):
                        copy.wait()
            s_hi, s_lo = split(now_src[part, :])
            for e, m in groups:
                some = pl.ds(e, m)
                picked[part, some] = nn(s_hi, hot[:, some]) + nn(s_lo, hot[:, some])
        relation[...] = lane_gather(rel_ref[...], rid)
        for e, m in groups:
            some = pl.ds(e, m)
            hi, lo = split(picked[:, some] * relation[:, some])
            q_ref[0, :, some] = hi
            q_ref[1, :, some] = lo

        def turn():
            for e, m in groups:
                some = pl.ds(e, m)
                hi, lo = split(jnp.transpose(picked[:, some] * relation[:, some] * 0.5))
                qt_ref[0, some, :] = hi
                qt_ref[1, some, :] = lo
            nid = column(nid_ref[pl.ds(bucket, 1), :])
            for start in range(0, rows, LANES):
                lane = lax.broadcasted_iota(jnp.int32, (negs, LANES), 1) + start
                counts[:, pl.ds(start, LANES)] = jnp.sum(
                    (lane == nid).astype(F32), axis=0, keepdims=True
                ) * (0.5 / negs)
            rhot[...] = one_hot(rid, rels)
            return column(tid_ref[pl.ds(bucket, 1), :])

        def weigh_turned():
            table = tgt_ref[:, :LANES]
            hi, lo = split(table)
            put_pair(tables[0], hi, lo, True)
            hi, lo = split(jnp.transpose(table) * 0.5)
            wide = nn(jnp.concatenate([hi, lo], axis=0), q_ref[0])
            score = wide[:LANES] + wide[LANES:] + nn(hi, q_ref[1])
            half = jnp.tanh(score)
            here = lax.broadcasted_iota(jnp.int32, (LANES, negs), 0) == nid_ref[pl.ds(bucket, 1), :]
            count = jnp.sum(here.astype(F32), axis=1, keepdims=True) * (0.5 / negs)
            here = lax.broadcasted_iota(jnp.int32, (LANES, edges), 0) == tid_ref[pl.ds(bucket, 1), :]
            weight = count * half + count - jnp.where(here, 0.5 - 0.5 * half, 0.0)
            hi, lo = split(weight)
            turned[:LANES, :] = hi
            turned[LANES:, :] = lo

        def weigh(c):
            start, width = plan[c]
            cols = pl.ds(start, width)
            table = tgt_ref[:, cols] if bucket == 0 else recv[c][bucket - 1]
            t_hi, t_lo = split(table)
            put_pair(tables[c], t_hi, t_lo, True)
            count = counts[:, cols]
            lane = lax.broadcasted_iota(jnp.int32, (edges // len(groups), width), 1) + start
            for e, m in groups:
                some = pl.ds(e, m)
                if width == LANES:
                    score = fold(nn(qt_ref[0, some, :], tables[c][0])) + nn(qt_ref[1, some, :], t_hi)
                else:
                    score = (
                        nn(qt_ref[0, some, :], t_hi) + nn(qt_ref[0, some, :], t_lo) + nn(qt_ref[1, some, :], t_hi)
                    )
                half = jnp.tanh(score)
                weight = count * half + count - jnp.where(lane == tid[e:e + m], 0.5 - 0.5 * half, 0.0)
                w_hi, w_lo = split(weight)
                put_pair(weights[c], w_hi, w_lo, False, some)

        def query_part(c, part, some=slice(None)):
            if bucket == 0 and c == 0:
                return (
                    nn(tables[c][1, part, :], turned[:, some])
                    + nn(tables[c][0, part, LANES:], turned[:LANES, some])
                )
            if plan[c][1] == LANES:
                return (
                    nt(tables[c][1, part, :], weights[c][0, some, :])
                    + nt(tables[c][0, part, LANES:], weights[c][0, some, :LANES])
                )
            return (
                nt(tables[c][0, part, :], weights[c][0, some, :])
                + nt(tables[c][0, part, :], weights[c][1, some, :])
                + nt(tables[c][1, part, :], weights[c][0, some, :])
            )

        def finish(c):
            start, width = plan[c]
            cols = pl.ds(start, width)
            if bucket == 0:
                table = tgt_ref[:, cols]
                state = trow_ref[cols].reshape(1, width)
            else:
                table = recv[c][bucket - 1]
                state = row_recv[bucket - 1, c, :, :width]
            if bucket == 0 and c == 0:
                grad = fold(nt(q_ref[0], turned[...])) + nt(q_ref[1], turned[:LANES, :])
            elif width == LANES:
                grad = fold(nn(q_ref[0], weights[c][0])) + nn(q_ref[1], weights[c][0, :, :LANES])
            else:
                grad = nn(q_ref[0], weights[c][0]) + nn(q_ref[0], weights[c][1]) + nn(q_ref[1], weights[c][0])
            fresh = state + jnp.sum(grad * grad, axis=0, keepdims=True) * (1.0 / dims)
            new = table - grad * (learn_rate / (jnp.sqrt(fresh) + epsilon))
            if last:
                out_tgt[:, cols] = new
                out_trow[:, cols] = fresh
            else:
                send[c][bucket] = new
                row_send[bucket, c, :, :width] = fresh

        def relate(part, whole):
            g_hi, g_lo = split(whole * picked[part, :])
            rel_grad = nt(g_hi, rhot[...]) + nt(g_lo, rhot[...])
            if bucket == 0:
                rel_all[my_rel, part, :] = rel_grad
            else:
                rel_all[my_rel, part, :] = rel_all[my_rel, part, :] + rel_grad

        everything = pl.ds(0, dims)

        def arrive(c):
            if bucket > 0:
                hop(bucket - 1, c).wait_recv()
                row_hop(bucket - 1, c).wait_recv()

        def depart(c):
            hop(bucket, c).start()
            row_hop(bucket, c).start()

        if not last:
            if bucket == 0:
                weigh_turned()
                finish(0)
                pl.semaphore_wait(barrier, n_rel)
                depart(0)
                for copy in load_tgt[1:] + load_late[1:]:
                    copy.wait()
                tid = turn()
            else:
                tid = turn()
                arrive(0)
                weigh(0)
                finish(0)
                depart(0)
            if final > 0:
                arrive(1)
                weigh(1)
            for c in range(1, final + 1):
                if c < final:
                    arrive(c + 1)
                finish(c)
                if c == 1:
                    depart(c)
                if c < final:
                    weigh(c + 1)
                if c > 1:
                    depart(c)
            total = query_part(0, everything)
            for c in range(1, len(plan)):
                total += query_part(c, everything)
            gq_ref[...] = total
            relate(everything, total)
        else:
            def gather_query(c):
                part = query_part(c, everything)
                gq_ref[...] = part if c == 0 else gq_ref[...] + part

            tid = turn()
            if bucket == 0:
                pl.semaphore_wait(barrier, n_rel)
                for copy in load_tgt[1:] + load_late[1:]:
                    copy.wait()
            for c in range(final):
                arrive(c)
                weigh_turned() if bucket == 0 and c == 0 else weigh(c)
                if c > 0:
                    gather_query(c - 1)
                    finish(c - 1)
            if final > 0:
                gather_query(final - 1)
                finish(final - 1)
            arrive(final)
            weigh(final)
            for b, (r, n) in enumerate(blocks):
                part = pl.ds(r, n)
                rel_grad = rel_all[my_rel, part, :] if bucket > 0 else 0.0
                for e, m in groups:
                    some = pl.ds(e, m)
                    whole = query_part(final, part, some)
                    if final > 0:
                        whole = gq_ref[part, some] + whole
                    gq_ref[part, some] = whole
                    g_hi, g_lo = split(whole * picked[part, some])
                    rel_grad += nt(g_hi, rhot[:, some]) + nt(g_lo, rhot[:, some])
                rel_all[my_rel, part, :] = rel_grad
                for step in range(1, n_rel):
                    rel_hop(lax.rem(my_rel + step, n_rel), my_rel, step, b).start()
            finish(final)
        g_hi, g_lo = split(gq_ref[...] * relation[...])
        src_grad = nt(g_hi, hot[...]) + nt(g_lo, hot[...])
        now_srow = srow_ref[...].reshape(1, rows) if bucket == 0 else out_srow[...]
        fresh = now_srow + jnp.sum(src_grad * src_grad, axis=0, keepdims=True) * (1.0 / dims)
        out_src[...] = now_src[...] - src_grad * (learn_rate / (jnp.sqrt(fresh) + epsilon))
        out_srow[...] = fresh

    for bucket in range(buckets - 1):
        for c in range(len(plan)):
            hop(bucket, c).wait_send()
            row_hop(bucket, c).wait_send()
    for b, (r, n) in enumerate(blocks):
        part = pl.ds(r, n)
        for step in range(1, n_rel):
            peer = lax.rem(my_rel + n_rel - step, n_rel)
            arrived = rel_hop(peer, peer, step, b)
            arrived.wait_send()
            arrived.wait_recv()
        total = rel_all[0, part, :]
        for step in range(1, n_rel):
            total = total + rel_all[step, part, :]
        new_state = rstate_ref[part, :] + total * total
        out_rstate[part, :] = new_state
        out_rel[part, :] = rel_ref[part, :] - learn_rate * total / (jnp.sqrt(new_state) + epsilon)


def solution(mesh):
    n_blk, n_rel = mesh.shape["blk"], mesh.shape["rel"]

    def per_device(
        source_table, source_state, target_table, target_state, relation_ops, relation_state,
        source_ids, target_ids, relation_ids, negative_ids,
    ):
        dims, rows = source_table.shape
        rels = relation_ops.shape[1]
        buckets, edges = source_ids.shape
        plan = chunk_plan(rows)
        blocks = row_blocks(dims)
        chunks = len(plan)
        vmem = pl.BlockSpec(memory_space=pltpu.VMEM)
        shape = jax.ShapeDtypeStruct
        moves = [pltpu.VMEM((buckets - 1, dims, width), F32) for _, width in plan]
        out = pl.pallas_call(
            functools.partial(kernel, n_blk, n_rel, plan, blocks),
            out_shape=(
                pltpu.VMEM((dims, rows), F32), pltpu.VMEM((1, rows), F32),
                pltpu.VMEM((dims, rows), F32), pltpu.VMEM((1, rows), F32),
                pltpu.VMEM((dims, rels), F32), pltpu.VMEM((dims, rels), F32),
            ),
            in_specs=[pl.BlockSpec(memory_space=pltpu.HBM)] * 10,
            out_specs=(vmem,) * 6,
            scratch_shapes=[
                pltpu.VMEM((dims, rows), F32), pltpu.VMEM((rows,), F32),
                pltpu.VMEM((dims, rows), F32), pltpu.VMEM((rows,), F32),
                pltpu.VMEM((dims, rels), F32), pltpu.VMEM((dims, rels), F32),
                *[pltpu.VMEM(ids.shape, jnp.int32) for ids in (source_ids, relation_ids, target_ids, negative_ids)],
                pltpu.SemaphoreType.DMA((14,)),
                pltpu.VMEM((rows, edges), BF16),
                pltpu.VMEM((rels, edges), BF16),
                pltpu.VMEM((2, edges, dims), BF16),
                pltpu.VMEM((2, dims, edges), BF16),
                pltpu.VMEM((dims, edges), F32),
                pltpu.VMEM((dims, edges), F32),
                pltpu.VMEM((dims, edges), F32),
                pltpu.VMEM((1, rows), F32),
                pltpu.VMEM((n_rel, dims, rels), F32),
                pltpu.SemaphoreType.DMA((n_rel, len(blocks))),
                pltpu.SemaphoreType.DMA((n_rel, len(blocks))),
                pltpu.SemaphoreType.DMA((2, buckets - 1, chunks)),
                pltpu.SemaphoreType.DMA((2, buckets - 1, chunks)),
                pltpu.VMEM((buckets - 1, chunks, 1, 256), F32),
                pltpu.VMEM((buckets - 1, chunks, 1, 256), F32),
                pltpu.VMEM((2 * LANES, edges), BF16),
                *[pltpu.VMEM((2, dims, 256), BF16) for _ in plan],
                *[pltpu.VMEM((2, edges, 256), BF16) for _ in plan],
                *moves,
                *moves,
            ],
            compiler_params=pltpu.CompilerParams(
                collective_id=0, has_side_effects=True, vmem_limit_bytes=40 * 1024 * 1024
            ),
        )(*(
            pltpu.with_memory_space_constraint(x, pltpu.HBM) for x in (
                source_table, source_state, target_table, target_state,
                relation_ops, relation_state, source_ids, relation_ids,
                target_ids, negative_ids,
            )
        ))
        hbm = pl.BlockSpec(memory_space=pl.ANY)
        return pl.pallas_call(
            emit,
            out_shape=(
                shape((dims, rows), F32), shape((rows,), F32),
                shape((dims, rows), F32), shape((rows,), F32),
                shape((dims, rels), F32), shape((dims, rels), F32),
            ),
            in_specs=[vmem] * 6,
            out_specs=(hbm,) * 6,
            scratch_shapes=[pltpu.VMEM((rows,), F32), pltpu.VMEM((rows,), F32), pltpu.SemaphoreType.DMA((6,))],
            compiler_params=pltpu.CompilerParams(vmem_limit_bytes=16 * 1024 * 1024),
        )(*out)

    split_both = ("blk", "rel")
    return jax.shard_map(
        per_device,
        mesh=mesh,
        in_specs=(
            P(None, split_both), P(split_both), P(None, split_both), P(split_both),
            P(None, "blk"), P(None, "blk"),
            P(None, split_both), P(None, split_both), P(None, split_both), P(None, split_both),
        ),
        out_specs=(
            P(None, split_both), P(split_both), P(None, split_both), P(split_both),
            P(None, "blk"), P(None, "blk"),
        ),
        check_vma=False,
    )
```

```python
import functools

import jax
import jax.numpy as jnp
from jax import lax
from jax.experimental import pallas as pl
from jax.experimental.pallas import tpu as pltpu
from jax.sharding import PartitionSpec as P

learn_rate = 0.1
epsilon = 1e-06
LANES = 128
MESH = pl.DeviceIdType.MESH
F32 = jnp.float32
BF16 = jnp.bfloat16


def split(x):
    high = x.astype(BF16)
    return high, (x - high.astype(F32)).astype(BF16)


def nn(a, b):
    return lax.dot_general(a, b, (((1,), (0,)), ((), ())), preferred_element_type=F32)


def nt(a, b):
    return lax.dot_general(a, b, (((1,), (1,)), ((), ())), preferred_element_type=F32)


def column(row):
    wide = jnp.broadcast_to(row.astype(F32), (8, row.shape[1]))
    return jnp.transpose(wide)[:, :1].astype(jnp.int32)


def one_hot(row, height):
    low = lax.rem(row, LANES)
    inner = (lax.broadcasted_iota(jnp.int32, (LANES, row.shape[1]), 0) == low).astype(F32).astype(BF16)
    if height == LANES:
        return inner
    out = []
    for start in range(0, height, LANES):
        here = (row - low == start).astype(F32).astype(BF16)
        out.append(inner * jnp.broadcast_to(here, inner.shape))
    return jnp.concatenate(out, axis=0)


def chunk_plan(rows):
    if rows % 256 == 0 and rows >= 512:
        widths = [LANES] + [256] * (rows // 256 - 1) + [LANES]
    else:
        widths = [LANES] * (rows // LANES)
    return [(sum(widths[:i]), w) for i, w in enumerate(widths)]


def row_blocks(dims):
    first = dims // 64 * 16
    second = first + (dims - first + 31) // 32 * 16
    return [(0, first), (first, second - first), (second, dims - second)]


def lane_gather(table, index):
    tall = table.shape[0]
    groups = table.shape[1] // LANES
    out = []
    for start in range(0, index.shape[1], LANES):
        one = jnp.broadcast_to(index[:, start:start + LANES], (tall, LANES))
        low = lax.rem(one, LANES)
        got = jnp.take_along_axis(table[:, :LANES], low, axis=1)
        for g in range(1, groups):
            other = jnp.take_along_axis(table[:, g * LANES:(g + 1) * LANES], low, axis=1)
            got = jnp.where(one >= g * LANES, other, got)
        out.append(got)
    return jnp.concatenate(out, axis=1)


def emit(*refs):
    inputs, outputs, (first, second, sem) = refs[:6], refs[6:12], refs[12:]
    copies = []
    for i in (0, 2, 4, 5):
        copies.append(pltpu.make_async_copy(inputs[i], outputs[i], sem.at[i]))
        copies[-1].start()
    for i, line in ((1, first), (3, second)):
        line[...] = inputs[i][0, :]
        copies.append(pltpu.make_async_copy(line, outputs[i], sem.at[i]))
        copies[-1].start()
    for copy in copies:
        copy.wait()


def kernel(n_blk, n_rel, plan, blocks, *refs):
    refs = list(refs)

    def take(n):
        out = refs[:n]
        del refs[:n]
        return out

    src_in, srow_in, tgt_in, trow_in, rel_in, rstate_in, sid_in, rid_in, tid_in, nid_in = take(10)
    out_src, out_srow, out_tgt, out_trow, out_rel, out_rstate = take(6)
    src_ref, srow_ref, tgt_ref, trow_ref, rel_ref, rstate_ref, sid_ref, rid_ref, tid_ref, nid_ref = take(10)
    load_sem, hot, rhot, qt_ref, q_ref, picked, relation, gq_ref, counts, rel_all = take(10)
    rsend_sem, rrecv_sem, send_sem, recv_sem, row_send, row_recv = take(6)
    turned, base_ref, gain_ref = take(3)
    tables, weights = take(len(plan)), take(len(plan))
    send, recv = take(len(plan)), take(len(plan))
    dims, rows = src_ref.shape
    buckets, edges = sid_ref.shape
    negs = nid_ref.shape[1]
    rels = rel_ref.shape[1]
    final = len(plan) - 1
    groups = [(e, min(256, edges - e)) for e in range(0, edges, 256)]
    my_blk = lax.axis_index("blk")
    my_rel = lax.axis_index("rel")
    nxt = lax.rem(my_blk + 1, n_blk)
    prv = lax.rem(my_blk + n_blk - 1, n_blk)

    loads = []

    def load(there, here):
        loads.append(pltpu.make_async_copy(there, here, load_sem.at[len(loads)]))
        loads[-1].start()
        return loads[-1]

    load_ids = [
        load(sid_in, sid_ref), load(rid_in, rid_ref), load(nid_in, nid_ref), load(tid_in, tid_ref)
    ]
    quarter = dims // 64 * 16
    ends = [0, quarter, 2 * quarter, 3 * quarter, dims]
    load_src = [
        load(src_in.at[pl.ds(r, n - r)], src_ref.at[pl.ds(r, n - r)]) for r, n in zip(ends[:2], ends[1:3])
    ]
    load_rel = load(rel_in, rel_ref)
    load_src += [
        load(src_in.at[pl.ds(r, n - r)], src_ref.at[pl.ds(r, n - r)]) for r, n in zip(ends[2:4], ends[3:])
    ]
    wide = plan[0][1]
    load_first = [load(tgt_in.at[:, pl.ds(0, wide)], tgt_ref.at[:, pl.ds(0, wide)]), load(trow_in, trow_ref)]
    load_rest = []

    barrier = pltpu.get_barrier_semaphore()
    pl.semaphore_signal(barrier, inc=1, device_id={"blk": prv}, device_id_type=MESH)
    for step in range(1, n_rel):
        pl.semaphore_signal(
            barrier, inc=1, device_id={"rel": lax.rem(my_rel + step, n_rel)}, device_id_type=MESH
        )

    def hop(bucket, c):
        return pltpu.make_async_remote_copy(
            src_ref=send[c].at[bucket],
            dst_ref=recv[c].at[bucket],
            send_sem=send_sem.at[0, bucket, c],
            recv_sem=recv_sem.at[0, bucket, c],
            device_id={"blk": nxt},
            device_id_type=MESH,
        )

    def row_hop(bucket, c):
        return pltpu.make_async_remote_copy(
            src_ref=row_send.at[bucket, c, :, pl.ds(0, plan[c][1])],
            dst_ref=row_recv.at[bucket, c, :, pl.ds(0, plan[c][1])],
            send_sem=send_sem.at[1, bucket, c],
            recv_sem=recv_sem.at[1, bucket, c],
            device_id={"blk": nxt},
            device_id_type=MESH,
        )

    def rel_hop(to, slot, step, b):
        r, n = blocks[b]
        return pltpu.make_async_remote_copy(
            src_ref=rel_all.at[slot, pl.ds(r, n)],
            dst_ref=rel_all.at[slot, pl.ds(r, n)],
            send_sem=rsend_sem.at[step - 1, b],
            recv_sem=rrecv_sem.at[slot, b],
            device_id={"rel": to},
            device_id_type=MESH,
        )

    def put_pair(ref, hi, lo, twice, part=slice(None)):
        width = hi.shape[1]
        if width == LANES:
            ref[0, part, :LANES] = hi
            ref[0, part, LANES:] = lo
            if twice:
                ref[1, :, :LANES] = hi
                ref[1, :, LANES:] = hi
        else:
            ref[0, part, :] = hi
            ref[1, part, :] = lo

    def fold(wide):
        return wide[:, :LANES] + wide[:, LANES:]

    for copy in load_ids:
        copy.wait()

    for bucket in range(buckets):
        last = bucket + 1 == buckets
        now_src = src_ref if bucket == 0 else out_src
        sid = sid_ref[pl.ds(bucket, 1), :]
        rid = rid_ref[pl.ds(bucket, 1), :]
        hot[...] = one_hot(sid, rows)
        for first in (0, 2):
            part = pl.ds(ends[first], ends[first + 2] - ends[first])
            if bucket == 0:
                for copy in load_src[first:first + 2]:
                    copy.wait()
                if first:
                    for copy in [load_rel] + load_first:
                        copy.wait()
                    if rows > wide:
                        late = pl.ds(wide, rows - wide)
                        load_rest.append(load(tgt_in.at[:, late], tgt_ref.at[:, late]))
                    load_rest.extend([load(srow_in, srow_ref), load(rstate_in, rstate_ref)])
            s_hi, s_lo = split(now_src[part, :])
            for e, m in groups:
                some = pl.ds(e, m)
                picked[part, some] = nn(s_hi, hot[:, some]) + nn(s_lo, hot[:, some])
        relation[...] = lane_gather(rel_ref[...], rid)
        for e, m in groups:
            some = pl.ds(e, m)
            hi, lo = split(picked[:, some] * relation[:, some])
            q_ref[0, :, some] = hi
            q_ref[1, :, some] = lo

        def turn():
            for e, m in groups:
                some = pl.ds(e, m)
                hi, lo = split(jnp.transpose(picked[:, some] * relation[:, some] * 0.5))
                qt_ref[0, some, :] = hi
                qt_ref[1, some, :] = lo
            nid = column(nid_ref[pl.ds(bucket, 1), :])
            for start in range(0, rows, LANES):
                lane = lax.broadcasted_iota(jnp.int32, (negs, LANES), 1) + start
                counts[:, pl.ds(start, LANES)] = jnp.sum(
                    (lane == nid).astype(F32), axis=0, keepdims=True
                ) * (0.5 / negs)
            rhot[...] = one_hot(rid, rels)
            return column(tid_ref[pl.ds(bucket, 1), :])

        def weigh_turned():
            table = tgt_ref[:, :LANES]
            hi, lo = split(table)
            put_pair(tables[0], hi, lo, True)
            hi, lo = split(jnp.transpose(table) * 0.5)
            wide = nn(jnp.concatenate([hi, lo], axis=0), q_ref[0])
            score = wide[:LANES] + wide[LANES:] + nn(hi, q_ref[1])
            half = jnp.tanh(score)
            here = lax.broadcasted_iota(jnp.int32, (LANES, negs), 0) == nid_ref[pl.ds(bucket, 1), :]
            count = jnp.sum(here.astype(F32), axis=1, keepdims=True) * (0.5 / negs)
            here = lax.broadcasted_iota(jnp.int32, (LANES, edges), 0) == tid_ref[pl.ds(bucket, 1), :]
            weight = count * half + count - jnp.where(here, 0.5 - 0.5 * half, 0.0)
            hi, lo = split(weight)
            turned[:LANES, :] = hi
            turned[LANES:, :] = lo

        base, gain = {}, {}

        def prepare(c):
            start, width = plan[c]
            count = counts[:, pl.ds(start, width)]
            base[c], gain[c] = {}, {}
            for e, m in groups:
                own = lax.broadcasted_iota(jnp.int32, (m, width), 1) + start == tid[e:e + m]
                half = jnp.where(own, 0.5, 0.0)
                base[c][e], gain[c][e] = count - half, count + half
                if c == final and bucket > 0:
                    base_ref[e:e + m, :], gain_ref[e:e + m, :] = base[c][e], gain[c][e]

        def weigh(c):
            start, width = plan[c]
            if c == final and bucket > 0:
                for e, m in groups:
                    base[c][e], gain[c][e] = base_ref[e:e + m, :], gain_ref[e:e + m, :]
            else:
                prepare(c)
            cols = pl.ds(start, width)
            table = tgt_ref[:, cols] if bucket == 0 else recv[c][bucket - 1]
            t_hi, t_lo = split(table)
            put_pair(tables[c], t_hi, t_lo, True)
            for e, m in groups:
                some = pl.ds(e, m)
                if width == LANES:
                    score = fold(nn(qt_ref[0, some, :], tables[c][0])) + nn(qt_ref[1, some, :], t_hi)
                else:
                    score = (
                        nn(qt_ref[0, some, :], t_hi) + nn(qt_ref[0, some, :], t_lo) + nn(qt_ref[1, some, :], t_hi)
                    )
                half = jnp.tanh(score)
                weight = base[c][e] + gain[c][e] * half
                w_hi, w_lo = split(weight)
                put_pair(weights[c], w_hi, w_lo, False, some)

        def query_part(c, part, some=slice(None)):
            if bucket == 0 and c == 0:
                return (
                    nn(tables[c][1, part, :], turned[:, some])
                    + nn(tables[c][0, part, LANES:], turned[:LANES, some])
                )
            if plan[c][1] == LANES:
                return (
                    nt(tables[c][1, part, :], weights[c][0, some, :])
                    + nt(tables[c][0, part, LANES:], weights[c][0, some, :LANES])
                )
            return (
                nt(tables[c][0, part, :], weights[c][0, some, :])
                + nt(tables[c][0, part, :], weights[c][1, some, :])
                + nt(tables[c][1, part, :], weights[c][0, some, :])
            )

        def finish(c):
            start, width = plan[c]
            cols = pl.ds(start, width)
            if bucket == 0:
                table = tgt_ref[:, cols]
                state = trow_ref[cols].reshape(1, width)
            else:
                if c == final:
                    row_hop(bucket - 1, c).wait_recv()
                table = recv[c][bucket - 1]
                state = row_recv[bucket - 1, c, :, :width]
            if bucket == 0 and c == 0:
                grad = fold(nt(q_ref[0], turned[...])) + nt(q_ref[1], turned[:LANES, :])
            elif width == LANES:
                grad = fold(nn(q_ref[0], weights[c][0])) + nn(q_ref[1], weights[c][0, :, :LANES])
            else:
                grad = nn(q_ref[0], weights[c][0]) + nn(q_ref[0], weights[c][1]) + nn(q_ref[1], weights[c][0])
            fresh = state + jnp.sum(grad * grad, axis=0, keepdims=True) * (1.0 / dims)
            new = table - grad * (learn_rate / (jnp.sqrt(fresh) + epsilon))
            if last:
                out_tgt[:, cols] = new
                out_trow[:, cols] = fresh
            else:
                send[c][bucket] = new
                row_send[bucket, c, :, :width] = fresh

        def relate(part, whole):
            g_hi, g_lo = split(whole * picked[part, :])
            rel_grad = nt(g_hi, rhot[...]) + nt(g_lo, rhot[...])
            if bucket == 0:
                rel_all[my_rel, part, :] = rel_grad
            else:
                rel_all[my_rel, part, :] = rel_all[my_rel, part, :] + rel_grad

        everything = pl.ds(0, dims)

        def arrive(c):
            if bucket > 0:
                hop(bucket - 1, c).wait_recv()
                if c < final:
                    row_hop(bucket - 1, c).wait_recv()

        def depart(c):
            row_hop(bucket, c).start()
            hop(bucket, c).start()

        if not last:
            if bucket == 0:
                weigh_turned()
                finish(0)
                pl.semaphore_wait(barrier, n_rel)
                depart(0)
                for copy in load_rest:
                    copy.wait()
                tid = turn()
            else:
                tid = turn()
                arrive(0)
                weigh(0)
                finish(0)
                depart(0)
            if final > 0:
                arrive(1)
                weigh(1)
            for c in range(1, final + 1):
                if c < final:
                    arrive(c + 1)
                finish(c)
                if c == 1:
                    depart(c)
                if c < final:
                    weigh(c + 1)
                if c > 1:
                    depart(c)
            total = query_part(0, everything)
            for c in range(1, len(plan)):
                total += query_part(c, everything)
            gq_ref[...] = total
            relate(everything, total)
        else:
            def gather_query(c):
                part = query_part(c, everything)
                gq_ref[...] = part if c == 0 else gq_ref[...] + part

            tid = turn()
            if bucket == 0:
                pl.semaphore_wait(barrier, n_rel)
                for copy in load_rest:
                    copy.wait()
            for c in range(final):
                arrive(c)
                weigh_turned() if bucket == 0 and c == 0 else weigh(c)
                if c > 0:
                    gather_query(c - 1)
                    finish(c - 1)
            if final > 0:
                gather_query(final - 1)
                finish(final - 1)
            if bucket > 0:
                prepare(final)
            arrive(final)
            weigh(final)
            for b, (r, n) in enumerate(blocks):
                part = pl.ds(r, n)
                rel_grad = rel_all[my_rel, part, :] if bucket > 0 else 0.0
                for e, m in groups:
                    some = pl.ds(e, m)
                    whole = query_part(final, part, some)
                    if final > 0:
                        whole = gq_ref[part, some] + whole
                    gq_ref[part, some] = whole
                    g_hi, g_lo = split(whole * picked[part, some])
                    rel_grad += nt(g_hi, rhot[:, some]) + nt(g_lo, rhot[:, some])
                rel_all[my_rel, part, :] = rel_grad
                for step in range(1, n_rel):
                    rel_hop(lax.rem(my_rel + step, n_rel), my_rel, step, b).start()
            finish(final)
        g_hi, g_lo = split(gq_ref[...] * relation[...])
        src_grad = nt(g_hi, hot[...]) + nt(g_lo, hot[...])
        now_srow = srow_ref[...].reshape(1, rows) if bucket == 0 else out_srow[...]
        fresh = now_srow + jnp.sum(src_grad * src_grad, axis=0, keepdims=True) * (1.0 / dims)
        out_src[...] = now_src[...] - src_grad * (learn_rate / (jnp.sqrt(fresh) + epsilon))
        out_srow[...] = fresh

    for bucket in range(buckets - 1):
        for c in range(len(plan)):
            hop(bucket, c).wait_send()
            row_hop(bucket, c).wait_send()
    for b, (r, n) in enumerate(blocks):
        part = pl.ds(r, n)
        for step in range(1, n_rel):
            peer = lax.rem(my_rel + n_rel - step, n_rel)
            arrived = rel_hop(peer, peer, step, b)
            arrived.wait_send()
            arrived.wait_recv()
        total = rel_all[0, part, :]
        for step in range(1, n_rel):
            total = total + rel_all[step, part, :]
        new_state = rstate_ref[part, :] + total * total
        out_rstate[part, :] = new_state
        out_rel[part, :] = rel_ref[part, :] - learn_rate * total / (jnp.sqrt(new_state) + epsilon)


def solution(mesh):
    n_blk, n_rel = mesh.shape["blk"], mesh.shape["rel"]

    def per_device(
        source_table, source_state, target_table, target_state, relation_ops, relation_state,
        source_ids, target_ids, relation_ids, negative_ids,
    ):
        dims, rows = source_table.shape
        rels = relation_ops.shape[1]
        buckets, edges = source_ids.shape
        plan = chunk_plan(rows)
        blocks = row_blocks(dims)
        chunks = len(plan)
        vmem = pl.BlockSpec(memory_space=pltpu.VMEM)
        shape = jax.ShapeDtypeStruct
        moves = [pltpu.VMEM((buckets - 1, dims, width), F32) for _, width in plan]
        out = pl.pallas_call(
            functools.partial(kernel, n_blk, n_rel, plan, blocks),
            out_shape=(
                pltpu.VMEM((dims, rows), F32), pltpu.VMEM((1, rows), F32),
                pltpu.VMEM((dims, rows), F32), pltpu.VMEM((1, rows), F32),
                pltpu.VMEM((dims, rels), F32), pltpu.VMEM((dims, rels), F32),
            ),
            in_specs=[pl.BlockSpec(memory_space=pltpu.HBM)] * 10,
            out_specs=(vmem,) * 6,
            scratch_shapes=[
                pltpu.VMEM((dims, rows), F32), pltpu.VMEM((rows,), F32),
                pltpu.VMEM((dims, rows), F32), pltpu.VMEM((rows,), F32),
                pltpu.VMEM((dims, rels), F32), pltpu.VMEM((dims, rels), F32),
                *[pltpu.VMEM(ids.shape, jnp.int32) for ids in (source_ids, relation_ids, target_ids, negative_ids)],
                pltpu.SemaphoreType.DMA((14,)),
                pltpu.VMEM((rows, edges), BF16),
                pltpu.VMEM((rels, edges), BF16),
                pltpu.VMEM((2, edges, dims), BF16),
                pltpu.VMEM((2, dims, edges), BF16),
                pltpu.VMEM((dims, edges), F32),
                pltpu.VMEM((dims, edges), F32),
                pltpu.VMEM((dims, edges), F32),
                pltpu.VMEM((1, rows), F32),
                pltpu.VMEM((n_rel, dims, rels), F32),
                pltpu.SemaphoreType.DMA((n_rel, len(blocks))),
                pltpu.SemaphoreType.DMA((n_rel, len(blocks))),
                pltpu.SemaphoreType.DMA((2, buckets - 1, chunks)),
                pltpu.SemaphoreType.DMA((2, buckets - 1, chunks)),
                pltpu.VMEM((buckets - 1, chunks, 1, 256), F32),
                pltpu.VMEM((buckets - 1, chunks, 1, 256), F32),
                pltpu.VMEM((2 * LANES, edges), BF16),
                pltpu.VMEM((edges, plan[-1][1]), F32),
                pltpu.VMEM((edges, plan[-1][1]), F32),
                *[pltpu.VMEM((2, dims, 256), BF16) for _ in plan],
                *[pltpu.VMEM((2, edges, 256), BF16) for _ in plan],
                *moves,
                *moves,
            ],
            compiler_params=pltpu.CompilerParams(
                collective_id=0, has_side_effects=True, vmem_limit_bytes=40 * 1024 * 1024
            ),
        )(*(
            pltpu.with_memory_space_constraint(x, pltpu.HBM) for x in (
                source_table, source_state, target_table, target_state,
                relation_ops, relation_state, source_ids, relation_ids,
                target_ids, negative_ids,
            )
        ))
        hbm = pl.BlockSpec(memory_space=pl.ANY)
        return pl.pallas_call(
            emit,
            out_shape=(
                shape((dims, rows), F32), shape((rows,), F32),
                shape((dims, rows), F32), shape((rows,), F32),
                shape((dims, rels), F32), shape((dims, rels), F32),
            ),
            in_specs=[vmem] * 6,
            out_specs=(hbm,) * 6,
            scratch_shapes=[pltpu.VMEM((rows,), F32), pltpu.VMEM((rows,), F32), pltpu.SemaphoreType.DMA((6,))],
            compiler_params=pltpu.CompilerParams(vmem_limit_bytes=16 * 1024 * 1024),
        )(*out)

    split_both = ("blk", "rel")
    return jax.shard_map(
        per_device,
        mesh=mesh,
        in_specs=(
            P(None, split_both), P(split_both), P(None, split_both), P(split_both),
            P(None, "blk"), P(None, "blk"),
            P(None, split_both), P(None, split_both), P(None, split_both), P(None, split_both),
        ),
        out_specs=(
            P(None, split_both), P(split_both), P(None, split_both), P(split_both),
            P(None, "blk"), P(None, "blk"),
        ),
        check_vma=False,
    )
```

```python
import functools

import jax
import jax.numpy as jnp
from jax import lax
from jax.experimental import pallas as pl
from jax.experimental.pallas import tpu as pltpu
from jax.sharding import PartitionSpec as P

learn_rate = 0.1
epsilon = 1e-06
LANES = 128
MESH = pl.DeviceIdType.MESH
F32 = jnp.float32
BF16 = jnp.bfloat16


def split(x):
    high = x.astype(BF16)
    return high, (x - high.astype(F32)).astype(BF16)


def nn(a, b):
    return lax.dot_general(a, b, (((1,), (0,)), ((), ())), preferred_element_type=F32)


def nt(a, b):
    return lax.dot_general(a, b, (((1,), (1,)), ((), ())), preferred_element_type=F32)


def both_nn(hi, lo, b):
    n = hi.shape[0]
    tall = nn(jnp.concatenate([hi, lo], axis=0), b)
    return tall[:n] + tall[n:]


def both_nt(hi, lo, b):
    n = hi.shape[0]
    tall = nt(jnp.concatenate([hi, lo], axis=0), b)
    return tall[:n] + tall[n:]


def column(row):
    wide = jnp.broadcast_to(row.astype(F32), (8, row.shape[1]))
    return jnp.transpose(wide)[:, :1].astype(jnp.int32)


def one_hot(row, height):
    low = lax.rem(row, LANES)
    inner = (lax.broadcasted_iota(jnp.int32, (LANES, row.shape[1]), 0) == low).astype(F32).astype(BF16)
    if height == LANES:
        return inner
    out = []
    for start in range(0, height, LANES):
        here = (row - low == start).astype(F32).astype(BF16)
        out.append(inner * jnp.broadcast_to(here, inner.shape))
    return jnp.concatenate(out, axis=0)


def chunk_plan(rows):
    if rows % 256 == 0 and rows >= 512:
        widths = [LANES] + [256] * (rows // 256 - 1) + [LANES]
    else:
        widths = [LANES] * (rows // LANES)
    return [(sum(widths[:i]), w) for i, w in enumerate(widths)]


def row_blocks(dims):
    first = dims // 128 * 16
    second = first + dims // 64 * 16
    third = second + (dims - second + 31) // 32 * 16
    return [(0, first), (first, second - first), (second, third - second), (third, dims - third)]


def lane_gather(table, index):
    tall = table.shape[0]
    groups = table.shape[1] // LANES
    out = []
    for start in range(0, index.shape[1], LANES):
        one = jnp.broadcast_to(index[:, start:start + LANES], (tall, LANES))
        low = lax.rem(one, LANES)
        got = jnp.take_along_axis(table[:, :LANES], low, axis=1)
        for g in range(1, groups):
            other = jnp.take_along_axis(table[:, g * LANES:(g + 1) * LANES], low, axis=1)
            got = jnp.where(one >= g * LANES, other, got)
        out.append(got)
    return jnp.concatenate(out, axis=1)


def emit(*refs):
    inputs, outputs, (first, second, sem) = refs[:6], refs[6:12], refs[12:]
    copies = []
    for i in (0, 2, 4, 5):
        copies.append(pltpu.make_async_copy(inputs[i], outputs[i], sem.at[i]))
        copies[-1].start()
    for i, line in ((1, first), (3, second)):
        line[...] = inputs[i][0, :]
        copies.append(pltpu.make_async_copy(line, outputs[i], sem.at[i]))
        copies[-1].start()
    for copy in copies:
        copy.wait()


def kernel(n_blk, n_rel, plan, blocks, *refs):
    refs = list(refs)

    def take(n):
        out = refs[:n]
        del refs[:n]
        return out

    src_in, srow_in, tgt_in, trow_in, rel_in, rstate_in, sid_in, rid_in, tid_in, nid_in = take(10)
    out_src, out_srow, out_tgt, out_trow, out_rel, out_rstate = take(6)
    src_ref, srow_ref, tgt_ref, trow_ref, rel_ref, rstate_ref, sid_ref, rid_ref, tid_ref, nid_ref = take(10)
    load_sem, hot, rhot, qt_ref, q_ref, picked, relation, gq_ref, counts, rel_all = take(10)
    rsend_sem, rrecv_sem, send_sem, recv_sem, row_send, row_recv = take(6)
    turned, base_ref, gain_ref = take(3)
    tables, weights = take(len(plan)), take(len(plan))
    send, recv = take(len(plan)), take(len(plan))
    dims, rows = src_ref.shape
    buckets, edges = sid_ref.shape
    negs = nid_ref.shape[1]
    rels = rel_ref.shape[1]
    final = len(plan) - 1
    groups = [(e, min(256, edges - e)) for e in range(0, edges, 256)]
    my_blk = lax.axis_index("blk")
    my_rel = lax.axis_index("rel")
    nxt = lax.rem(my_blk + 1, n_blk)
    prv = lax.rem(my_blk + n_blk - 1, n_blk)

    loads = []

    def load(there, here):
        loads.append(pltpu.make_async_copy(there, here, load_sem.at[len(loads)]))
        loads[-1].start()
        return loads[-1]

    load_ids = [
        load(sid_in, sid_ref), load(rid_in, rid_ref), load(nid_in, nid_ref), load(tid_in, tid_ref)
    ]
    quarter = dims // 64 * 16
    ends = [0, quarter, 2 * quarter, 3 * quarter, dims]
    load_src = [
        load(src_in.at[pl.ds(r, n - r)], src_ref.at[pl.ds(r, n - r)]) for r, n in zip(ends[:2], ends[1:3])
    ]
    load_rel = load(rel_in, rel_ref)
    load_src += [
        load(src_in.at[pl.ds(r, n - r)], src_ref.at[pl.ds(r, n - r)]) for r, n in zip(ends[2:4], ends[3:])
    ]
    wide = plan[0][1]
    load_first = [load(tgt_in.at[:, pl.ds(0, wide)], tgt_ref.at[:, pl.ds(0, wide)]), load(trow_in, trow_ref)]
    load_rest = []

    barrier = pltpu.get_barrier_semaphore()
    pl.semaphore_signal(barrier, inc=1, device_id={"blk": prv}, device_id_type=MESH)
    for step in range(1, n_rel):
        pl.semaphore_signal(
            barrier, inc=1, device_id={"rel": lax.rem(my_rel + step, n_rel)}, device_id_type=MESH
        )

    def hop(bucket, c):
        return pltpu.make_async_remote_copy(
            src_ref=send[c].at[bucket],
            dst_ref=recv[c].at[bucket],
            send_sem=send_sem.at[0, bucket, c],
            recv_sem=recv_sem.at[0, bucket, c],
            device_id={"blk": nxt},
            device_id_type=MESH,
        )

    def row_hop(bucket, c):
        return pltpu.make_async_remote_copy(
            src_ref=row_send.at[bucket, c, :, pl.ds(0, plan[c][1])],
            dst_ref=row_recv.at[bucket, c, :, pl.ds(0, plan[c][1])],
            send_sem=send_sem.at[1, bucket, c],
            recv_sem=recv_sem.at[1, bucket, c],
            device_id={"blk": nxt},
            device_id_type=MESH,
        )

    def rel_hop(to, slot, step, b):
        r, n = blocks[b]
        return pltpu.make_async_remote_copy(
            src_ref=rel_all.at[slot, pl.ds(r, n)],
            dst_ref=rel_all.at[slot, pl.ds(r, n)],
            send_sem=rsend_sem.at[step - 1, b],
            recv_sem=rrecv_sem.at[slot, b],
            device_id={"rel": to},
            device_id_type=MESH,
        )

    def put_pair(ref, hi, lo, twice, part=slice(None)):
        width = hi.shape[1]
        if width == LANES:
            ref[0, part, :LANES] = hi
            ref[0, part, LANES:] = lo
            if twice:
                ref[1, :, :LANES] = hi
                ref[1, :, LANES:] = hi
        else:
            ref[0, part, :] = hi
            ref[1, part, :] = lo

    def fold(wide):
        return wide[:, :LANES] + wide[:, LANES:]

    for copy in load_ids:
        copy.wait()

    for bucket in range(buckets):
        last = bucket + 1 == buckets
        now_src = src_ref if bucket == 0 else out_src
        sid = sid_ref[pl.ds(bucket, 1), :]
        rid = rid_ref[pl.ds(bucket, 1), :]
        hot[...] = one_hot(sid, rows)
        for first in (0, 2):
            part = pl.ds(ends[first], ends[first + 2] - ends[first])
            if bucket == 0:
                for copy in load_src[first:first + 2]:
                    copy.wait()
                if first:
                    for copy in [load_rel] + load_first:
                        copy.wait()
                    if rows > wide:
                        late = pl.ds(wide, rows - wide)
                        load_rest.append(load(tgt_in.at[:, late], tgt_ref.at[:, late]))
                    load_rest.extend([load(srow_in, srow_ref), load(rstate_in, rstate_ref)])
            s_hi, s_lo = split(now_src[part, :])
            for e, m in groups:
                some = pl.ds(e, m)
                picked[part, some] = both_nn(s_hi, s_lo, hot[:, some])
        relation[...] = lane_gather(rel_ref[...], rid)
        for e, m in groups:
            some = pl.ds(e, m)
            hi, lo = split(picked[:, some] * relation[:, some])
            q_ref[0, :, some] = hi
            q_ref[1, :, some] = lo

        def turn():
            for e, m in groups:
                some = pl.ds(e, m)
                hi, lo = split(jnp.transpose(picked[:, some] * relation[:, some] * 0.5))
                qt_ref[0, some, :] = hi
                qt_ref[1, some, :] = lo
            nid = column(nid_ref[pl.ds(bucket, 1), :])
            for start in range(0, rows, LANES):
                lane = lax.broadcasted_iota(jnp.int32, (negs, LANES), 1) + start
                counts[:, pl.ds(start, LANES)] = jnp.sum(
                    (lane == nid).astype(F32), axis=0, keepdims=True
                ) * (0.5 / negs)
            rhot[...] = one_hot(rid, rels)
            return column(tid_ref[pl.ds(bucket, 1), :])

        def weigh_turned():
            table = tgt_ref[:, :LANES]
            hi, lo = split(table)
            put_pair(tables[0], hi, lo, True)
            hi, lo = split(jnp.transpose(table) * 0.5)
            wide = nn(jnp.concatenate([hi, lo], axis=0), q_ref[0])
            score = wide[:LANES] + wide[LANES:] + nn(hi, q_ref[1])
            half = jnp.tanh(score)
            here = lax.broadcasted_iota(jnp.int32, (LANES, negs), 0) == nid_ref[pl.ds(bucket, 1), :]
            count = jnp.sum(here.astype(F32), axis=1, keepdims=True) * (0.5 / negs)
            here = lax.broadcasted_iota(jnp.int32, (LANES, edges), 0) == tid_ref[pl.ds(bucket, 1), :]
            weight = count * half + count - jnp.where(here, 0.5 - 0.5 * half, 0.0)
            hi, lo = split(weight)
            turned[:LANES, :] = hi
            turned[LANES:, :] = lo

        base, gain = {}, {}

        def prepare(c):
            start, width = plan[c]
            count = counts[:, pl.ds(start, width)]
            base[c], gain[c] = {}, {}
            for e, m in groups:
                own = lax.broadcasted_iota(jnp.int32, (m, width), 1) + start == tid[e:e + m]
                half = jnp.where(own, 0.5, 0.0)
                base[c][e], gain[c][e] = count - half, count + half
                if c == final and bucket > 0:
                    base_ref[e:e + m, :], gain_ref[e:e + m, :] = base[c][e], gain[c][e]

        def weigh(c):
            start, width = plan[c]
            if c == final and bucket > 0:
                for e, m in groups:
                    base[c][e], gain[c][e] = base_ref[e:e + m, :], gain_ref[e:e + m, :]
            else:
                prepare(c)
            cols = pl.ds(start, width)
            table = tgt_ref[:, cols] if bucket == 0 else recv[c][bucket - 1]
            t_hi, t_lo = split(table)
            put_pair(tables[c], t_hi, t_lo, True)
            for e, m in groups:
                some = pl.ds(e, m)
                if width == LANES:
                    score = fold(nn(qt_ref[0, some, :], tables[c][0])) + nn(qt_ref[1, some, :], t_hi)
                else:
                    score = (
                        both_nn(qt_ref[0, some, :], qt_ref[1, some, :], t_hi) + nn(qt_ref[0, some, :], t_lo)
                    )
                half = jnp.tanh(score)
                weight = base[c][e] + gain[c][e] * half
                w_hi, w_lo = split(weight)
                put_pair(weights[c], w_hi, w_lo, False, some)

        def query_part(c, part, some=slice(None)):
            if bucket == 0 and c == 0:
                return (
                    nn(tables[c][1, part, :], turned[:, some])
                    + nn(tables[c][0, part, LANES:], turned[:LANES, some])
                )
            if plan[c][1] == LANES:
                return (
                    nt(tables[c][1, part, :], weights[c][0, some, :])
                    + nt(tables[c][0, part, LANES:], weights[c][0, some, :LANES])
                )
            return (
                both_nt(tables[c][0, part, :], tables[c][1, part, :], weights[c][0, some, :])
                + nt(tables[c][0, part, :], weights[c][1, some, :])
            )

        def finish(c):
            start, width = plan[c]
            cols = pl.ds(start, width)
            if bucket == 0:
                table = tgt_ref[:, cols]
                state = trow_ref[cols].reshape(1, width)
            else:
                if c == final:
                    row_hop(bucket - 1, c).wait_recv()
                table = recv[c][bucket - 1]
                state = row_recv[bucket - 1, c, :, :width]
            if bucket == 0 and c == 0:
                grad = fold(nt(q_ref[0], turned[...])) + nt(q_ref[1], turned[:LANES, :])
            elif width == LANES:
                grad = fold(nn(q_ref[0], weights[c][0])) + nn(q_ref[1], weights[c][0, :, :LANES])
            else:
                grad = both_nn(q_ref[0], q_ref[1], weights[c][0]) + nn(q_ref[0], weights[c][1])
            fresh = state + jnp.sum(grad * grad, axis=0, keepdims=True) * (1.0 / dims)
            new = table - grad * (learn_rate / (jnp.sqrt(fresh) + epsilon))
            if last:
                out_tgt[:, cols] = new
                out_trow[:, cols] = fresh
            else:
                send[c][bucket] = new
                row_send[bucket, c, :, :width] = fresh

        def relate(part, whole):
            g_hi, g_lo = split(whole * picked[part, :])
            rel_grad = both_nt(g_hi, g_lo, rhot[...])
            if bucket == 0:
                rel_all[my_rel, part, :] = rel_grad
            else:
                rel_all[my_rel, part, :] = rel_all[my_rel, part, :] + rel_grad

        everything = pl.ds(0, dims)

        def arrive(c):
            if bucket > 0:
                hop(bucket - 1, c).wait_recv()
                if c < final:
                    row_hop(bucket - 1, c).wait_recv()

        def depart(c):
            row_hop(bucket, c).start()
            hop(bucket, c).start()

        if not last:
            if bucket == 0:
                weigh_turned()
                finish(0)
                pl.semaphore_wait(barrier, n_rel)
                depart(0)
                for copy in load_rest:
                    copy.wait()
                tid = turn()
            else:
                tid = turn()
                arrive(0)
                weigh(0)
                finish(0)
                depart(0)
            if final > 0:
                arrive(1)
                weigh(1)
            for c in range(1, final + 1):
                if c < final:
                    arrive(c + 1)
                finish(c)
                if c == 1:
                    depart(c)
                if c < final:
                    weigh(c + 1)
                if c > 1:
                    depart(c)
            total = query_part(0, everything)
            for c in range(1, len(plan)):
                total += query_part(c, everything)
            gq_ref[...] = total
            relate(everything, total)
        else:
            def gather_query(c):
                part = query_part(c, everything)
                gq_ref[...] = part if c == 0 else gq_ref[...] + part

            tid = turn()
            if bucket == 0:
                pl.semaphore_wait(barrier, n_rel)
                for copy in load_rest:
                    copy.wait()
            for c in range(final):
                arrive(c)
                weigh_turned() if bucket == 0 and c == 0 else weigh(c)
                if c > 0:
                    gather_query(c - 1)
                    finish(c - 1)
            if final > 0:
                gather_query(final - 1)
                finish(final - 1)
            if bucket > 0:
                prepare(final)
            arrive(final)
            weigh(final)
            for b, (r, n) in enumerate(blocks):
                part = pl.ds(r, n)
                rel_grad = rel_all[my_rel, part, :] if bucket > 0 else 0.0
                for e, m in groups:
                    some = pl.ds(e, m)
                    whole = query_part(final, part, some)
                    if final > 0:
                        whole = gq_ref[part, some] + whole
                    gq_ref[part, some] = whole
                    g_hi, g_lo = split(whole * picked[part, some])
                    rel_grad += both_nt(g_hi, g_lo, rhot[:, some])
                rel_all[my_rel, part, :] = rel_grad
                for step in range(1, n_rel):
                    rel_hop(lax.rem(my_rel + step, n_rel), my_rel, step, b).start()
            finish(final)
        g_hi, g_lo = split(gq_ref[...] * relation[...])
        src_grad = both_nt(g_hi, g_lo, hot[...])
        now_srow = srow_ref[...].reshape(1, rows) if bucket == 0 else out_srow[...]
        fresh = now_srow + jnp.sum(src_grad * src_grad, axis=0, keepdims=True) * (1.0 / dims)
        out_src[...] = now_src[...] - src_grad * (learn_rate / (jnp.sqrt(fresh) + epsilon))
        out_srow[...] = fresh

    for bucket in range(buckets - 1):
        for c in range(len(plan)):
            hop(bucket, c).wait_send()
            row_hop(bucket, c).wait_send()
    for b, (r, n) in enumerate(blocks):
        part = pl.ds(r, n)
        for step in range(1, n_rel):
            peer = lax.rem(my_rel + n_rel - step, n_rel)
            arrived = rel_hop(peer, peer, step, b)
            arrived.wait_send()
            arrived.wait_recv()
        total = rel_all[0, part, :]
        for step in range(1, n_rel):
            total = total + rel_all[step, part, :]
        new_state = rstate_ref[part, :] + total * total
        out_rstate[part, :] = new_state
        out_rel[part, :] = rel_ref[part, :] - learn_rate * total / (jnp.sqrt(new_state) + epsilon)


def solution(mesh):
    n_blk, n_rel = mesh.shape["blk"], mesh.shape["rel"]

    def per_device(
        source_table, source_state, target_table, target_state, relation_ops, relation_state,
        source_ids, target_ids, relation_ids, negative_ids,
    ):
        dims, rows = source_table.shape
        rels = relation_ops.shape[1]
        buckets, edges = source_ids.shape
        plan = chunk_plan(rows)
        blocks = row_blocks(dims)
        chunks = len(plan)
        vmem = pl.BlockSpec(memory_space=pltpu.VMEM)
        shape = jax.ShapeDtypeStruct
        moves = [pltpu.VMEM((buckets - 1, dims, width), F32) for _, width in plan]
        out = pl.pallas_call(
            functools.partial(kernel, n_blk, n_rel, plan, blocks),
            out_shape=(
                pltpu.VMEM((dims, rows), F32), pltpu.VMEM((1, rows), F32),
                pltpu.VMEM((dims, rows), F32), pltpu.VMEM((1, rows), F32),
                pltpu.VMEM((dims, rels), F32), pltpu.VMEM((dims, rels), F32),
            ),
            in_specs=[pl.BlockSpec(memory_space=pltpu.HBM)] * 10,
            out_specs=(vmem,) * 6,
            scratch_shapes=[
                pltpu.VMEM((dims, rows), F32), pltpu.VMEM((rows,), F32),
                pltpu.VMEM((dims, rows), F32), pltpu.VMEM((rows,), F32),
                pltpu.VMEM((dims, rels), F32), pltpu.VMEM((dims, rels), F32),
                *[pltpu.VMEM(ids.shape, jnp.int32) for ids in (source_ids, relation_ids, target_ids, negative_ids)],
                pltpu.SemaphoreType.DMA((14,)),
                pltpu.VMEM((rows, edges), BF16),
                pltpu.VMEM((rels, edges), BF16),
                pltpu.VMEM((2, edges, dims), BF16),
                pltpu.VMEM((2, dims, edges), BF16),
                pltpu.VMEM((dims, edges), F32),
                pltpu.VMEM((dims, edges), F32),
                pltpu.VMEM((dims, edges), F32),
                pltpu.VMEM((1, rows), F32),
                pltpu.VMEM((n_rel, dims, rels), F32),
                pltpu.SemaphoreType.DMA((n_rel, len(blocks))),
                pltpu.SemaphoreType.DMA((n_rel, len(blocks))),
                pltpu.SemaphoreType.DMA((2, buckets - 1, chunks)),
                pltpu.SemaphoreType.DMA((2, buckets - 1, chunks)),
                pltpu.VMEM((buckets - 1, chunks, 1, 256), F32),
                pltpu.VMEM((buckets - 1, chunks, 1, 256), F32),
                pltpu.VMEM((2 * LANES, edges), BF16),
                pltpu.VMEM((edges, plan[-1][1]), F32),
                pltpu.VMEM((edges, plan[-1][1]), F32),
                *[pltpu.VMEM((2, dims, 256), BF16) for _ in plan],
                *[pltpu.VMEM((2, edges, 256), BF16) for _ in plan],
                *moves,
                *moves,
            ],
            compiler_params=pltpu.CompilerParams(
                collective_id=0, has_side_effects=True, vmem_limit_bytes=40 * 1024 * 1024
            ),
        )(*(
            pltpu.with_memory_space_constraint(x, pltpu.HBM) for x in (
                source_table, source_state, target_table, target_state,
                relation_ops, relation_state, source_ids, relation_ids,
                target_ids, negative_ids,
            )
        ))
        hbm = pl.BlockSpec(memory_space=pl.ANY)
        return pl.pallas_call(
            emit,
            out_shape=(
                shape((dims, rows), F32), shape((rows,), F32),
                shape((dims, rows), F32), shape((rows,), F32),
                shape((dims, rels), F32), shape((dims, rels), F32),
            ),
            in_specs=[vmem] * 6,
            out_specs=(hbm,) * 6,
            scratch_shapes=[pltpu.VMEM((rows,), F32), pltpu.VMEM((rows,), F32), pltpu.SemaphoreType.DMA((6,))],
            compiler_params=pltpu.CompilerParams(vmem_limit_bytes=16 * 1024 * 1024),
        )(*out)

    split_both = ("blk", "rel")
    return jax.shard_map(
        per_device,
        mesh=mesh,
        in_specs=(
            P(None, split_both), P(split_both), P(None, split_both), P(split_both),
            P(None, "blk"), P(None, "blk"),
            P(None, split_both), P(None, split_both), P(None, split_both), P(None, split_both),
        ),
        out_specs=(
            P(None, split_both), P(split_both), P(None, split_both), P(split_both),
            P(None, "blk"), P(None, "blk"),
        ),
        check_vma=False,
    )
```

```python
import functools

import jax
import jax.numpy as jnp
from jax import lax
from jax.experimental import pallas as pl
from jax.experimental.pallas import tpu as pltpu
from jax.sharding import PartitionSpec as P

learn_rate = 0.1
epsilon = 1e-06
LANES = 128
MESH = pl.DeviceIdType.MESH
F32 = jnp.float32
BF16 = jnp.bfloat16


def split(x):
    high = x.astype(BF16)
    return high, (x - high.astype(F32)).astype(BF16)


def nn(a, b):
    return lax.dot_general(a, b, (((1,), (0,)), ((), ())), preferred_element_type=F32)


def nt(a, b):
    return lax.dot_general(a, b, (((1,), (1,)), ((), ())), preferred_element_type=F32)


def both_nn(hi, lo, b):
    n = hi.shape[0]
    tall = nn(jnp.concatenate([hi, lo], axis=0), b)
    return tall[:n] + tall[n:]


def both_nt(hi, lo, b):
    n = hi.shape[0]
    tall = nt(jnp.concatenate([hi, lo], axis=0), b)
    return tall[:n] + tall[n:]


def column(row):
    wide = jnp.broadcast_to(row.astype(F32), (8, row.shape[1]))
    return jnp.transpose(wide)[:, :1].astype(jnp.int32)


def one_hot(row, height):
    low = lax.rem(row, LANES)
    inner = (lax.broadcasted_iota(jnp.int32, (LANES, row.shape[1]), 0) == low).astype(F32).astype(BF16)
    if height == LANES:
        return inner
    out = []
    for start in range(0, height, LANES):
        here = (row - low == start).astype(F32).astype(BF16)
        out.append(inner * jnp.broadcast_to(here, inner.shape))
    return jnp.concatenate(out, axis=0)


def chunk_plan(rows):
    if rows % 256 == 0 and rows >= 512:
        widths = [LANES] + [256] * (rows // 256 - 1) + [LANES]
    else:
        widths = [LANES] * (rows // LANES)
    return [(sum(widths[:i]), w) for i, w in enumerate(widths)]


def row_blocks(dims):
    first = (dims // 2 + 15) // 16 * 16
    return [(0, first), (first, dims - first)]


def lane_gather(table, index):
    tall = table.shape[0]
    groups = table.shape[1] // LANES
    out = []
    for start in range(0, index.shape[1], LANES):
        one = jnp.broadcast_to(index[:, start:start + LANES], (tall, LANES))
        low = lax.rem(one, LANES)
        got = jnp.take_along_axis(table[:, :LANES], low, axis=1)
        for g in range(1, groups):
            other = jnp.take_along_axis(table[:, g * LANES:(g + 1) * LANES], low, axis=1)
            got = jnp.where(one >= g * LANES, other, got)
        out.append(got)
    return jnp.concatenate(out, axis=1)


def emit(*refs):
    inputs, outputs, (first, second, sem) = refs[:6], refs[6:12], refs[12:]
    copies = []
    for i in (0, 2, 4, 5):
        copies.append(pltpu.make_async_copy(inputs[i], outputs[i], sem.at[i]))
        copies[-1].start()
    for i, line in ((1, first), (3, second)):
        line[...] = inputs[i][0, :]
        copies.append(pltpu.make_async_copy(line, outputs[i], sem.at[i]))
        copies[-1].start()
    for copy in copies:
        copy.wait()


def kernel(n_blk, n_rel, plan, blocks, *refs):
    refs = list(refs)

    def take(n):
        out = refs[:n]
        del refs[:n]
        return out

    src_in, srow_in, tgt_in, trow_in, rel_in, rstate_in, sid_in, rid_in, tid_in, nid_in = take(10)
    out_src, out_srow, out_tgt, out_trow, out_rel, out_rstate = take(6)
    src_ref, srow_ref, tgt_ref, trow_ref, rel_ref, rstate_ref, sid_ref, rid_ref, tid_ref, nid_ref = take(10)
    load_sem, hot, rhot, qt_ref, q_ref, picked, relation, gq_ref, counts, rel_all = take(10)
    rsend_sem, rrecv_sem, send_sem, recv_sem, row_send, row_recv = take(6)
    turned, base_ref, gain_ref = take(3)
    tables, weights = take(len(plan)), take(len(plan))
    send, recv = take(len(plan)), take(len(plan))
    dims, rows = src_ref.shape
    buckets, edges = sid_ref.shape
    negs = nid_ref.shape[1]
    rels = rel_ref.shape[1]
    final = len(plan) - 1
    groups = [(e, min(256, edges - e)) for e in range(0, edges, 256)]
    my_blk = lax.axis_index("blk")
    my_rel = lax.axis_index("rel")
    nxt = lax.rem(my_blk + 1, n_blk)
    prv = lax.rem(my_blk + n_blk - 1, n_blk)

    loads = []

    def load(there, here):
        loads.append(pltpu.make_async_copy(there, here, load_sem.at[len(loads)]))
        loads[-1].start()
        return loads[-1]

    load_ids = [
        load(sid_in, sid_ref), load(rid_in, rid_ref), load(nid_in, nid_ref), load(tid_in, tid_ref)
    ]
    quarter = dims // 64 * 16
    ends = [0, quarter, 2 * quarter, 3 * quarter, dims]
    load_src = [
        load(src_in.at[pl.ds(r, n - r)], src_ref.at[pl.ds(r, n - r)]) for r, n in zip(ends[:2], ends[1:3])
    ]
    load_rel = load(rel_in, rel_ref)
    load_src += [
        load(src_in.at[pl.ds(r, n - r)], src_ref.at[pl.ds(r, n - r)]) for r, n in zip(ends[2:4], ends[3:])
    ]
    wide = plan[0][1]
    load_first = [load(tgt_in.at[:, pl.ds(0, wide)], tgt_ref.at[:, pl.ds(0, wide)]), load(trow_in, trow_ref)]
    load_rest = []

    barrier = pltpu.get_barrier_semaphore()
    pl.semaphore_signal(barrier, inc=1, device_id={"blk": prv}, device_id_type=MESH)
    for step in range(1, n_rel):
        pl.semaphore_signal(
            barrier, inc=1, device_id={"rel": lax.rem(my_rel + step, n_rel)}, device_id_type=MESH
        )

    def hop(bucket, c):
        return pltpu.make_async_remote_copy(
            src_ref=send[c].at[bucket],
            dst_ref=recv[c].at[bucket],
            send_sem=send_sem.at[0, bucket, c],
            recv_sem=recv_sem.at[0, bucket, c],
            device_id={"blk": nxt},
            device_id_type=MESH,
        )

    def row_hop(bucket, c):
        return pltpu.make_async_remote_copy(
            src_ref=row_send.at[bucket, c, :, pl.ds(0, plan[c][1])],
            dst_ref=row_recv.at[bucket, c, :, pl.ds(0, plan[c][1])],
            send_sem=send_sem.at[1, bucket, c],
            recv_sem=recv_sem.at[1, bucket, c],
            device_id={"blk": nxt},
            device_id_type=MESH,
        )

    def rel_hop(to, slot, step, b):
        r, n = blocks[b]
        return pltpu.make_async_remote_copy(
            src_ref=rel_all.at[slot, pl.ds(r, n)],
            dst_ref=rel_all.at[slot, pl.ds(r, n)],
            send_sem=rsend_sem.at[step - 1, b],
            recv_sem=rrecv_sem.at[slot, b],
            device_id={"rel": to},
            device_id_type=MESH,
        )

    def put_pair(ref, hi, lo, twice, part=slice(None)):
        width = hi.shape[1]
        if width == LANES:
            ref[0, part, :LANES] = hi
            ref[0, part, LANES:] = lo
            if twice:
                ref[1, :, :LANES] = hi
                ref[1, :, LANES:] = hi
        else:
            ref[0, part, :] = hi
            ref[1, part, :] = lo

    def fold(wide):
        return wide[:, :LANES] + wide[:, LANES:]

    for copy in load_ids:
        copy.wait()

    for bucket in range(buckets):
        last = bucket + 1 == buckets
        now_src = src_ref if bucket == 0 else out_src
        sid = sid_ref[pl.ds(bucket, 1), :]
        rid = rid_ref[pl.ds(bucket, 1), :]
        hot[...] = one_hot(sid, rows)
        for first in (0, 2):
            part = pl.ds(ends[first], ends[first + 2] - ends[first])
            if bucket == 0:
                for copy in load_src[first:first + 2]:
                    copy.wait()
                if first:
                    for copy in [load_rel] + load_first:
                        copy.wait()
                    if rows > wide:
                        late = pl.ds(wide, rows - wide)
                        load_rest.append(load(tgt_in.at[:, late], tgt_ref.at[:, late]))
                    load_rest.extend([load(srow_in, srow_ref), load(rstate_in, rstate_ref)])
            s_hi, s_lo = split(now_src[part, :])
            for e, m in groups:
                some = pl.ds(e, m)
                picked[part, some] = both_nn(s_hi, s_lo, hot[:, some])
        relation[...] = lane_gather(rel_ref[...], rid)
        for e, m in groups:
            some = pl.ds(e, m)
            hi, lo = split(picked[:, some] * relation[:, some])
            q_ref[0, :, some] = hi
            q_ref[1, :, some] = lo

        def turn():
            for e, m in groups:
                some = pl.ds(e, m)
                hi, lo = split(jnp.transpose(picked[:, some] * relation[:, some] * 0.5))
                qt_ref[0, some, :] = hi
                qt_ref[1, some, :] = lo
            nid = column(nid_ref[pl.ds(bucket, 1), :])
            for start in range(0, rows, LANES):
                lane = lax.broadcasted_iota(jnp.int32, (negs, LANES), 1) + start
                counts[:, pl.ds(start, LANES)] = jnp.sum(
                    (lane == nid).astype(F32), axis=0, keepdims=True
                ) * (0.5 / negs)
            rhot[...] = one_hot(rid, rels)
            return column(tid_ref[pl.ds(bucket, 1), :])

        def weigh_turned():
            table = tgt_ref[:, :LANES]
            hi, lo = split(table)
            put_pair(tables[0], hi, lo, True)
            hi, lo = split(jnp.transpose(table) * 0.5)
            wide = nn(jnp.concatenate([hi, lo], axis=0), q_ref[0])
            score = wide[:LANES] + wide[LANES:] + nn(hi, q_ref[1])
            half = jnp.tanh(score)
            here = lax.broadcasted_iota(jnp.int32, (LANES, negs), 0) == nid_ref[pl.ds(bucket, 1), :]
            count = jnp.sum(here.astype(F32), axis=1, keepdims=True) * (0.5 / negs)
            here = lax.broadcasted_iota(jnp.int32, (LANES, edges), 0) == tid_ref[pl.ds(bucket, 1), :]
            weight = count * half + count - jnp.where(here, 0.5 - 0.5 * half, 0.0)
            hi, lo = split(weight)
            turned[:LANES, :] = hi
            turned[LANES:, :] = lo

        base, gain = {}, {}

        def prepare(c):
            start, width = plan[c]
            count = counts[:, pl.ds(start, width)]
            base[c], gain[c] = {}, {}
            for e, m in groups:
                own = lax.broadcasted_iota(jnp.int32, (m, width), 1) + start == tid[e:e + m]
                half = jnp.where(own, 0.5, 0.0)
                base[c][e], gain[c][e] = count - half, count + half
                if c == final and bucket > 0:
                    base_ref[e:e + m, :], gain_ref[e:e + m, :] = base[c][e], gain[c][e]

        def weigh(c):
            start, width = plan[c]
            if c == final and bucket > 0:
                for e, m in groups:
                    base[c][e], gain[c][e] = base_ref[e:e + m, :], gain_ref[e:e + m, :]
            else:
                prepare(c)
            cols = pl.ds(start, width)
            table = tgt_ref[:, cols] if bucket == 0 else recv[c][bucket - 1]
            t_hi, t_lo = split(table)
            put_pair(tables[c], t_hi, t_lo, True)
            for e, m in groups:
                some = pl.ds(e, m)
                if width == LANES:
                    score = fold(nn(qt_ref[0, some, :], tables[c][0])) + nn(qt_ref[1, some, :], t_hi)
                else:
                    score = (
                        both_nn(qt_ref[0, some, :], qt_ref[1, some, :], t_hi) + nn(qt_ref[0, some, :], t_lo)
                    )
                half = jnp.tanh(score)
                weight = base[c][e] + gain[c][e] * half
                w_hi, w_lo = split(weight)
                put_pair(weights[c], w_hi, w_lo, False, some)

        def query_part(c, part, some=slice(None)):
            if bucket == 0 and c == 0:
                return (
                    nn(tables[c][1, part, :], turned[:, some])
                    + nn(tables[c][0, part, LANES:], turned[:LANES, some])
                )
            if plan[c][1] == LANES:
                return (
                    nt(tables[c][1, part, :], weights[c][0, some, :])
                    + nt(tables[c][0, part, LANES:], weights[c][0, some, :LANES])
                )
            return (
                both_nt(tables[c][0, part, :], tables[c][1, part, :], weights[c][0, some, :])
                + nt(tables[c][0, part, :], weights[c][1, some, :])
            )

        def finish(c):
            start, width = plan[c]
            cols = pl.ds(start, width)
            if bucket == 0:
                table = tgt_ref[:, cols]
                state = trow_ref[cols].reshape(1, width)
            else:
                if c == final:
                    row_hop(bucket - 1, c).wait_recv()
                table = recv[c][bucket - 1]
                state = row_recv[bucket - 1, c, :, :width]
            if bucket == 0 and c == 0:
                grad = fold(nt(q_ref[0], turned[...])) + nt(q_ref[1], turned[:LANES, :])
            elif width == LANES:
                grad = fold(nn(q_ref[0], weights[c][0])) + nn(q_ref[1], weights[c][0, :, :LANES])
            else:
                grad = both_nn(q_ref[0], q_ref[1], weights[c][0]) + nn(q_ref[0], weights[c][1])
            fresh = state + jnp.sum(grad * grad, axis=0, keepdims=True) * (1.0 / dims)
            new = table - grad * (learn_rate / (jnp.sqrt(fresh) + epsilon))
            if last:
                out_tgt[:, cols] = new
                out_trow[:, cols] = fresh
            else:
                send[c][bucket] = new
                row_send[bucket, c, :, :width] = fresh

        def relate(part, whole):
            g_hi, g_lo = split(whole * picked[part, :])
            rel_grad = both_nt(g_hi, g_lo, rhot[...])
            if bucket == 0:
                rel_all[my_rel, part, :] = rel_grad
            else:
                rel_all[my_rel, part, :] = rel_all[my_rel, part, :] + rel_grad

        everything = pl.ds(0, dims)

        def arrive(c):
            if bucket > 0:
                hop(bucket - 1, c).wait_recv()
                if c < final:
                    row_hop(bucket - 1, c).wait_recv()

        def depart(c):
            row_hop(bucket, c).start()
            hop(bucket, c).start()

        if not last:
            if bucket == 0:
                weigh_turned()
                finish(0)
                pl.semaphore_wait(barrier, n_rel)
                depart(0)
                for copy in load_rest:
                    copy.wait()
                tid = turn()
            else:
                tid = turn()
                arrive(0)
                weigh(0)
                finish(0)
                depart(0)
            if final > 0:
                arrive(1)
                weigh(1)
            for c in range(1, final + 1):
                if c < final:
                    arrive(c + 1)
                finish(c)
                if c == 1:
                    depart(c)
                if c < final:
                    weigh(c + 1)
                if c > 1:
                    depart(c)
            total = query_part(0, everything)
            for c in range(1, len(plan)):
                total += query_part(c, everything)
            gq_ref[...] = total
            relate(everything, total)
        else:
            def gather_query(c):
                part = query_part(c, everything)
                gq_ref[...] = part if c == 0 else gq_ref[...] + part

            tid = turn()
            if bucket == 0:
                pl.semaphore_wait(barrier, n_rel)
                for copy in load_rest:
                    copy.wait()
            for c in range(final):
                arrive(c)
                weigh_turned() if bucket == 0 and c == 0 else weigh(c)
                if c > 0:
                    gather_query(c - 1)
                    finish(c - 1)
            if final > 0:
                gather_query(final - 1)
                finish(final - 1)
            if bucket > 0:
                prepare(final)
            arrive(final)
            weigh(final)
            for b, (r, n) in enumerate(blocks):
                part = pl.ds(r, n)
                rel_grad = rel_all[my_rel, part, :] if bucket > 0 else 0.0
                for e, m in groups:
                    some = pl.ds(e, m)
                    whole = query_part(final, part, some)
                    if final > 0:
                        whole = gq_ref[part, some] + whole
                    gq_ref[part, some] = whole
                    g_hi, g_lo = split(whole * picked[part, some])
                    rel_grad += both_nt(g_hi, g_lo, rhot[:, some])
                rel_all[my_rel, part, :] = rel_grad
                for step in range(1, n_rel):
                    rel_hop(lax.rem(my_rel + step, n_rel), my_rel, step, b).start()
            finish(final)
        g_hi, g_lo = split(gq_ref[...] * relation[...])
        src_grad = both_nt(g_hi, g_lo, hot[...])
        now_srow = srow_ref[...].reshape(1, rows) if bucket == 0 else out_srow[...]
        fresh = now_srow + jnp.sum(src_grad * src_grad, axis=0, keepdims=True) * (1.0 / dims)
        out_src[...] = now_src[...] - src_grad * (learn_rate / (jnp.sqrt(fresh) + epsilon))
        out_srow[...] = fresh

    for bucket in range(buckets - 1):
        for c in range(len(plan)):
            hop(bucket, c).wait_send()
            row_hop(bucket, c).wait_send()
    for b, (r, n) in enumerate(blocks):
        part = pl.ds(r, n)
        for step in range(1, n_rel):
            peer = lax.rem(my_rel + n_rel - step, n_rel)
            arrived = rel_hop(peer, peer, step, b)
            arrived.wait_send()
            arrived.wait_recv()
        total = rel_all[0, part, :]
        for step in range(1, n_rel):
            total = total + rel_all[step, part, :]
        new_state = rstate_ref[part, :] + total * total
        out_rstate[part, :] = new_state
        out_rel[part, :] = rel_ref[part, :] - learn_rate * total / (jnp.sqrt(new_state) + epsilon)


def solution(mesh):
    n_blk, n_rel = mesh.shape["blk"], mesh.shape["rel"]

    def per_device(
        source_table, source_state, target_table, target_state, relation_ops, relation_state,
        source_ids, target_ids, relation_ids, negative_ids,
    ):
        dims, rows = source_table.shape
        rels = relation_ops.shape[1]
        buckets, edges = source_ids.shape
        plan = chunk_plan(rows)
        blocks = row_blocks(dims)
        chunks = len(plan)
        vmem = pl.BlockSpec(memory_space=pltpu.VMEM)
        shape = jax.ShapeDtypeStruct
        moves = [pltpu.VMEM((buckets - 1, dims, width), F32) for _, width in plan]
        out = pl.pallas_call(
            functools.partial(kernel, n_blk, n_rel, plan, blocks),
            out_shape=(
                pltpu.VMEM((dims, rows), F32), pltpu.VMEM((1, rows), F32),
                pltpu.VMEM((dims, rows), F32), pltpu.VMEM((1, rows), F32),
                pltpu.VMEM((dims, rels), F32), pltpu.VMEM((dims, rels), F32),
            ),
            in_specs=[pl.BlockSpec(memory_space=pltpu.HBM)] * 10,
            out_specs=(vmem,) * 6,
            scratch_shapes=[
                pltpu.VMEM((dims, rows), F32), pltpu.VMEM((rows,), F32),
                pltpu.VMEM((dims, rows), F32), pltpu.VMEM((rows,), F32),
                pltpu.VMEM((dims, rels), F32), pltpu.VMEM((dims, rels), F32),
                *[pltpu.VMEM(ids.shape, jnp.int32) for ids in (source_ids, relation_ids, target_ids, negative_ids)],
                pltpu.SemaphoreType.DMA((14,)),
                pltpu.VMEM((rows, edges), BF16),
                pltpu.VMEM((rels, edges), BF16),
                pltpu.VMEM((2, edges, dims), BF16),
                pltpu.VMEM((2, dims, edges), BF16),
                pltpu.VMEM((dims, edges), F32),
                pltpu.VMEM((dims, edges), F32),
                pltpu.VMEM((dims, edges), F32),
                pltpu.VMEM((1, rows), F32),
                pltpu.VMEM((n_rel, dims, rels), F32),
                pltpu.SemaphoreType.DMA((n_rel, len(blocks))),
                pltpu.SemaphoreType.DMA((n_rel, len(blocks))),
                pltpu.SemaphoreType.DMA((2, buckets - 1, chunks)),
                pltpu.SemaphoreType.DMA((2, buckets - 1, chunks)),
                pltpu.VMEM((buckets - 1, chunks, 1, 256), F32),
                pltpu.VMEM((buckets - 1, chunks, 1, 256), F32),
                pltpu.VMEM((2 * LANES, edges), BF16),
                pltpu.VMEM((edges, plan[-1][1]), F32),
                pltpu.VMEM((edges, plan[-1][1]), F32),
                *[pltpu.VMEM((2, dims, 256), BF16) for _ in plan],
                *[pltpu.VMEM((2, edges, 256), BF16) for _ in plan],
                *moves,
                *moves,
            ],
            compiler_params=pltpu.CompilerParams(
                collective_id=0, has_side_effects=True, vmem_limit_bytes=40 * 1024 * 1024
            ),
        )(*(
            pltpu.with_memory_space_constraint(x, pltpu.HBM) for x in (
                source_table, source_state, target_table, target_state,
                relation_ops, relation_state, source_ids, relation_ids,
                target_ids, negative_ids,
            )
        ))
        hbm = pl.BlockSpec(memory_space=pl.ANY)
        return pl.pallas_call(
            emit,
            out_shape=(
                shape((dims, rows), F32), shape((rows,), F32),
                shape((dims, rows), F32), shape((rows,), F32),
                shape((dims, rels), F32), shape((dims, rels), F32),
            ),
            in_specs=[vmem] * 6,
            out_specs=(hbm,) * 6,
            scratch_shapes=[pltpu.VMEM((rows,), F32), pltpu.VMEM((rows,), F32), pltpu.SemaphoreType.DMA((6,))],
            compiler_params=pltpu.CompilerParams(vmem_limit_bytes=16 * 1024 * 1024),
        )(*out)

    split_both = ("blk", "rel")
    return jax.shard_map(
        per_device,
        mesh=mesh,
        in_specs=(
            P(None, split_both), P(split_both), P(None, split_both), P(split_both),
            P(None, "blk"), P(None, "blk"),
            P(None, split_both), P(None, split_both), P(None, split_both), P(None, split_both),
        ),
        out_specs=(
            P(None, split_both), P(split_both), P(None, split_both), P(split_both),
            P(None, "blk"), P(None, "blk"),
        ),
        check_vma=False,
    )
```

```python
import functools

import jax
import jax.numpy as jnp
from jax import lax
from jax.experimental import pallas as pl
from jax.experimental.pallas import tpu as pltpu
from jax.sharding import PartitionSpec as P

learn_rate = 0.1
epsilon = 1e-06
LANES = 128
MESH = pl.DeviceIdType.MESH
F32 = jnp.float32
BF16 = jnp.bfloat16


def split(x):
    high = x.astype(BF16)
    return high, (x - high.astype(F32)).astype(BF16)


def nn(a, b):
    return lax.dot_general(a, b, (((1,), (0,)), ((), ())), preferred_element_type=F32)


def nt(a, b):
    return lax.dot_general(a, b, (((1,), (1,)), ((), ())), preferred_element_type=F32)


def both_nn(hi, lo, b):
    n = hi.shape[0]
    tall = nn(jnp.concatenate([hi, lo], axis=0), b)
    return tall[:n] + tall[n:]


def both_nt(hi, lo, b):
    n = hi.shape[0]
    tall = nt(jnp.concatenate([hi, lo], axis=0), b)
    return tall[:n] + tall[n:]


def column(row):
    wide = jnp.broadcast_to(row.astype(F32), (8, row.shape[1]))
    return jnp.transpose(wide)[:, :1].astype(jnp.int32)


def one_hot(row, height):
    low = lax.rem(row, LANES)
    inner = (lax.broadcasted_iota(jnp.int32, (LANES, row.shape[1]), 0) == low).astype(F32).astype(BF16)
    if height == LANES:
        return inner
    out = []
    for start in range(0, height, LANES):
        here = (row - low == start).astype(F32).astype(BF16)
        out.append(inner * jnp.broadcast_to(here, inner.shape))
    return jnp.concatenate(out, axis=0)


def chunk_plan(rows):
    if rows % 256 == 0 and rows >= 512:
        widths = [LANES] + [256] * (rows // 256 - 1) + [LANES]
    else:
        widths = [LANES] * (rows // LANES)
    return [(sum(widths[:i]), w) for i, w in enumerate(widths)]


def row_blocks(dims):
    first = (dims // 2 + 15) // 16 * 16
    return [(0, first), (first, dims - first)]


def lane_gather(table, index):
    tall = table.shape[0]
    groups = table.shape[1] // LANES
    out = []
    for start in range(0, index.shape[1], LANES):
        one = jnp.broadcast_to(index[:, start:start + LANES], (tall, LANES))
        low = lax.rem(one, LANES)
        got = jnp.take_along_axis(table[:, :LANES], low, axis=1)
        for g in range(1, groups):
            other = jnp.take_along_axis(table[:, g * LANES:(g + 1) * LANES], low, axis=1)
            got = jnp.where(one >= g * LANES, other, got)
        out.append(got)
    return jnp.concatenate(out, axis=1)


def emit(*refs):
    inputs, outputs, (first, second, sem) = refs[:6], refs[6:12], refs[12:]
    copies = []
    for i in (0, 2, 4, 5):
        copies.append(pltpu.make_async_copy(inputs[i], outputs[i], sem.at[i]))
        copies[-1].start()
    for i, line in ((1, first), (3, second)):
        line[...] = inputs[i][0, :]
        copies.append(pltpu.make_async_copy(line, outputs[i], sem.at[i]))
        copies[-1].start()
    for copy in copies:
        copy.wait()


def kernel(n_blk, n_rel, plan, blocks, *refs):
    refs = list(refs)

    def take(n):
        out = refs[:n]
        del refs[:n]
        return out

    src_in, srow_in, tgt_in, trow_in, rel_in, rstate_in, sid_in, rid_in, tid_in, nid_in = take(10)
    out_src, out_srow, out_tgt, out_trow, out_rel, out_rstate = take(6)
    src_ref, srow_ref, tgt_ref, trow_ref, rel_ref, rstate_ref, sid_ref, rid_ref, tid_ref, nid_ref = take(10)
    load_sem, hot, rhot, qt_ref, q_ref, picked, relation, gq_ref, counts, rel_all = take(10)
    rsend_sem, rrecv_sem, send_sem, recv_sem, row_send, row_recv = take(6)
    turned, base_ref, gain_ref = take(3)
    tables, weights = take(len(plan)), take(len(plan))
    send, recv = take(len(plan)), take(len(plan))
    dims, rows = src_ref.shape
    buckets, edges = sid_ref.shape
    negs = nid_ref.shape[1]
    rels = rel_ref.shape[1]
    final = len(plan) - 1
    groups = [(e, min(256, edges - e)) for e in range(0, edges, 256)]
    my_blk = lax.axis_index("blk")
    my_rel = lax.axis_index("rel")
    nxt = lax.rem(my_blk + 1, n_blk)
    prv = lax.rem(my_blk + n_blk - 1, n_blk)

    loads = []

    def load(there, here):
        loads.append(pltpu.make_async_copy(there, here, load_sem.at[len(loads)]))
        loads[-1].start()
        return loads[-1]

    load_ids = [
        load(sid_in, sid_ref), load(rid_in, rid_ref), load(nid_in, nid_ref), load(tid_in, tid_ref)
    ]
    quarter = dims // 64 * 16
    ends = [0, quarter, 2 * quarter, 3 * quarter, dims]
    load_src = [
        load(src_in.at[pl.ds(r, n - r)], src_ref.at[pl.ds(r, n - r)]) for r, n in zip(ends[:2], ends[1:3])
    ]
    load_rel = load(rel_in, rel_ref)
    load_src += [
        load(src_in.at[pl.ds(r, n - r)], src_ref.at[pl.ds(r, n - r)]) for r, n in zip(ends[2:4], ends[3:])
    ]
    wide = plan[0][1]
    load_first = [load(tgt_in.at[:, pl.ds(0, wide)], tgt_ref.at[:, pl.ds(0, wide)]), load(trow_in, trow_ref)]
    load_rest = []

    barrier = pltpu.get_barrier_semaphore()
    pl.semaphore_signal(barrier, inc=1, device_id={"blk": prv}, device_id_type=MESH)
    for step in range(1, n_rel):
        pl.semaphore_signal(
            barrier, inc=1, device_id={"rel": lax.rem(my_rel + step, n_rel)}, device_id_type=MESH
        )

    def hop(bucket, c):
        return pltpu.make_async_remote_copy(
            src_ref=send[c].at[bucket],
            dst_ref=recv[c].at[bucket],
            send_sem=send_sem.at[0, bucket, c],
            recv_sem=recv_sem.at[0, bucket, c],
            device_id={"blk": nxt},
            device_id_type=MESH,
        )

    def row_hop(bucket, c):
        return pltpu.make_async_remote_copy(
            src_ref=row_send.at[bucket, c, :, pl.ds(0, plan[c][1])],
            dst_ref=row_recv.at[bucket, c, :, pl.ds(0, plan[c][1])],
            send_sem=send_sem.at[1, bucket, c],
            recv_sem=recv_sem.at[1, bucket, c],
            device_id={"blk": nxt},
            device_id_type=MESH,
        )

    def rel_hop(to, slot, step, b):
        r, n = blocks[b]
        return pltpu.make_async_remote_copy(
            src_ref=rel_all.at[slot, pl.ds(r, n)],
            dst_ref=rel_all.at[slot, pl.ds(r, n)],
            send_sem=rsend_sem.at[step - 1, b],
            recv_sem=rrecv_sem.at[slot, b],
            device_id={"rel": to},
            device_id_type=MESH,
        )

    def put_pair(ref, hi, lo, twice, part=slice(None)):
        width = hi.shape[1]
        if width == LANES:
            ref[0, part, :LANES] = hi
            ref[0, part, LANES:] = lo
            if twice:
                ref[1, :, :LANES] = hi
                ref[1, :, LANES:] = hi
        else:
            ref[0, part, :] = hi
            ref[1, part, :] = lo

    def fold(wide):
        return wide[:, :LANES] + wide[:, LANES:]

    for copy in load_ids:
        copy.wait()

    for bucket in range(buckets):
        last = bucket + 1 == buckets
        now_src = src_ref if bucket == 0 else out_src
        sid = sid_ref[pl.ds(bucket, 1), :]
        rid = rid_ref[pl.ds(bucket, 1), :]
        hot[...] = one_hot(sid, rows)
        for first in (0, 2):
            part = pl.ds(ends[first], ends[first + 2] - ends[first])
            if bucket == 0:
                for copy in load_src[first:first + 2]:
                    copy.wait()
                if first:
                    for copy in [load_rel] + load_first:
                        copy.wait()
                    if rows > wide:
                        late = pl.ds(wide, rows - wide)
                        load_rest.append(load(tgt_in.at[:, late], tgt_ref.at[:, late]))
                    load_rest.extend([load(srow_in, srow_ref), load(rstate_in, rstate_ref)])
            s_hi, s_lo = split(now_src[part, :])
            for e, m in groups:
                some = pl.ds(e, m)
                picked[part, some] = both_nn(s_hi, s_lo, hot[:, some])
        relation[...] = lane_gather(rel_ref[...], rid)
        for e, m in groups:
            some = pl.ds(e, m)
            hi, lo = split(picked[:, some] * relation[:, some])
            q_ref[0, :, some] = hi
            q_ref[1, :, some] = lo

        def turn():
            for e, m in groups:
                some = pl.ds(e, m)
                hi, lo = split(jnp.transpose(picked[:, some] * relation[:, some] * 0.5))
                qt_ref[0, some, :] = hi
                qt_ref[1, some, :] = lo
            nid = column(nid_ref[pl.ds(bucket, 1), :])
            for start in range(0, rows, LANES):
                lane = lax.broadcasted_iota(jnp.int32, (negs, LANES), 1) + start
                counts[:, pl.ds(start, LANES)] = jnp.sum(
                    (lane == nid).astype(F32), axis=0, keepdims=True
                ) * (0.5 / negs)
            rhot[...] = one_hot(rid, rels)
            return column(tid_ref[pl.ds(bucket, 1), :])

        def weigh_turned():
            table = tgt_ref[:, :LANES]
            hi, lo = split(table)
            put_pair(tables[0], hi, lo, True)
            hi, lo = split(jnp.transpose(table) * 0.5)
            wide = nn(jnp.concatenate([hi, lo], axis=0), q_ref[0])
            score = wide[:LANES] + wide[LANES:] + nn(hi, q_ref[1])
            half = jnp.tanh(score)
            here = lax.broadcasted_iota(jnp.int32, (LANES, negs), 0) == nid_ref[pl.ds(bucket, 1), :]
            count = jnp.sum(here.astype(F32), axis=1, keepdims=True) * (0.5 / negs)
            here = lax.broadcasted_iota(jnp.int32, (LANES, edges), 0) == tid_ref[pl.ds(bucket, 1), :]
            weight = count * half + count - jnp.where(here, 0.5 - 0.5 * half, 0.0)
            hi, lo = split(weight)
            turned[:LANES, :] = hi
            turned[LANES:, :] = lo

        base, gain = {}, {}

        def prepare(c):
            start, width = plan[c]
            count = counts[:, pl.ds(start, width)]
            base[c], gain[c] = {}, {}
            for e, m in groups:
                own = lax.broadcasted_iota(jnp.int32, (m, width), 1) + start == tid[e:e + m]
                half = jnp.where(own, 0.5, 0.0)
                base[c][e], gain[c][e] = count - half, count + half
                if c == final and bucket > 0:
                    base_ref[e:e + m, :], gain_ref[e:e + m, :] = base[c][e], gain[c][e]

        def weigh(c):
            start, width = plan[c]
            if c == final and bucket > 0:
                for e, m in groups:
                    base[c][e], gain[c][e] = base_ref[e:e + m, :], gain_ref[e:e + m, :]
            else:
                prepare(c)
            cols = pl.ds(start, width)
            table = tgt_ref[:, cols] if bucket == 0 else recv[c][bucket - 1]
            t_hi, t_lo = split(table)
            put_pair(tables[c], t_hi, t_lo, True)
            for e, m in groups:
                some = pl.ds(e, m)
                if width == LANES:
                    score = fold(nn(qt_ref[0, some, :], tables[c][0])) + nn(qt_ref[1, some, :], t_hi)
                else:
                    score = (
                        both_nn(qt_ref[0, some, :], qt_ref[1, some, :], t_hi) + nn(qt_ref[0, some, :], t_lo)
                    )
                half = jnp.tanh(score)
                weight = base[c][e] + gain[c][e] * half
                w_hi, w_lo = split(weight)
                put_pair(weights[c], w_hi, w_lo, False, some)

        def query_part(c, part, some=slice(None)):
            if bucket == 0 and c == 0:
                return (
                    nn(tables[c][1, part, :], turned[:, some])
                    + nn(tables[c][0, part, LANES:], turned[:LANES, some])
                )
            if plan[c][1] == LANES:
                return (
                    nt(tables[c][1, part, :], weights[c][0, some, :])
                    + nt(tables[c][0, part, LANES:], weights[c][0, some, :LANES])
                )
            return (
                both_nt(tables[c][0, part, :], tables[c][1, part, :], weights[c][0, some, :])
                + nt(tables[c][0, part, :], weights[c][1, some, :])
            )

        def finish(c):
            start, width = plan[c]
            cols = pl.ds(start, width)
            if bucket == 0:
                table = tgt_ref[:, cols]
                state = trow_ref[cols].reshape(1, width)
            else:
                if c == final:
                    row_hop(bucket - 1, c).wait_recv()
                table = recv[c][bucket - 1]
                state = row_recv[bucket - 1, c, :, :width]
            if bucket == 0 and c == 0:
                grad = fold(nt(q_ref[0], turned[...])) + nt(q_ref[1], turned[:LANES, :])
            elif width == LANES:
                grad = fold(nn(q_ref[0], weights[c][0])) + nn(q_ref[1], weights[c][0, :, :LANES])
            else:
                grad = both_nn(q_ref[0], q_ref[1], weights[c][0]) + nn(q_ref[0], weights[c][1])
            fresh = state + jnp.sum(grad * grad, axis=0, keepdims=True) * (1.0 / dims)
            new = table - grad * (learn_rate / (jnp.sqrt(fresh) + epsilon))
            if last:
                out_tgt[:, cols] = new
                out_trow[:, cols] = fresh
            else:
                send[c][bucket] = new
                row_send[bucket, c, :, :width] = fresh

        def relate(part, whole):
            g_hi, g_lo = split(whole * picked[part, :])
            rel_grad = both_nt(g_hi, g_lo, rhot[...])
            if bucket == 0:
                rel_all[my_rel, part, :] = rel_grad
            else:
                rel_all[my_rel, part, :] = rel_all[my_rel, part, :] + rel_grad

        everything = pl.ds(0, dims)

        def arrive(c):
            if bucket > 0:
                hop(bucket - 1, c).wait_recv()
                if c < final:
                    row_hop(bucket - 1, c).wait_recv()

        def depart(c):
            hop(bucket, c).start()
            row_hop(bucket, c).start()

        if not last:
            if bucket == 0:
                weigh_turned()
                finish(0)
                pl.semaphore_wait(barrier, n_rel)
                depart(0)
                for copy in load_rest:
                    copy.wait()
                tid = turn()
            else:
                tid = turn()
                arrive(0)
                weigh(0)
                finish(0)
                depart(0)
            if final > 0:
                arrive(1)
                weigh(1)
            for c in range(1, final + 1):
                if c < final:
                    arrive(c + 1)
                finish(c)
                if c == 1:
                    depart(c)
                if c < final:
                    weigh(c + 1)
                if c > 1:
                    depart(c)
            total = query_part(0, everything)
            for c in range(1, len(plan)):
                total += query_part(c, everything)
            gq_ref[...] = total
            relate(everything, total)
        else:
            def gather_query(c):
                part = query_part(c, everything)
                gq_ref[...] = part if c == 0 else gq_ref[...] + part

            tid = turn()
            if bucket == 0:
                pl.semaphore_wait(barrier, n_rel)
                for copy in load_rest:
                    copy.wait()
            for c in range(final):
                arrive(c)
                weigh_turned() if bucket == 0 and c == 0 else weigh(c)
                if c > 0:
                    gather_query(c - 1)
                    finish(c - 1)
            if final > 0:
                gather_query(final - 1)
                finish(final - 1)
            if bucket > 0:
                prepare(final)
            arrive(final)
            weigh(final)
            for b, (r, n) in enumerate(blocks):
                part = pl.ds(r, n)
                rel_grad = rel_all[my_rel, part, :] if bucket > 0 else 0.0
                for e, m in groups:
                    some = pl.ds(e, m)
                    whole = query_part(final, part, some)
                    if final > 0:
                        whole = gq_ref[part, some] + whole
                    gq_ref[part, some] = whole
                    g_hi, g_lo = split(whole * picked[part, some])
                    rel_grad += both_nt(g_hi, g_lo, rhot[:, some])
                rel_all[my_rel, part, :] = rel_grad
                for step in range(1, n_rel):
                    rel_hop(lax.rem(my_rel + step, n_rel), my_rel, step, b).start()
            finish(final)
        g_hi, g_lo = split(gq_ref[...] * relation[...])
        src_grad = both_nt(g_hi, g_lo, hot[...])
        now_srow = srow_ref[...].reshape(1, rows) if bucket == 0 else out_srow[...]
        fresh = now_srow + jnp.sum(src_grad * src_grad, axis=0, keepdims=True) * (1.0 / dims)
        out_src[...] = now_src[...] - src_grad * (learn_rate / (jnp.sqrt(fresh) + epsilon))
        out_srow[...] = fresh

    for bucket in range(buckets - 1):
        for c in range(len(plan)):
            hop(bucket, c).wait_send()
            row_hop(bucket, c).wait_send()
    for b, (r, n) in enumerate(blocks):
        part = pl.ds(r, n)
        for step in range(1, n_rel):
            peer = lax.rem(my_rel + n_rel - step, n_rel)
            arrived = rel_hop(peer, peer, step, b)
            arrived.wait_send()
            arrived.wait_recv()
        total = rel_all[0, part, :]
        for step in range(1, n_rel):
            total = total + rel_all[step, part, :]
        new_state = rstate_ref[part, :] + total * total
        out_rstate[part, :] = new_state
        out_rel[part, :] = rel_ref[part, :] - learn_rate * total / (jnp.sqrt(new_state) + epsilon)


def solution(mesh):
    n_blk, n_rel = mesh.shape["blk"], mesh.shape["rel"]

    def per_device(
        source_table, source_state, target_table, target_state, relation_ops, relation_state,
        source_ids, target_ids, relation_ids, negative_ids,
    ):
        dims, rows = source_table.shape
        rels = relation_ops.shape[1]
        buckets, edges = source_ids.shape
        plan = chunk_plan(rows)
        blocks = row_blocks(dims)
        chunks = len(plan)
        vmem = pl.BlockSpec(memory_space=pltpu.VMEM)
        shape = jax.ShapeDtypeStruct
        moves = [pltpu.VMEM((buckets - 1, dims, width), F32) for _, width in plan]
        out = pl.pallas_call(
            functools.partial(kernel, n_blk, n_rel, plan, blocks),
            out_shape=(
                pltpu.VMEM((dims, rows), F32), pltpu.VMEM((1, rows), F32),
                pltpu.VMEM((dims, rows), F32), pltpu.VMEM((1, rows), F32),
                pltpu.VMEM((dims, rels), F32), pltpu.VMEM((dims, rels), F32),
            ),
            in_specs=[pl.BlockSpec(memory_space=pltpu.HBM)] * 10,
            out_specs=(vmem,) * 6,
            scratch_shapes=[
                pltpu.VMEM((dims, rows), F32), pltpu.VMEM((rows,), F32),
                pltpu.VMEM((dims, rows), F32), pltpu.VMEM((rows,), F32),
                pltpu.VMEM((dims, rels), F32), pltpu.VMEM((dims, rels), F32),
                *[pltpu.VMEM(ids.shape, jnp.int32) for ids in (source_ids, relation_ids, target_ids, negative_ids)],
                pltpu.SemaphoreType.DMA((14,)),
                pltpu.VMEM((rows, edges), BF16),
                pltpu.VMEM((rels, edges), BF16),
                pltpu.VMEM((2, edges, dims), BF16),
                pltpu.VMEM((2, dims, edges), BF16),
                pltpu.VMEM((dims, edges), F32),
                pltpu.VMEM((dims, edges), F32),
                pltpu.VMEM((dims, edges), F32),
                pltpu.VMEM((1, rows), F32),
                pltpu.VMEM((n_rel, dims, rels), F32),
                pltpu.SemaphoreType.DMA((n_rel, len(blocks))),
                pltpu.SemaphoreType.DMA((n_rel, len(blocks))),
                pltpu.SemaphoreType.DMA((2, buckets - 1, chunks)),
                pltpu.SemaphoreType.DMA((2, buckets - 1, chunks)),
                pltpu.VMEM((buckets - 1, chunks, 1, 256), F32),
                pltpu.VMEM((buckets - 1, chunks, 1, 256), F32),
                pltpu.VMEM((2 * LANES, edges), BF16),
                pltpu.VMEM((edges, plan[-1][1]), F32),
                pltpu.VMEM((edges, plan[-1][1]), F32),
                *[pltpu.VMEM((2, dims, 256), BF16) for _ in plan],
                *[pltpu.VMEM((2, edges, 256), BF16) for _ in plan],
                *moves,
                *moves,
            ],
            compiler_params=pltpu.CompilerParams(
                collective_id=0, has_side_effects=True, vmem_limit_bytes=40 * 1024 * 1024
            ),
        )(*(
            pltpu.with_memory_space_constraint(x, pltpu.HBM) for x in (
                source_table, source_state, target_table, target_state,
                relation_ops, relation_state, source_ids, relation_ids,
                target_ids, negative_ids,
            )
        ))
        hbm = pl.BlockSpec(memory_space=pl.ANY)
        return pl.pallas_call(
            emit,
            out_shape=(
                shape((dims, rows), F32), shape((rows,), F32),
                shape((dims, rows), F32), shape((rows,), F32),
                shape((dims, rels), F32), shape((dims, rels), F32),
            ),
            in_specs=[vmem] * 6,
            out_specs=(hbm,) * 6,
            scratch_shapes=[pltpu.VMEM((rows,), F32), pltpu.VMEM((rows,), F32), pltpu.SemaphoreType.DMA((6,))],
            compiler_params=pltpu.CompilerParams(vmem_limit_bytes=16 * 1024 * 1024),
        )(*out)

    split_both = ("blk", "rel")
    return jax.shard_map(
        per_device,
        mesh=mesh,
        in_specs=(
            P(None, split_both), P(split_both), P(None, split_both), P(split_both),
            P(None, "blk"), P(None, "blk"),
            P(None, split_both), P(None, split_both), P(None, split_both), P(None, split_both),
        ),
        out_specs=(
            P(None, split_both), P(split_both), P(None, split_both), P(split_both),
            P(None, "blk"), P(None, "blk"),
        ),
        check_vma=False,
    )
```

```python
import functools

import jax
import jax.numpy as jnp
from jax import lax
from jax.experimental import pallas as pl
from jax.experimental.pallas import tpu as pltpu
from jax.sharding import PartitionSpec as P

learn_rate = 0.1
epsilon = 1e-06
LANES = 128
MESH = pl.DeviceIdType.MESH
F32 = jnp.float32
BF16 = jnp.bfloat16


def split(x):
    high = x.astype(BF16)
    return high, (x - high.astype(F32)).astype(BF16)


def nn(a, b):
    return lax.dot_general(a, b, (((1,), (0,)), ((), ())), preferred_element_type=F32)


def nt(a, b):
    return lax.dot_general(a, b, (((1,), (1,)), ((), ())), preferred_element_type=F32)


def both_nn(hi, lo, b):
    n = hi.shape[0]
    tall = nn(jnp.concatenate([hi, lo], axis=0), b)
    return tall[:n] + tall[n:]


def both_nt(hi, lo, b):
    n = hi.shape[0]
    tall = nt(jnp.concatenate([hi, lo], axis=0), b)
    return tall[:n] + tall[n:]


def column(row):
    wide = jnp.broadcast_to(row.astype(F32), (8, row.shape[1]))
    return jnp.transpose(wide)[:, :1].astype(jnp.int32)


def one_hot(row, height):
    low = lax.rem(row, LANES)
    inner = (lax.broadcasted_iota(jnp.int32, (LANES, row.shape[1]), 0) == low).astype(F32).astype(BF16)
    if height == LANES:
        return inner
    out = []
    for start in range(0, height, LANES):
        here = (row - low == start).astype(F32).astype(BF16)
        out.append(inner * jnp.broadcast_to(here, inner.shape))
    return jnp.concatenate(out, axis=0)


def chunk_plan(rows):
    if rows % 256 == 0 and rows >= 512:
        widths = [LANES] + [256] * (rows // 256 - 1) + [LANES]
    else:
        widths = [LANES] * (rows // LANES)
    return [(sum(widths[:i]), w) for i, w in enumerate(widths)]


def row_blocks(dims):
    first = (dims // 2 + 15) // 16 * 16
    return [(0, first), (first, dims - first)]


def lane_gather(table, index):
    tall = table.shape[0]
    groups = table.shape[1] // LANES
    out = []
    for start in range(0, index.shape[1], LANES):
        one = jnp.broadcast_to(index[:, start:start + LANES], (tall, LANES))
        low = lax.rem(one, LANES)
        got = jnp.take_along_axis(table[:, :LANES], low, axis=1)
        for g in range(1, groups):
            other = jnp.take_along_axis(table[:, g * LANES:(g + 1) * LANES], low, axis=1)
            got = jnp.where(one >= g * LANES, other, got)
        out.append(got)
    return jnp.concatenate(out, axis=1)


def emit(*refs):
    inputs, outputs, (first, second, sem) = refs[:6], refs[6:12], refs[12:]
    copies = []
    for i in (0, 2, 4, 5):
        copies.append(pltpu.make_async_copy(inputs[i], outputs[i], sem.at[i]))
        copies[-1].start()
    for i, line in ((1, first), (3, second)):
        line[...] = inputs[i][0, :]
        copies.append(pltpu.make_async_copy(line, outputs[i], sem.at[i]))
        copies[-1].start()
    for copy in copies:
        copy.wait()


def kernel(n_blk, n_rel, plan, blocks, *refs):
    refs = list(refs)

    def take(n):
        out = refs[:n]
        del refs[:n]
        return out

    src_in, srow_in, tgt_in, trow_in, rel_in, rstate_in, sid_in, rid_in, tid_in, nid_in = take(10)
    out_src, out_srow, out_tgt, out_trow, out_rel, out_rstate = take(6)
    src_ref, srow_ref, tgt_ref, trow_ref, rel_ref, rstate_ref, sid_ref, rid_ref, tid_ref, nid_ref = take(10)
    load_sem, hot, rhot, qt_ref, q_ref, picked, relation, gq_ref, counts, rel_all = take(10)
    rsend_sem, rrecv_sem, send_sem, recv_sem, row_send, row_recv = take(6)
    turned, base_ref, gain_ref = take(3)
    tables, weights = take(len(plan)), take(len(plan))
    send, recv = take(len(plan)), take(len(plan))
    dims, rows = src_ref.shape
    buckets, edges = sid_ref.shape
    negs = nid_ref.shape[1]
    rels = rel_ref.shape[1]
    final = len(plan) - 1
    groups = [(e, min(256, edges - e)) for e in range(0, edges, 256)]
    my_blk = lax.axis_index("blk")
    my_rel = lax.axis_index("rel")
    nxt = lax.rem(my_blk + 1, n_blk)
    prv = lax.rem(my_blk + n_blk - 1, n_blk)

    loads = []

    def load(there, here):
        loads.append(pltpu.make_async_copy(there, here, load_sem.at[len(loads)]))
        loads[-1].start()
        return loads[-1]

    load_ids = [
        load(sid_in, sid_ref), load(rid_in, rid_ref), load(nid_in, nid_ref), load(tid_in, tid_ref)
    ]
    quarter = dims // 64 * 16
    ends = [0, quarter, 2 * quarter, 3 * quarter, dims]
    load_src = [
        load(src_in.at[pl.ds(r, n - r)], src_ref.at[pl.ds(r, n - r)]) for r, n in ((0, ends[2]),)
    ]
    load_rel = load(rel_in, rel_ref)
    load_src += [
        load(src_in.at[pl.ds(r, n - r)], src_ref.at[pl.ds(r, n - r)]) for r, n in ((ends[2], dims),)
    ]
    wide = plan[0][1]
    load_first = [load(tgt_in.at[:, pl.ds(0, wide)], tgt_ref.at[:, pl.ds(0, wide)]), load(trow_in, trow_ref)]
    load_rest = []

    barrier = pltpu.get_barrier_semaphore()
    pl.semaphore_signal(barrier, inc=1, device_id={"blk": prv}, device_id_type=MESH)
    for step in range(1, n_rel):
        pl.semaphore_signal(
            barrier, inc=1, device_id={"rel": lax.rem(my_rel + step, n_rel)}, device_id_type=MESH
        )

    def hop(bucket, c):
        return pltpu.make_async_remote_copy(
            src_ref=send[c].at[bucket],
            dst_ref=recv[c].at[bucket],
            send_sem=send_sem.at[0, bucket, c],
            recv_sem=recv_sem.at[0, bucket, c],
            device_id={"blk": nxt},
            device_id_type=MESH,
        )

    def row_hop(bucket, c):
        return pltpu.make_async_remote_copy(
            src_ref=row_send.at[bucket, c, :, pl.ds(0, plan[c][1])],
            dst_ref=row_recv.at[bucket, c, :, pl.ds(0, plan[c][1])],
            send_sem=send_sem.at[1, bucket, c],
            recv_sem=recv_sem.at[1, bucket, c],
            device_id={"blk": nxt},
            device_id_type=MESH,
        )

    def rel_hop(to, slot, step, b):
        r, n = blocks[b]
        return pltpu.make_async_remote_copy(
            src_ref=rel_all.at[slot, pl.ds(r, n)],
            dst_ref=rel_all.at[slot, pl.ds(r, n)],
            send_sem=rsend_sem.at[step - 1, b],
            recv_sem=rrecv_sem.at[slot, b],
            device_id={"rel": to},
            device_id_type=MESH,
        )

    def put_pair(ref, hi, lo, twice, part=slice(None)):
        width = hi.shape[1]
        if width == LANES:
            ref[0, part, :LANES] = hi
            ref[0, part, LANES:] = lo
            if twice:
                ref[1, :, :LANES] = hi
                ref[1, :, LANES:] = hi
        else:
            ref[0, part, :] = hi
            ref[1, part, :] = lo

    def fold(wide):
        return wide[:, :LANES] + wide[:, LANES:]

    for copy in load_ids:
        copy.wait()

    for bucket in range(buckets):
        last = bucket + 1 == buckets
        now_src = src_ref if bucket == 0 else out_src
        sid = sid_ref[pl.ds(bucket, 1), :]
        rid = rid_ref[pl.ds(bucket, 1), :]
        hot[...] = one_hot(sid, rows)
        for first in (0, 2):
            part = pl.ds(ends[first], ends[first + 2] - ends[first])
            if bucket == 0:
                load_src[first // 2].wait()
                if first:
                    for copy in [load_rel] + load_first:
                        copy.wait()
                    if rows > wide:
                        late = pl.ds(wide, rows - wide)
                        load_rest.append(load(tgt_in.at[:, late], tgt_ref.at[:, late]))
                    load_rest.extend([load(srow_in, srow_ref), load(rstate_in, rstate_ref)])
            s_hi, s_lo = split(now_src[part, :])
            for e, m in groups:
                some = pl.ds(e, m)
                picked[part, some] = both_nn(s_hi, s_lo, hot[:, some])
        relation[...] = lane_gather(rel_ref[...], rid)
        for e, m in groups:
            some = pl.ds(e, m)
            hi, lo = split(picked[:, some] * relation[:, some])
            q_ref[0, :, some] = hi
            q_ref[1, :, some] = lo

        def turn():
            for e, m in groups:
                some = pl.ds(e, m)
                hi, lo = split(jnp.transpose(picked[:, some] * relation[:, some] * 0.5))
                qt_ref[0, some, :] = hi
                qt_ref[1, some, :] = lo
            nid = column(nid_ref[pl.ds(bucket, 1), :])
            for start in range(0, rows, LANES):
                lane = lax.broadcasted_iota(jnp.int32, (negs, LANES), 1) + start
                counts[:, pl.ds(start, LANES)] = jnp.sum(
                    (lane == nid).astype(F32), axis=0, keepdims=True
                ) * (0.5 / negs)
            rhot[...] = one_hot(rid, rels)
            return column(tid_ref[pl.ds(bucket, 1), :])

        def weigh_turned():
            table = tgt_ref[:, :LANES]
            hi, lo = split(table)
            put_pair(tables[0], hi, lo, True)
            hi, lo = split(jnp.transpose(table) * 0.5)
            wide = nn(jnp.concatenate([hi, lo], axis=0), q_ref[0])
            score = wide[:LANES] + wide[LANES:] + nn(hi, q_ref[1])
            half = jnp.tanh(score)
            here = lax.broadcasted_iota(jnp.int32, (LANES, negs), 0) == nid_ref[pl.ds(bucket, 1), :]
            count = jnp.sum(here.astype(F32), axis=1, keepdims=True) * (0.5 / negs)
            here = lax.broadcasted_iota(jnp.int32, (LANES, edges), 0) == tid_ref[pl.ds(bucket, 1), :]
            weight = count * half + count - jnp.where(here, 0.5 - 0.5 * half, 0.0)
            hi, lo = split(weight)
            turned[:LANES, :] = hi
            turned[LANES:, :] = lo

        base, gain = {}, {}

        def prepare(c):
            start, width = plan[c]
            count = counts[:, pl.ds(start, width)]
            base[c], gain[c] = {}, {}
            for e, m in groups:
                own = lax.broadcasted_iota(jnp.int32, (m, width), 1) + start == tid[e:e + m]
                half = jnp.where(own, 0.5, 0.0)
                base[c][e], gain[c][e] = count - half, count + half
                if c == final and bucket > 0:
                    base_ref[e:e + m, :], gain_ref[e:e + m, :] = base[c][e], gain[c][e]

        def weigh(c):
            start, width = plan[c]
            if c == final and bucket > 0:
                for e, m in groups:
                    base[c][e], gain[c][e] = base_ref[e:e + m, :], gain_ref[e:e + m, :]
            else:
                prepare(c)
            cols = pl.ds(start, width)
            table = tgt_ref[:, cols] if bucket == 0 else recv[c][bucket - 1]
            t_hi, t_lo = split(table)
            put_pair(tables[c], t_hi, t_lo, True)
            for e, m in groups:
                some = pl.ds(e, m)
                if width == LANES:
                    score = fold(nn(qt_ref[0, some, :], tables[c][0])) + nn(qt_ref[1, some, :], t_hi)
                else:
                    score = (
                        both_nn(qt_ref[0, some, :], qt_ref[1, some, :], t_hi) + nn(qt_ref[0, some, :], t_lo)
                    )
                half = jnp.tanh(score)
                weight = base[c][e] + gain[c][e] * half
                w_hi, w_lo = split(weight)
                put_pair(weights[c], w_hi, w_lo, False, some)

        def query_part(c, part, some=slice(None)):
            if bucket == 0 and c == 0:
                return (
                    nn(tables[c][1, part, :], turned[:, some])
                    + nn(tables[c][0, part, LANES:], turned[:LANES, some])
                )
            if plan[c][1] == LANES:
                return (
                    nt(tables[c][1, part, :], weights[c][0, some, :])
                    + nt(tables[c][0, part, LANES:], weights[c][0, some, :LANES])
                )
            return (
                both_nt(tables[c][0, part, :], tables[c][1, part, :], weights[c][0, some, :])
                + nt(tables[c][0, part, :], weights[c][1, some, :])
            )

        def finish(c):
            start, width = plan[c]
            cols = pl.ds(start, width)
            if bucket == 0:
                table = tgt_ref[:, cols]
                state = trow_ref[cols].reshape(1, width)
            else:
                if c == final:
                    row_hop(bucket - 1, c).wait_recv()
                table = recv[c][bucket - 1]
                state = row_recv[bucket - 1, c, :, :width]
            if bucket == 0 and c == 0:
                grad = fold(nt(q_ref[0], turned[...])) + nt(q_ref[1], turned[:LANES, :])
            elif width == LANES:
                grad = fold(nn(q_ref[0], weights[c][0])) + nn(q_ref[1], weights[c][0, :, :LANES])
            else:
                grad = both_nn(q_ref[0], q_ref[1], weights[c][0]) + nn(q_ref[0], weights[c][1])
            fresh = state + jnp.sum(grad * grad, axis=0, keepdims=True) * (1.0 / dims)
            new = table - grad * (learn_rate / (jnp.sqrt(fresh) + epsilon))
            if last:
                out_tgt[:, cols] = new
                out_trow[:, cols] = fresh
            else:
                send[c][bucket] = new
                row_send[bucket, c, :, :width] = fresh

        def relate(part, whole):
            g_hi, g_lo = split(whole * picked[part, :])
            rel_grad = both_nt(g_hi, g_lo, rhot[...])
            if bucket == 0:
                rel_all[my_rel, part, :] = rel_grad
            else:
                rel_all[my_rel, part, :] = rel_all[my_rel, part, :] + rel_grad

        everything = pl.ds(0, dims)

        def arrive(c):
            if bucket > 0:
                hop(bucket - 1, c).wait_recv()
                if c < final:
                    row_hop(bucket - 1, c).wait_recv()

        def depart(c):
            hop(bucket, c).start()
            row_hop(bucket, c).start()

        if not last:
            if bucket == 0:
                weigh_turned()
                finish(0)
                pl.semaphore_wait(barrier, n_rel)
                depart(0)
                for copy in load_rest:
                    copy.wait()
                tid = turn()
            else:
                tid = turn()
                arrive(0)
                weigh(0)
                finish(0)
                depart(0)
            if final > 0:
                arrive(1)
                weigh(1)
            for c in range(1, final + 1):
                if c < final:
                    arrive(c + 1)
                finish(c)
                if c == 1:
                    depart(c)
                if c < final:
                    weigh(c + 1)
                if c > 1:
                    depart(c)
            total = query_part(0, everything)
            for c in range(1, len(plan)):
                total += query_part(c, everything)
            gq_ref[...] = total
            relate(everything, total)
        else:
            def gather_query(c):
                part = query_part(c, everything)
                gq_ref[...] = part if c == 0 else gq_ref[...] + part

            tid = turn()
            if bucket == 0:
                pl.semaphore_wait(barrier, n_rel)
                for copy in load_rest:
                    copy.wait()
            for c in range(final):
                arrive(c)
                weigh_turned() if bucket == 0 and c == 0 else weigh(c)
                if c > 0:
                    gather_query(c - 1)
                    finish(c - 1)
            if final > 0:
                gather_query(final - 1)
                finish(final - 1)
            if bucket > 0:
                prepare(final)
            arrive(final)
            weigh(final)
            for b, (r, n) in enumerate(blocks):
                part = pl.ds(r, n)
                rel_grad = rel_all[my_rel, part, :] if bucket > 0 else 0.0
                for e, m in groups:
                    some = pl.ds(e, m)
                    whole = query_part(final, part, some)
                    if final > 0:
                        whole = gq_ref[part, some] + whole
                    gq_ref[part, some] = whole
                    g_hi, g_lo = split(whole * picked[part, some])
                    rel_grad += both_nt(g_hi, g_lo, rhot[:, some])
                rel_all[my_rel, part, :] = rel_grad
                for step in range(1, n_rel):
                    rel_hop(lax.rem(my_rel + step, n_rel), my_rel, step, b).start()
            finish(final)
        g_hi, g_lo = split(gq_ref[...] * relation[...])
        src_grad = both_nt(g_hi, g_lo, hot[...])
        now_srow = srow_ref[...].reshape(1, rows) if bucket == 0 else out_srow[...]
        fresh = now_srow + jnp.sum(src_grad * src_grad, axis=0, keepdims=True) * (1.0 / dims)
        out_src[...] = now_src[...] - src_grad * (learn_rate / (jnp.sqrt(fresh) + epsilon))
        out_srow[...] = fresh

    for bucket in range(buckets - 1):
        for c in range(len(plan)):
            hop(bucket, c).wait_send()
            row_hop(bucket, c).wait_send()
    for b, (r, n) in enumerate(blocks):
        part = pl.ds(r, n)
        for step in range(1, n_rel):
            peer = lax.rem(my_rel + n_rel - step, n_rel)
            arrived = rel_hop(peer, peer, step, b)
            arrived.wait_send()
            arrived.wait_recv()
        total = rel_all[0, part, :]
        for step in range(1, n_rel):
            total = total + rel_all[step, part, :]
        new_state = rstate_ref[part, :] + total * total
        out_rstate[part, :] = new_state
        out_rel[part, :] = rel_ref[part, :] - learn_rate * total / (jnp.sqrt(new_state) + epsilon)


def solution(mesh):
    n_blk, n_rel = mesh.shape["blk"], mesh.shape["rel"]

    def per_device(
        source_table, source_state, target_table, target_state, relation_ops, relation_state,
        source_ids, target_ids, relation_ids, negative_ids,
    ):
        dims, rows = source_table.shape
        rels = relation_ops.shape[1]
        buckets, edges = source_ids.shape
        plan = chunk_plan(rows)
        blocks = row_blocks(dims)
        chunks = len(plan)
        vmem = pl.BlockSpec(memory_space=pltpu.VMEM)
        shape = jax.ShapeDtypeStruct
        moves = [pltpu.VMEM((buckets - 1, dims, width), F32) for _, width in plan]
        out = pl.pallas_call(
            functools.partial(kernel, n_blk, n_rel, plan, blocks),
            out_shape=(
                pltpu.VMEM((dims, rows), F32), pltpu.VMEM((1, rows), F32),
                pltpu.VMEM((dims, rows), F32), pltpu.VMEM((1, rows), F32),
                pltpu.VMEM((dims, rels), F32), pltpu.VMEM((dims, rels), F32),
            ),
            in_specs=[pl.BlockSpec(memory_space=pltpu.HBM)] * 10,
            out_specs=(vmem,) * 6,
            scratch_shapes=[
                pltpu.VMEM((dims, rows), F32), pltpu.VMEM((rows,), F32),
                pltpu.VMEM((dims, rows), F32), pltpu.VMEM((rows,), F32),
                pltpu.VMEM((dims, rels), F32), pltpu.VMEM((dims, rels), F32),
                *[pltpu.VMEM(ids.shape, jnp.int32) for ids in (source_ids, relation_ids, target_ids, negative_ids)],
                pltpu.SemaphoreType.DMA((14,)),
                pltpu.VMEM((rows, edges), BF16),
                pltpu.VMEM((rels, edges), BF16),
                pltpu.VMEM((2, edges, dims), BF16),
                pltpu.VMEM((2, dims, edges), BF16),
                pltpu.VMEM((dims, edges), F32),
                pltpu.VMEM((dims, edges), F32),
                pltpu.VMEM((dims, edges), F32),
                pltpu.VMEM((1, rows), F32),
                pltpu.VMEM((n_rel, dims, rels), F32),
                pltpu.SemaphoreType.DMA((n_rel, len(blocks))),
                pltpu.SemaphoreType.DMA((n_rel, len(blocks))),
                pltpu.SemaphoreType.DMA((2, buckets - 1, chunks)),
                pltpu.SemaphoreType.DMA((2, buckets - 1, chunks)),
                pltpu.VMEM((buckets - 1, chunks, 1, 256), F32),
                pltpu.VMEM((buckets - 1, chunks, 1, 256), F32),
                pltpu.VMEM((2 * LANES, edges), BF16),
                pltpu.VMEM((edges, plan[-1][1]), F32),
                pltpu.VMEM((edges, plan[-1][1]), F32),
                *[pltpu.VMEM((2, dims, 256), BF16) for _ in plan],
                *[pltpu.VMEM((2, edges, 256), BF16) for _ in plan],
                *moves,
                *moves,
            ],
            compiler_params=pltpu.CompilerParams(
                collective_id=0, has_side_effects=True, vmem_limit_bytes=40 * 1024 * 1024
            ),
        )(*(
            pltpu.with_memory_space_constraint(x, pltpu.HBM) for x in (
                source_table, source_state, target_table, target_state,
                relation_ops, relation_state, source_ids, relation_ids,
                target_ids, negative_ids,
            )
        ))
        hbm = pl.BlockSpec(memory_space=pl.ANY)
        return pl.pallas_call(
            emit,
            out_shape=(
                shape((dims, rows), F32), shape((rows,), F32),
                shape((dims, rows), F32), shape((rows,), F32),
                shape((dims, rels), F32), shape((dims, rels), F32),
            ),
            in_specs=[vmem] * 6,
            out_specs=(hbm,) * 6,
            scratch_shapes=[pltpu.VMEM((rows,), F32), pltpu.VMEM((rows,), F32), pltpu.SemaphoreType.DMA((6,))],
            compiler_params=pltpu.CompilerParams(vmem_limit_bytes=16 * 1024 * 1024),
        )(*out)

    split_both = ("blk", "rel")
    return jax.shard_map(
        per_device,
        mesh=mesh,
        in_specs=(
            P(None, split_both), P(split_both), P(None, split_both), P(split_both),
            P(None, "blk"), P(None, "blk"),
            P(None, split_both), P(None, split_both), P(None, split_both), P(None, split_both),
        ),
        out_specs=(
            P(None, split_both), P(split_both), P(None, split_both), P(split_both),
            P(None, "blk"), P(None, "blk"),
        ),
        check_vma=False,
    )
```
